8 devices in a mesh: cp: 8 (over z, y, x, core).
Axes of the slice: x: 2, y: 2, z: 1, core: 2. Of those that a mesh axis runs over, the one named last changes fastest.
Arguments:
- query: bfloat16 [4, 2048, 12, 128], P(None, 'cp')
- key_in: bfloat16 [4, 2048, 12, 128], P(None, 'cp')
- value: bfloat16 [4, 2048, 12, 128], P(None, 'cp')
- bias_u: bfloat16 [12, 128], replicated
- bias_w: bfloat16 [12, 128], replicated
- rel_k: bfloat16 [2048, 12, 128], replicated
- d_out: bfloat16 [4, 2048, 12, 128], P(None, 'cp')
Outputs:
- output 1: bfloat16 [4, 2048, 12, 128], P(None, 'cp')
- output 2: bfloat16 [4, 2048, 12, 128], P(None, 'cp')
- output 3: bfloat16 [4, 2048, 12, 128], P(None, 'cp')
- output 4: bfloat16 [4, 2048, 12, 128], P(None, 'cp')
- output 5: float32 [12, 128], replicated
- output 6: float32 [12, 128], replicated
- output 7: float32 [2048, 12, 128], replicated
All inputs are finite; a program needn't handle non-finite values.
Results may differ from the reference program's by a relative error of at most 0.00869742.
Values are sent between devices in bfloat16 or wider.
A program may use at most 1 GiB of HBM per device.

```python
import jax
import jax.numpy as jnp
from jax import lax

BATCH = 4
SEQ_DEV = 256
SEQ = 2048
HEADS = 12
HEAD = 128
FREQS = 64


def rel_table(rng_key):
    distance = jnp.arange(SEQ, dtype=jnp.float32)[:, None]
    inv_freq = 1.0 / (10000.0 ** (jnp.arange(FREQS, dtype=jnp.float32) / FREQS))
    angles = distance * inv_freq[None, :]
    sinusoid = jnp.concatenate([jnp.sin(angles), jnp.cos(angles)], axis=1)
    rel_proj = jax.random.normal(rng_key, (2 * FREQS, HEADS * HEAD), jnp.float32) * FREQS ** -0.5
    return jnp.dot(sinusoid, rel_proj).reshape(SEQ, HEADS, HEAD).astype(jnp.bfloat16)


def setup_inputs(seed: int = 0) -> dict:
    rng_keys = jax.random.split(jax.random.key(seed), 7)
    act_shape = (BATCH, SEQ, HEADS, HEAD)
    query = jax.random.normal(rng_keys[0], act_shape, jnp.float32)
    key_in = jax.random.normal(rng_keys[1], act_shape, jnp.float32)
    value = jax.random.normal(rng_keys[2], act_shape, jnp.float32)
    d_out = jax.random.normal(rng_keys[3], act_shape, jnp.float32)
    bias_u = 0.5 * jax.random.normal(rng_keys[4], (HEADS, HEAD), jnp.float32)
    bias_w = 0.5 * jax.random.normal(rng_keys[5], (HEADS, HEAD), jnp.float32)
    return {
        'query': query.astype(jnp.bfloat16),
        'key_in': key_in.astype(jnp.bfloat16),
        'value': value.astype(jnp.bfloat16),
        'bias_u': bias_u.astype(jnp.bfloat16),
        'bias_w': bias_w.astype(jnp.bfloat16),
        'rel_k': rel_table(rng_keys[6]),
        'd_out': d_out.astype(jnp.bfloat16),
    }


def reference(query, key_in, value, bias_u, bias_w, rel_k, d_out):
    inv_sqrt = HEAD ** -0.5
    n_blocks = SEQ // SEQ_DEV
    q_u = (query.astype(jnp.float32) + bias_u.astype(jnp.float32)).astype(jnp.bfloat16)
    q_w = (query.astype(jnp.float32) + bias_w.astype(jnp.float32)).astype(jnp.bfloat16)
    pos_row = jnp.arange(SEQ_DEV)[:, None]
    pos_col = jnp.arange(SEQ)[None, :]

    def per_head(head_args):
        qu_h, qw_h, key_h, val_h, dout_h, rel_h = head_args

        def per_row(row_carry, row_args):
            qu_r, qw_r, key_r, val_r, dout_r = row_args

            def per_block(blk_carry, blk_idx):
                dk_acc, dv_acc, drel_acc, du_acc, dw_acc = blk_carry
                start = blk_idx * SEQ_DEV
                qu_b = lax.dynamic_slice_in_dim(qu_r, start, SEQ_DEV, 0)
                qw_b = lax.dynamic_slice_in_dim(qw_r, start, SEQ_DEV, 0)
                dout_b = lax.dynamic_slice_in_dim(dout_r, start, SEQ_DEV, 0)
                pos_q = start + pos_row
                causal = pos_col <= pos_q
                dist_idx = jnp.clip(pos_q - pos_col, 0, SEQ - 1)
                content = jnp.dot(qu_b, key_r.T, preferred_element_type=jnp.float32)
                by_dist = jnp.dot(qw_b, rel_h.T, preferred_element_type=jnp.float32)
                rel_part = jnp.take_along_axis(by_dist, dist_idx, axis=1)
                logits = jnp.where(causal, (content + rel_part) * inv_sqrt, -jnp.inf)
                attn_p = jax.nn.softmax(logits, axis=-1)
                probs_b = attn_p.astype(jnp.bfloat16)
                out_b = jnp.dot(probs_b, val_r, preferred_element_type=jnp.float32).astype(jnp.bfloat16)
                d_probs = jnp.dot(dout_b, val_r.T, preferred_element_type=jnp.float32)
                row_dot = jnp.sum(d_probs * attn_p, axis=-1, keepdims=True)
                d_logit = (attn_p * (d_probs - row_dot) * inv_sqrt).astype(jnp.bfloat16)
                d_dist = jnp.where(causal, jnp.take_along_axis(d_logit, dist_idx, axis=1), 0.0).astype(jnp.bfloat16)
                dq_cont = jnp.dot(d_logit, key_r, preferred_element_type=jnp.float32)
                dq_rel = jnp.dot(d_dist, rel_h, preferred_element_type=jnp.float32)
                dq_b = (dq_cont + dq_rel).astype(jnp.bfloat16)
                dk_acc = dk_acc + jnp.dot(d_logit.T, qu_b, preferred_element_type=jnp.float32)
                dv_acc = dv_acc + jnp.dot(probs_b.T, dout_b, preferred_element_type=jnp.float32)
                drel_acc = drel_acc + jnp.dot(d_dist.T, qw_b, preferred_element_type=jnp.float32)
                du_acc = du_acc + jnp.sum(dq_cont, axis=0)
                dw_acc = dw_acc + jnp.sum(dq_rel, axis=0)
                return (dk_acc, dv_acc, drel_acc, du_acc, dw_acc), (out_b, dq_b)

            drel_acc, du_acc, dw_acc = row_carry
            zeros_seq = jnp.zeros((SEQ, HEAD), jnp.float32)
            blk_out, blk_ys = lax.scan(per_block, (zeros_seq, zeros_seq, drel_acc, du_acc, dw_acc), jnp.arange(n_blocks))
            dk_acc, dv_acc, drel_acc, du_acc, dw_acc = blk_out
            out_r, dq_r = blk_ys
            row_outs = (out_r.reshape(SEQ, HEAD), dq_r.reshape(SEQ, HEAD), dk_acc.astype(jnp.bfloat16), dv_acc.astype(jnp.bfloat16))
            return (drel_acc, du_acc, dw_acc), row_outs

        zeros_dim = jnp.zeros((HEAD,), jnp.float32)
        head_carry, row_outs = lax.scan(per_row, (jnp.zeros((SEQ, HEAD), jnp.float32), zeros_dim, zeros_dim), (qu_h, qw_h, key_h, val_h, dout_h))
        drel_h, du_h, dw_h = head_carry
        return row_outs + (du_h, dw_h, drel_h)

    def by_head(tensor):
        return jnp.transpose(tensor, (2, 0, 1, 3))

    def by_pos(tensor):
        return jnp.transpose(tensor, (1, 2, 0, 3))

    head_outs = lax.map(per_head, (by_head(q_u), by_head(q_w), by_head(key_in), by_head(value), by_head(d_out), jnp.transpose(rel_k, (1, 0, 2))))
    out_h, dq_h, dk_h, dv_h, du_h, dw_h, drel_h = head_outs
    return (by_pos(out_h), by_pos(dq_h), by_pos(dk_h), by_pos(dv_h), du_h, dw_h, jnp.transpose(drel_h, (1, 0, 2)))
```

```python
import jax
import jax.numpy as jnp
from jax import lax
from jax.experimental import pallas as pl
from jax.experimental.pallas import tpu as pltpu
from jax.sharding import PartitionSpec as P

T = 256
D = 128
H = 128
NT = 8
NU = 6
F32 = jnp.float32
BF = jnp.bfloat16
MESH = pl.DeviceIdType.MESH


def dot_nt(lhs, rhs):
    return lax.dot_general(lhs, rhs, (((1,), (1,)), ((), ())), preferred_element_type=F32)


def dot_nn(lhs, rhs):
    return lax.dot_general(lhs, rhs, (((1,), (0,)), ((), ())), preferred_element_type=F32)


def dot_tn(lhs, rhs):
    return lax.dot_general(lhs, rhs, (((0,), (0,)), ((), ())), preferred_element_type=F32)


def unit(x, rk, u, w, stage, drk, duw, scratch, after_tile):
    s_ref, dp_ref, r_ref, r_ref2, u_ref, dk_ref, dv_ref, a_ref, c_ref, oacc, qc_acc, qr_acc = scratch
    scale = D ** -0.5
    c2 = scale * 1.4426950408889634
    low = lax.broadcasted_iota(jnp.int32, (H, H), 1) <= lax.broadcasted_iota(jnp.int32, (H, H), 0)
    idx = (lax.broadcasted_iota(jnp.int32, (T, H), 0) - lax.broadcasted_iota(jnp.int32, (T, H), 1)) & (H - 1)

    def gather(arr):
        return jnp.take_along_axis(arr, idx, axis=1, mode="promise_in_bounds")

    dk_ref[...] = jnp.zeros_like(dk_ref)
    dv_ref[...] = jnp.zeros_like(dv_ref)

    def tile(ii, _):
        i = NT - 1 - ii
        q = x[i, 0].astype(F32)
        a_ref[...] = (q + u[...]).astype(BF)
        c_ref[...] = (q + w[...]).astype(BF)

        def logits(n, mx):
            j = i - n
            by = dot_nt(c_ref[...], rk[n])
            s = dot_nt(a_ref[...], x[j, 1])
            n0 = gather(by[:, :H])
            n1 = gather(by[:, H:])
            p0 = jnp.where(n == 0, -jnp.inf, r_ref2[...])
            p1 = jnp.where(n == 0, -jnp.inf, r_ref[...])
            lo = jnp.concatenate([jnp.where(low, n0[:H], p1[:H]), jnp.where(low, n1[H:], n0[H:])], 0)
            hi = jnp.concatenate([jnp.where(low, p1[:H], p0), jnp.where(low, n0[H:], p1[H:])], 0)
            s = s + jnp.concatenate([lo, hi], 1)
            r_ref[...] = n1
            r_ref2[...] = n0[:H]
            s_ref[j] = s
            return jnp.maximum(mx, jnp.maximum(s[:, :H], s[:, H:]))

        mx = lax.fori_loop(0, i + 1, logits, jnp.full((T, H), -jnp.inf, F32))
        m = jnp.max(mx, axis=1, keepdims=True)

        def weights(j, carry):
            total, dots = carry
            p = jnp.exp2((s_ref[j] - m) * c2)
            dp = dot_nt(x[i, 3], x[j, 2])
            s_ref[j] = p
            dp_ref[j] = dp
            pd = p * dp
            return total + (p[:, :H] + p[:, H:]), dots + (pd[:, :H] + pd[:, H:])

        zero = jnp.zeros((T, H), F32)
        total, dots = lax.fori_loop(0, i + 1, weights, (zero, zero))
        inv = 1.0 / jnp.sum(total, axis=1, keepdims=True)
        row_dot = jnp.sum(dots, axis=1, keepdims=True) * inv
        oacc[...] = zero
        qc_acc[...] = zero
        qr_acc[...] = zero
        u_ref[...] = jnp.zeros_like(u_ref)

        def grads(j, _):
            pn = s_ref[j] * inv
            pb = pn.astype(BF)
            ds = pn * (dp_ref[j] - row_dot) * scale
            dsb = ds.astype(BF)
            oacc[...] += dot_nn(pb, x[j, 2])
            dv_ref[j] += dot_tn(pb, x[i, 3])
            qc_acc[...] += dot_nn(dsb, x[j, 1])
            dk_ref[j] += dot_tn(dsb, a_ref[...])
            g0 = gather(ds[:, :H])
            g1 = gather(ds[:, H:])
            d0 = jnp.concatenate([jnp.where(low, g0[:H], u_ref[1, :H]), jnp.where(low, g1[H:], g0[H:])], 0)
            d1 = jnp.concatenate([jnp.where(low, u_ref[1, :H], u_ref[0, :H]), jnp.where(low, g0[H:], u_ref[1, H:])], 0)
            dist = jnp.concatenate([d0, d1], 1).astype(BF)
            u_ref[0] = g0
            u_ref[1] = g1
            qr_acc[...] += dot_nn(dist, rk[i - j])
            drk[i - j] += dot_tn(dist, c_ref[...])
            return 0

        lax.fori_loop(0, i + 1, grads, 0)
        qc = qc_acc[...]
        qr = qr_acc[...]
        duw[0:1] += jnp.sum(qc, axis=0, keepdims=True)
        duw[1:2] += jnp.sum(qr, axis=0, keepdims=True)
        stage[i, 0] = oacc[...].astype(BF)
        stage[i, 1] = (qc + qr).astype(BF)
        stage[i, 2] = dk_ref[i].astype(BF)
        stage[i, 3] = dv_ref[i].astype(BF)
        after_tile(i)
        return 0

    lax.fori_loop(0, NT, tile, 0)


UNIT_SCRATCH = [
    pltpu.VMEM((NT, T, T), F32), pltpu.VMEM((NT, T, T), F32), pltpu.VMEM((T, H), F32), pltpu.VMEM((H, H), F32),
    pltpu.VMEM((2, T, H), F32), pltpu.VMEM((NT, T, D), F32), pltpu.VMEM((NT, T, D), F32), pltpu.VMEM((T, D), BF),
    pltpu.VMEM((T, D), BF), pltpu.VMEM((T, D), F32), pltpu.VMEM((T, D), F32), pltpu.VMEM((T, D), F32)]


def kernel(xq, xk, xv, xd, rel, uw, oq, odq, odk, odv, drk_out, duw_out, rin, stage, drk, pbuf, dfin, duw, rk,
           in_send, in_recv, in_loc, out_send, out_recv, out_loc, half_send, half_recv,
           fin_send, fin_recv, fin_loc, rel_send, rel_recv, duw_send, duw_recv, duw_loc, rk_sem, *scratch):
    me = lax.axis_index('cp')
    chip = me // 2
    core = me % 2
    ins = (xq, xk, xv, xd)
    outs = (oq, odq, odk, odv)

    def remote(src, dst, ssem, rsem, dev):
        return pltpu.make_async_remote_copy(src_ref=src, dst_ref=dst, send_sem=ssem, recv_sem=rsem,
                                            device_id=(dev,), device_id_type=MESH)

    def spot(arr, dev, n):
        return arr.at[2 * (dev % 2) + n % 2, 3 * (dev // 2) + n // 2]

    def send_in(n, mask):
        dev = jnp.bitwise_xor(me, mask)
        for a in range(4):
            remote(spot(ins[a], dev, n), rin.at[n, me, a], in_send.at[n, mask], in_recv.at[n, mask], dev).start()

    def in_wait(n, mask):
        dev = jnp.bitwise_xor(me, mask)
        return remote(rin.at[n, dev], rin.at[n, dev], in_send.at[n, mask], in_recv.at[n, mask], dev)

    rk_copy = pltpu.make_async_copy(rel.at[pl.ds(3 * chip, 3)], rk, rk_sem)
    rk_copy.start()
    for n in range(NU):
        for a in range(4):
            pltpu.make_async_copy(spot(ins[a], me, n), rin.at[n, me, a], in_loc.at[n]).start()
        for mask in (6, 2, 4, 7, 3, 5, 1):
            send_in(n, mask)

    drk[...] = jnp.zeros_like(drk)
    duw[...] = jnp.zeros_like(duw)
    rk_copy.wait()

    def half_copy(k):
        return remote(drk.at[k, pl.ds(4 * (1 - core), 4)], pbuf.at[k], half_send.at[k], half_recv.at[k],
                      jnp.bitwise_xor(me, 1))

    def fin_copy(k, n, mask):
        return remote(dfin.at[k], drk_out.at[3 * chip + k, pl.ds(4 * core, 4)], fin_send.at[k, n], fin_recv.at[k, n],
                      jnp.bitwise_xor(me, mask))

    def fin_own(k):
        return pltpu.make_async_copy(dfin.at[k], drk_out.at[3 * chip + k, pl.ds(4 * core, 4)], fin_loc.at[k])

    fin_masks = (1, 6, 2, 4)

    def run_unit(n, _):
        k = n // 2
        pltpu.make_async_copy(rin.at[n, me], rin.at[n, me], in_loc.at[n]).wait()
        for mask in range(1, 8):
            in_wait(n, mask).wait_recv()

        def after_tile(i):
            mask = jnp.bitwise_xor(me, i)

            @pl.when(mask != 0)
            def _():
                for a in range(4):
                    remote(stage.at[n, i, a], spot(outs[a], me, n), out_send.at[n, i], out_recv.at[n, mask], i).start()

            @pl.when(mask == 0)
            def _():
                for a in range(4):
                    pltpu.make_async_copy(stage.at[n, i, a], spot(outs[a], me, n), out_loc.at[n]).start()

        unit(rin.at[n], rk.at[k], uw.at[k, 0:1], uw.at[k, 1:2], stage.at[n], drk.at[k], duw.at[k], scratch, after_tile)

        @pl.when(n % 2 == 1)
        def _():
            copy = half_copy(k)
            copy.start()
            copy.wait()
            dfin[k] = drk[k, pl.ds(4 * core, 4)] + pbuf[k]
            for s, mask in enumerate(fin_masks):
                fin_copy(k, s, mask).start()
            fin_own(k).start()
        return 0

    lax.fori_loop(0, NU, run_unit, 0)

    def duw_copy(mask):
        return remote(duw, duw_out.at[me], duw_send.at[mask], duw_recv.at[mask], jnp.bitwise_xor(me, mask))

    for mask in range(1, 8):
        duw_copy(mask).start()
    duw_own = pltpu.make_async_copy(duw, duw_out.at[me], duw_loc)
    duw_own.start()

    def relay(k, s):
        part = drk_out.at[3 * jnp.bitwise_xor(chip, fin_masks[s] // 2) + k, pl.ds(4 * core, 4)]
        return remote(part, part, rel_send.at[k, s], rel_recv.at[k, s], jnp.bitwise_xor(me, 1))

    for k in range(3):
        for s in range(1, 4):
            fin_copy(k, s, fin_masks[s]).wait_recv()
            relay(k, s).start()

    def finish(n, _):
        for mask in range(1, 8):
            dev = jnp.bitwise_xor(me, mask)
            in_wait(n, mask).wait_send()
            remote(stage.at[n, dev], stage.at[n, dev], out_send.at[n, dev], out_recv.at[n, mask], dev).wait()
        pltpu.make_async_copy(stage.at[n, me], stage.at[n, me], out_loc.at[n]).wait()
        return 0

    lax.fori_loop(0, NU, finish, 0)
    for k in range(3):
        fin_copy(k, 0, 1).wait()
        fin_own(k).wait()
        for s in range(1, 4):
            fin_copy(k, s, fin_masks[s]).wait_send()
            relay(k, s).wait()
    for mask in range(1, 8):
        duw_copy(mask).wait()
    duw_own.wait()


def exchange_attend(xq, xk, xv, xd, rel, uw):
    any_spec = pl.BlockSpec(memory_space=pl.ANY)
    vmem_spec = pl.BlockSpec(memory_space=pltpu.VMEM)
    dma = pltpu.SemaphoreType.DMA
    act = jax.ShapeDtypeStruct((4, 12, T, D), BF)
    return pl.pallas_call(
        kernel,
        out_shape=(act, act, act, act, jax.ShapeDtypeStruct((12, NT, T, D), F32),
                   jax.ShapeDtypeStruct((8, 3, 8, D), F32)),
        in_specs=[any_spec] * 5 + [vmem_spec],
        out_specs=(any_spec,) * 6,
        scratch_shapes=[
            pltpu.VMEM((NU, 8, 4, T, D), BF), pltpu.VMEM((NU, NT, 4, T, D), BF), pltpu.VMEM((3, NT, T, D), F32),
            pltpu.VMEM((3, 4, T, D), F32), pltpu.VMEM((3, 4, T, D), F32), pltpu.VMEM((3, 8, D), F32),
            pltpu.VMEM((3, NT, T, D), BF),
            dma((NU, 8)), dma((NU, 8)), dma((NU,)), dma((NU, 8)), dma((NU, 8)), dma((NU,)), dma((3,)), dma((3,)),
            dma((3, 4)), dma((3, 4)), dma((3,)), dma((3, 4)), dma((3, 4)), dma((8,)), dma((8,)), dma(()), dma(())]
        + UNIT_SCRATCH,
        compiler_params=pltpu.CompilerParams(has_side_effects=True, vmem_limit_bytes=62 * 1024 * 1024),
    )(xq, xk, xv, xd, rel, uw)


def solution(mesh):
    seq_spec = P(None, 'cp', None, None)

    def local(query, key_in, value, bias_u, bias_w, rel_k, d_out):
        chip = lax.axis_index('cp') // 2

        def by_head(arr):
            return arr.transpose(0, 2, 1, 3)

        rel = rel_k.transpose(1, 0, 2).reshape(12, NT, T, D)
        both = jnp.stack([bias_u, bias_w], axis=1).astype(F32)
        uw = lax.dynamic_slice_in_dim(both, 3 * chip, 3, 0)
        res = exchange_attend(by_head(query), by_head(key_in), by_head(value), by_head(d_out), rel, uw)
        d_rel = res[4].reshape(12, NT * T, D).transpose(1, 0, 2)
        duw = res[5].reshape(4, 2, 3, 8, D).sum(axis=1).reshape(12, 8, D)
        return tuple(by_head(arr) for arr in res[:4]) + (duw[:, 0], duw[:, 1], d_rel)

    return jax.shard_map(local, mesh=mesh,
                         in_specs=(seq_spec, seq_spec, seq_spec, P(), P(), P(), seq_spec),
                         out_specs=(seq_spec, seq_spec, seq_spec, seq_spec, P(), P(), P()),
                         check_vma=False)
```

```python
import jax
import jax.numpy as jnp
from jax import lax
from jax.experimental import pallas as pl
from jax.experimental.pallas import tpu as pltpu
from jax.sharding import PartitionSpec as P

T = 256
D = 128
H = 128
NT = 8
NU = 6
VMEM_LIMIT = 36 * 1024 * 1024
F32 = jnp.float32
BF = jnp.bfloat16
MESH = pl.DeviceIdType.MESH


def dot_nt(lhs, rhs):
    return lax.dot_general(lhs, rhs, (((1,), (1,)), ((), ())), preferred_element_type=F32)


def dot_nn(lhs, rhs):
    return lax.dot_general(lhs, rhs, (((1,), (0,)), ((), ())), preferred_element_type=F32)


def dot_tn(lhs, rhs):
    return lax.dot_general(lhs, rhs, (((0,), (0,)), ((), ())), preferred_element_type=F32)


def unit(x, rk, u, w, drk, duw, scratch, after_tile):
    s_ref, dp_ref, r_ref, r_ref2, u_ref, dk_ref, dv_ref, a_ref, c_ref, oacc, qc_acc, qr_acc = scratch
    scale = D ** -0.5
    c2 = scale * 1.4426950408889634
    low = lax.broadcasted_iota(jnp.int32, (H, H), 1) <= lax.broadcasted_iota(jnp.int32, (H, H), 0)
    idx = (lax.broadcasted_iota(jnp.int32, (T, H), 0) - lax.broadcasted_iota(jnp.int32, (T, H), 1)) & (H - 1)

    def gather(arr):
        return jnp.take_along_axis(arr, idx, axis=1, mode="promise_in_bounds")

    dk_ref[...] = jnp.zeros_like(dk_ref)
    dv_ref[...] = jnp.zeros_like(dv_ref)

    def tile(ii, _):
        i = NT - 1 - ii
        q = x[i, 0].astype(F32)
        a_ref[...] = (q + u).astype(BF)
        c_ref[...] = (q + w).astype(BF)

        def logits(n, mx):
            j = i - n
            by = dot_nt(c_ref[...], rk[n])
            s = dot_nt(a_ref[...], x[j, 1])
            n0 = gather(by[:, :H])
            n1 = gather(by[:, H:])
            p0 = jnp.where(n == 0, -jnp.inf, r_ref2[...])
            p1 = jnp.where(n == 0, -jnp.inf, r_ref[...])
            lo = jnp.concatenate([jnp.where(low, n0[:H], p1[:H]), jnp.where(low, n1[H:], n0[H:])], 0)
            hi = jnp.concatenate([jnp.where(low, p1[:H], p0), jnp.where(low, n0[H:], p1[H:])], 0)
            s = s + jnp.concatenate([lo, hi], 1)
            r_ref[...] = n1
            r_ref2[...] = n0[:H]
            s_ref[j] = s
            return jnp.maximum(mx, jnp.maximum(s[:, :H], s[:, H:]))

        mx = lax.fori_loop(0, i + 1, logits, jnp.full((T, H), -jnp.inf, F32))
        m = jnp.max(mx, axis=1, keepdims=True)

        def weights(j, carry):
            total, dots = carry
            p = jnp.exp2((s_ref[j] - m) * c2)
            dp = dot_nt(x[i, 3], x[j, 2])
            s_ref[j] = p
            dp_ref[j] = dp
            pd = p * dp
            return total + (p[:, :H] + p[:, H:]), dots + (pd[:, :H] + pd[:, H:])

        zero = jnp.zeros((T, H), F32)
        total, dots = lax.fori_loop(0, i + 1, weights, (zero, zero))
        inv = 1.0 / jnp.sum(total, axis=1, keepdims=True)
        row_dot = jnp.sum(dots, axis=1, keepdims=True) * inv
        oacc[...] = zero
        qc_acc[...] = zero
        qr_acc[...] = zero
        u_ref[...] = jnp.zeros_like(u_ref)

        def grads(j, _):
            pn = s_ref[j] * inv
            pb = pn.astype(BF)
            ds = pn * (dp_ref[j] - row_dot) * scale
            dsb = ds.astype(BF)
            oacc[...] += dot_nn(pb, x[j, 2])
            dv_ref[j] += dot_tn(pb, x[i, 3])
            qc_acc[...] += dot_nn(dsb, x[j, 1])
            dk_ref[j] += dot_tn(dsb, a_ref[...])
            g0 = gather(ds[:, :H])
            g1 = gather(ds[:, H:])
            d0 = jnp.concatenate([jnp.where(low, g0[:H], u_ref[1, :H]), jnp.where(low, g1[H:], g0[H:])], 0)
            d1 = jnp.concatenate([jnp.where(low, u_ref[1, :H], u_ref[0, :H]), jnp.where(low, g0[H:], u_ref[1, H:])], 0)
            dist = jnp.concatenate([d0, d1], 1).astype(BF)
            u_ref[0] = g0
            u_ref[1] = g1
            qr_acc[...] += dot_nn(dist, rk[i - j])
            drk[i - j] += dot_tn(dist, c_ref[...])
            return 0

        lax.fori_loop(0, i + 1, grads, 0)
        qc = qc_acc[...]
        qr = qr_acc[...]
        duw[0:1] += jnp.sum(qc, axis=0, keepdims=True)
        duw[1:2] += jnp.sum(qr, axis=0, keepdims=True)
        x[i, 0] = oacc[...].astype(BF)
        x[i, 1] = (qc + qr).astype(BF)
        x[i, 2] = dk_ref[i].astype(BF)
        x[i, 3] = dv_ref[i].astype(BF)
        after_tile(i)
        return 0

    lax.fori_loop(0, NT, tile, 0)


UNIT_SCRATCH = [
    pltpu.VMEM((NT, T, T), F32), pltpu.VMEM((NT, T, T), F32), pltpu.VMEM((T, H), F32), pltpu.VMEM((H, H), F32),
    pltpu.VMEM((2, T, H), F32), pltpu.VMEM((NT, T, D), F32), pltpu.VMEM((NT, T, D), F32), pltpu.VMEM((T, D), BF),
    pltpu.VMEM((T, D), BF), pltpu.VMEM((T, D), F32), pltpu.VMEM((T, D), F32), pltpu.VMEM((T, D), F32)]


def kernel(xq, xk, xv, xd, bias_u, bias_w, rel, oq, odq, odk, odv, drk_out, du_out, dw_out,
           rin, drk, pbuf, duw, duw_all, rk, bu, bw,
           in_send, in_recv, in_loc, out_send, out_recv, half_send, half_recv,
           fin_send, fin_recv, hop_send, hop_recv, rel_send, rel_recv, duw_send, duw_recv, rk_sem, *scratch):
    me = lax.axis_index('cp')
    chip = me // 2
    core = me % 2
    ins = (xq, xk, xv, xd)
    outs = (oq, odq, odk, odv)

    def remote(src, dst, ssem, rsem, dev):
        return pltpu.make_async_remote_copy(src_ref=src, dst_ref=dst, send_sem=ssem, recv_sem=rsem,
                                            device_id=(dev,), device_id_type=MESH)

    def spot(arr, dev, n):
        return arr.at[2 * (dev % 2) + n % 2, 3 * (dev // 2) + n // 2]

    def send_in(n, mask):
        dev = jnp.bitwise_xor(me, mask)
        for a in range(4):
            remote(spot(ins[a], dev, n), rin.at[n, me, a], in_send.at[n, mask], in_recv.at[n, mask], dev).start()

    def in_wait(n, mask):
        dev = jnp.bitwise_xor(me, mask)
        return remote(rin.at[n, dev], rin.at[n, dev], in_send.at[n, mask], in_recv.at[n, mask], dev)

    rk_copy = pltpu.make_async_copy(rel.at[pl.ds(3 * chip, 3)], rk, rk_sem)
    rk_copy.start()
    for n in range(NU):
        for a in range(4):
            pltpu.make_async_copy(spot(ins[a], me, n), rin.at[n, me, a], in_loc.at[n]).start()
        for mask in (6, 2, 4, 7, 3, 5, 1):
            send_in(n, mask)

    bu[...] = bias_u[...].astype(F32)
    bw[...] = bias_w[...].astype(F32)
    drk[...] = jnp.zeros_like(drk)
    duw[...] = jnp.zeros_like(duw)
    rk_copy.wait()

    def half_copy(k):
        return remote(drk.at[k, pl.ds(4 * (1 - core), 4)], pbuf.at[k], half_send.at[k], half_recv.at[k],
                      jnp.bitwise_xor(me, 1))

    def part(src_chip, k, lo, size):
        return drk_out.at[3 * src_chip + k, pl.ds(4 * core + lo, size)]

    def fin_copy(k, s):
        mine = part(chip, k, 0, 4)
        return remote(mine, mine, fin_send.at[k, s], fin_recv.at[k, s], jnp.bitwise_xor(me, (1, 2, 4)[s]))

    def fin_arrived(k, s):
        theirs = part(jnp.bitwise_xor(chip, s), k, 0, 4)
        return remote(theirs, theirs, fin_send.at[k, s], fin_recv.at[k, s], jnp.bitwise_xor(me, (1, 2, 4)[s]))

    def hop(k, s):
        piece = part(jnp.bitwise_xor(chip, s), k, 2 * (s - 1), 2)
        return remote(piece, piece, hop_send.at[k, s], hop_recv.at[k, s], jnp.bitwise_xor(me, (1, 4, 2)[s]))

    def hop_arrived(k, s):
        piece = part(jnp.bitwise_xor(chip, 3), k, 2 * (s - 1), 2)
        return remote(piece, piece, hop_send.at[k, s], hop_recv.at[k, s], jnp.bitwise_xor(me, (1, 4, 2)[s]))

    def relay(k, s):
        piece = part(jnp.bitwise_xor(chip, s), k, 0, 4)
        return remote(piece, piece, rel_send.at[k, s], rel_recv.at[k, s], jnp.bitwise_xor(me, 1))

    def relay_arrived(k, s):
        piece = drk_out.at[3 * jnp.bitwise_xor(chip, s) + k, pl.ds(4 * (1 - core), 4)]
        return remote(piece, piece, rel_send.at[k, s], rel_recv.at[k, s], jnp.bitwise_xor(me, 1))

    def pass_on(k):
        for s in (1, 2):
            fin_arrived(k, s).wait_recv()
            hop(k, s).start()
            relay(k, s).start()

    def run_unit(n, _):
        k = n // 2
        pltpu.make_async_copy(rin.at[n, me], rin.at[n, me], in_loc.at[n]).wait()
        for mask in range(1, 8):
            in_wait(n, mask).wait_recv()

        def after_tile(i):
            mask = jnp.bitwise_xor(me, i)

            @pl.when(mask != 0)
            def _():
                for a in range(4):
                    remote(rin.at[n, i, a], spot(outs[a], me, n), out_send.at[n, i], out_recv.at[n, mask], i).start()

            @pl.when(mask == 0)
            def _():
                for a in range(4):
                    spot(outs[a], me, n)[...] = rin[n, i, a]

        head = pl.ds(3 * chip + k, 1)
        unit(rin.at[n], rk.at[k], bu[head], bw[head], drk.at[k], duw.at[k], scratch, after_tile)

        @pl.when(n % 2 == 1)
        def _():
            copy = half_copy(k)
            copy.start()
            copy.wait()
            part(chip, k, 0, 4)[...] = drk[k, pl.ds(4 * core, 4)] + pbuf[k]
            for s in range(3):
                fin_copy(k, s).start()

        @pl.when((n % 2 == 1) & (n > 1))
        def _():
            pass_on(k - 1)
        return 0

    lax.fori_loop(0, NU, run_unit, 0)

    def duw_copy(mask, arrived):
        dev = jnp.bitwise_xor(me, mask)
        return remote(duw, duw_all.at[dev if arrived else me], duw_send.at[mask], duw_recv.at[mask], dev)

    for mask in range(1, 8):
        duw_copy(mask, False).start()
    duw_all[me] = duw[...]

    pass_on(2)
    for k in range(3):
        hop_arrived(k, 1).wait_recv()
        hop_arrived(k, 2).wait_recv()
        relay(k, 3).start()

    for mask in range(1, 8):
        duw_copy(mask, False).wait_send()
        duw_copy(mask, True).wait_recv()
    for h in range(12):
        both = duw_all[2 * (h // 3), h % 3] + duw_all[2 * (h // 3) + 1, h % 3]
        du_out[h:h + 1] = both[0:1]
        dw_out[h:h + 1] = both[1:2]

    def finish(n, _):
        for mask in range(1, 8):
            dev = jnp.bitwise_xor(me, mask)
            in_wait(n, mask).wait_send()
            remote(rin.at[n, dev], rin.at[n, dev], out_send.at[n, dev], out_recv.at[n, mask], dev).wait()
        return 0

    lax.fori_loop(0, NU, finish, 0)
    for k in range(3):
        fin_copy(k, 0).wait_send()
        theirs = drk_out.at[3 * chip + k, pl.ds(4 * (1 - core), 4)]
        remote(theirs, theirs, fin_send.at[k, 0], fin_recv.at[k, 0], jnp.bitwise_xor(me, 1)).wait_recv()
        for s in (1, 2):
            fin_copy(k, s).wait_send()
            hop(k, s).wait_send()
        for s in (1, 2, 3):
            relay(k, s).wait_send()
            relay_arrived(k, s).wait_recv()


def exchange_attend(xq, xk, xv, xd, bias_u, bias_w, rel):
    any_spec = pl.BlockSpec(memory_space=pl.ANY)
    vmem_spec = pl.BlockSpec(memory_space=pltpu.VMEM)
    dma = pltpu.SemaphoreType.DMA
    act = pltpu.VMEM((4, 12, T, D), BF)
    bias = pltpu.VMEM((12, D), F32)
    return pl.pallas_call(
        kernel,
        out_shape=(act, act, act, act, pltpu.VMEM((12, NT, T, D), F32), bias, bias),
        in_specs=[any_spec] * 4 + [vmem_spec] * 2 + [any_spec],
        out_specs=(vmem_spec,) * 7,
        scratch_shapes=[
            pltpu.VMEM((NU, 8, 4, T, D), BF), pltpu.VMEM((3, NT, T, D), F32),
            pltpu.VMEM((3, 4, T, D), F32), pltpu.VMEM((3, 8, D), F32), pltpu.VMEM((8, 3, 8, D), F32),
            pltpu.VMEM((3, NT, T, D), BF), pltpu.VMEM((12, D), F32), pltpu.VMEM((12, D), F32),
            dma((NU, 8)), dma((NU, 8)), dma((NU,)), dma((NU, 8)), dma((NU, 8)), dma((3,)), dma((3,)),
            dma((3, 3)), dma((3, 3)), dma((3, 3)), dma((3, 3)), dma((3, 4)), dma((3, 4)), dma((8,)), dma((8,)), dma(())]
        + UNIT_SCRATCH,
        compiler_params=pltpu.CompilerParams(has_side_effects=True, vmem_limit_bytes=VMEM_LIMIT),
    )(xq, xk, xv, xd, bias_u, bias_w, rel)


def solution(mesh):
    seq_spec = P(None, 'cp', None, None)

    def local(query, key_in, value, bias_u, bias_w, rel_k, d_out):
        def by_head(arr):
            return arr.transpose(0, 2, 1, 3)

        rel = rel_k.transpose(1, 0, 2).reshape(12, NT, T, D)
        res = exchange_attend(by_head(query), by_head(key_in), by_head(value), by_head(d_out), bias_u, bias_w, rel)
        d_rel = res[4].reshape(12, NT * T, D).transpose(1, 0, 2)
        return tuple(by_head(arr) for arr in res[:4]) + (res[5], res[6], d_rel)

    return jax.shard_map(local, mesh=mesh,
                         in_specs=(seq_spec, seq_spec, seq_spec, P(), P(), P(), seq_spec),
                         out_specs=(seq_spec, seq_spec, seq_spec, seq_spec, P(), P(), P()),
                         check_vma=False)
```

```python
import jax
import jax.numpy as jnp
from jax import lax
from jax.experimental import pallas as pl
from jax.experimental.pallas import tpu as pltpu
from jax.sharding import PartitionSpec as P

T = 256
D = 128
H = 128
NT = 8
NU = 6
VMEM_LIMIT = 36 * 1024 * 1024
F32 = jnp.float32
BF = jnp.bfloat16
MESH = pl.DeviceIdType.MESH


def dot_nt(lhs, rhs):
    return lax.dot_general(lhs, rhs, (((1,), (1,)), ((), ())), preferred_element_type=F32)


def dot_nn(lhs, rhs):
    return lax.dot_general(lhs, rhs, (((1,), (0,)), ((), ())), preferred_element_type=F32)


def unit(x, rk, rkr, u, w, drk, duw, scratch, after_tile):
    (s_ref, dp_ref, r_ref, mx_ref, l_ref, d_ref, u_ref, dk_ref, dv_ref, a_ref, c_ref, t_ref,
     oacc, qc_acc, qr_acc) = scratch
    nt = NT
    scale = D ** -0.5
    c2 = scale * 1.4426950408889634
    low = lax.broadcasted_iota(jnp.int32, (H, H), 1) <= lax.broadcasted_iota(jnp.int32, (H, H), 0)
    idx = (lax.broadcasted_iota(jnp.int32, (T, H), 0) - lax.broadcasted_iota(jnp.int32, (T, H), 1)) & (H - 1)

    def gather(t):
        return jnp.take_along_axis(t, idx, axis=1, mode="promise_in_bounds")
    dk_ref[...] = jnp.zeros_like(dk_ref)
    dv_ref[...] = jnp.zeros_like(dv_ref)


    def prep(i, sl):
        q = x[i, 0].astype(F32)
        a_ref[sl] = (q + u).astype(BF)
        c_ref[sl] = (q + w).astype(BF)
        mx_ref[...] = jnp.full((T, H), -jnp.inf, F32)
        r_ref[...] = jnp.full((2, T, H), -jnp.inf, F32)


    def logits(i, sl, n):
        j = i - n
        by = dot_nt(c_ref[sl], rkr[n])
        sc = dot_nt(a_ref[sl], x[j, 1])
        dp_ref[sl, j] = dot_nt(x[i, 3], x[j, 2])
        r0 = pltpu.roll(by[:, :H], 1, 1, stride=1, stride_axis=0)
        r1 = pltpu.roll(by[:, H:], 1, 1, stride=1, stride_axis=0)
        lo = sc[:, :H] + jnp.concatenate([jnp.where(low, r1[:H], r_ref[0, :H]), jnp.where(low, r0[H:], r1[H:])], 0)
        hi = sc[:, H:] + jnp.concatenate([jnp.where(low, r_ref[0, :H], r_ref[1, :H]), jnp.where(low, r1[H:], r_ref[0, H:])], 0)
        r_ref[0] = r0
        r_ref[1] = r1
        s_ref[sl, j, :, :H] = lo
        s_ref[sl, j, :, H:] = hi
        mx_ref[...] = jnp.maximum(mx_ref[...], jnp.maximum(lo, hi))


    def softmax(i, sl):
        m = jnp.max(mx_ref[...], axis=1, keepdims=True)
        l_ref[...] = jnp.zeros_like(l_ref)
        d_ref[...] = jnp.zeros_like(d_ref)
        def body(j, _):
            p = jnp.exp2((s_ref[sl, j] - m) * c2)
            s_ref[sl, j] = p
            pd = p * dp_ref[sl, j]
            l_ref[...] += p[:, :H] + p[:, H:]
            d_ref[...] += pd[:, :H] + pd[:, H:]
            return 0
        lax.fori_loop(0, i + 1, body, 0)
        inv = 1.0 / jnp.sum(l_ref[...], axis=1, keepdims=True)
        rd = jnp.sum(d_ref[...], axis=1, keepdims=True) * inv
        return inv, rd


    def grads(i, sl, j, inv, rd):
        pn = s_ref[sl, j] * inv
        pb = pn.astype(BF)
        ds = pn * (dp_ref[sl, j] - rd) * scale
        dsb = ds.astype(BF)
        oacc[...] += dot_nn(pb, x[j, 2])
        dv_ref[j] += dot_nn(t_ref[0], pb)
        qc_acc[...] += dot_nn(dsb, x[j, 1])
        dk_ref[j] += dot_nn(t_ref[1], dsb)
        g0 = gather(ds[:, :H])
        g1 = gather(ds[:, H:])
        d0 = jnp.concatenate([jnp.where(low, g0[:H], u_ref[1, :H]), jnp.where(low, g1[H:], g0[H:])], 0)
        d1 = jnp.concatenate([jnp.where(low, u_ref[1, :H], u_ref[0, :H]), jnp.where(low, g0[H:], u_ref[1, H:])], 0)
        dist = jnp.concatenate([d0, d1], 1).astype(BF)
        u_ref[0] = g0
        u_ref[1] = g1
        qr_acc[...] += dot_nn(dist, rk[i - j])
        drk[i - j] += dot_nn(t_ref[2], dist)

    prep(nt - 1, (nt - 1) % 2)

    def first(n, _):
        logits(nt - 1, (nt - 1) % 2, n)
        return 0
    lax.fori_loop(0, nt, first, 0)


    def tile(ii, _):
        i = nt - 1 - ii
        sl = i % 2
        inv, rd = softmax(i, sl)
        nxt = jnp.maximum(i - 1, 0)
        t_ref[0] = x[i, 3].T
        t_ref[1] = a_ref[sl].T
        t_ref[2] = c_ref[sl].T
        oacc[...] = jnp.zeros_like(oacc)
        qc_acc[...] = jnp.zeros_like(qc_acc)
        qr_acc[...] = jnp.zeros_like(qr_acc)
        u_ref[...] = jnp.zeros_like(u_ref)
        prep(nxt, 1 - sl)
        def both(n, _):
            grads(i, sl, n, inv, rd)
            logits(nxt, 1 - sl, n)
            return 0
        lax.fori_loop(0, i, both, 0)
        grads(i, sl, i, inv, rd)
        qc = qc_acc[...]
        qr = qr_acc[...]
        duw[0:1] += jnp.sum(qc, axis=0, keepdims=True)
        duw[1:2] += jnp.sum(qr, axis=0, keepdims=True)
        x[i, 0] = oacc[...].astype(BF)
        x[i, 1] = (qc + qr).astype(BF)
        x[i, 2] = dk_ref[i].T.astype(BF)
        x[i, 3] = dv_ref[i].T.astype(BF)
        after_tile(i)
        return 0
    lax.fori_loop(0, nt, tile, 0)


UNIT_SCRATCH = [
    pltpu.VMEM((2, NT, T, T), F32), pltpu.VMEM((2, NT, T, T), F32), pltpu.VMEM((2, T, H), F32), pltpu.VMEM((T, H), F32),
    pltpu.VMEM((T, H), F32), pltpu.VMEM((T, H), F32), pltpu.VMEM((2, T, H), F32), pltpu.VMEM((NT, D, T), F32),
    pltpu.VMEM((NT, D, T), F32), pltpu.VMEM((2, T, D), BF), pltpu.VMEM((2, T, D), BF), pltpu.VMEM((3, D, T), BF),
    pltpu.VMEM((T, D), F32), pltpu.VMEM((T, D), F32), pltpu.VMEM((T, D), F32)]


def kernel(xq, xk, xv, xd, bias_u, bias_w, rel, oq, odq, odk, odv, drk_out, du_out, dw_out,
           rin, drk, pbuf, duw, duw_all, rk, rkr, bu, bw,
           in_send, in_recv, in_loc, out_send, out_recv, half_send, half_recv,
           fin_send, fin_recv, hop_send, hop_recv, rel_send, rel_recv, duw_send, duw_recv, rk_sem, *scratch):
    me = lax.axis_index('cp')
    chip = me // 2
    core = me % 2
    ins = (xq, xk, xv, xd)
    outs = (oq, odq, odk, odv)

    def remote(src, dst, ssem, rsem, dev):
        return pltpu.make_async_remote_copy(src_ref=src, dst_ref=dst, send_sem=ssem, recv_sem=rsem,
                                            device_id=(dev,), device_id_type=MESH)

    def spot(arr, dev, n):
        return arr.at[2 * (dev % 2) + n % 2, 3 * (dev // 2) + n // 2]

    def send_in(n, mask):
        dev = jnp.bitwise_xor(me, mask)
        for a in range(4):
            remote(spot(ins[a], dev, n), rin.at[n, me, a], in_send.at[n, mask], in_recv.at[n, mask], dev).start()

    def in_wait(n, mask):
        dev = jnp.bitwise_xor(me, mask)
        return remote(rin.at[n, dev], rin.at[n, dev], in_send.at[n, mask], in_recv.at[n, mask], dev)

    rk_copy = pltpu.make_async_copy(rel.at[pl.ds(3 * chip, 3)], rk, rk_sem)
    rk_copy.start()
    for n in range(NU):
        for a in range(4):
            pltpu.make_async_copy(spot(ins[a], me, n), rin.at[n, me, a], in_loc.at[n]).start()
        for mask in (6, 2, 4, 7, 3, 5, 1):
            send_in(n, mask)

    bu[...] = bias_u[...].astype(F32)
    bw[...] = bias_w[...].astype(F32)
    drk[...] = jnp.zeros_like(drk)
    duw[...] = jnp.zeros_like(duw)
    rk_copy.wait()
    flip = (lax.broadcasted_iota(jnp.int32, (T, T), 0) + lax.broadcasted_iota(jnp.int32, (T, T), 1) == T - 1).astype(BF)
    for k in range(3):
        for n in range(NT):
            rkr[k, n] = dot_nn(flip, rk[k, n]).astype(BF)

    def half_copy(k):
        return remote(drk.at[k, pl.ds(4 * (1 - core), 4)], pbuf.at[k], half_send.at[k], half_recv.at[k],
                      jnp.bitwise_xor(me, 1))

    def part(src_chip, k, lo, size):
        return drk_out.at[3 * src_chip + k, pl.ds(4 * core + lo, size)]

    def fin_copy(k, s):
        mine = part(chip, k, 0, 4)
        return remote(mine, mine, fin_send.at[k, s], fin_recv.at[k, s], jnp.bitwise_xor(me, (1, 2, 4)[s]))

    def fin_arrived(k, s):
        theirs = part(jnp.bitwise_xor(chip, s), k, 0, 4)
        return remote(theirs, theirs, fin_send.at[k, s], fin_recv.at[k, s], jnp.bitwise_xor(me, (1, 2, 4)[s]))

    def hop(k, s):
        piece = part(jnp.bitwise_xor(chip, s), k, 2 * (s - 1), 2)
        return remote(piece, piece, hop_send.at[k, s], hop_recv.at[k, s], jnp.bitwise_xor(me, (1, 4, 2)[s]))

    def hop_arrived(k, s):
        piece = part(jnp.bitwise_xor(chip, 3), k, 2 * (s - 1), 2)
        return remote(piece, piece, hop_send.at[k, s], hop_recv.at[k, s], jnp.bitwise_xor(me, (1, 4, 2)[s]))

    def relay(k, s):
        piece = part(jnp.bitwise_xor(chip, s), k, 0, 4)
        return remote(piece, piece, rel_send.at[k, s], rel_recv.at[k, s], jnp.bitwise_xor(me, 1))

    def relay_arrived(k, s):
        piece = drk_out.at[3 * jnp.bitwise_xor(chip, s) + k, pl.ds(4 * (1 - core), 4)]
        return remote(piece, piece, rel_send.at[k, s], rel_recv.at[k, s], jnp.bitwise_xor(me, 1))

    def pass_on(k):
        for s in (1, 2):
            fin_arrived(k, s).wait_recv()
            hop(k, s).start()
            relay(k, s).start()

    def run_unit(n, _):
        k = n // 2
        pltpu.make_async_copy(rin.at[n, me], rin.at[n, me], in_loc.at[n]).wait()
        for mask in range(1, 8):
            in_wait(n, mask).wait_recv()

        def after_tile(i):
            mask = jnp.bitwise_xor(me, i)

            @pl.when(mask != 0)
            def _():
                for a in range(4):
                    remote(rin.at[n, i, a], spot(outs[a], me, n), out_send.at[n, i], out_recv.at[n, mask], i).start()

            @pl.when(mask == 0)
            def _():
                for a in range(4):
                    spot(outs[a], me, n)[...] = rin[n, i, a]

        head = pl.ds(3 * chip + k, 1)
        unit(rin.at[n], rk.at[k], rkr.at[k], bu[head], bw[head], drk.at[k], duw.at[k], scratch, after_tile)

        @pl.when(n % 2 == 1)
        def _():
            copy = half_copy(k)
            copy.start()
            copy.wait()
            for r in range(4):
                part(chip, k, r, 1)[0] = (drk[k, 4 * core + r] + pbuf[k, r]).T
            for s in range(3):
                fin_copy(k, s).start()

        @pl.when((n % 2 == 1) & (n > 1))
        def _():
            pass_on(k - 1)
        return 0

    lax.fori_loop(0, NU, run_unit, 0)

    def duw_copy(mask, arrived):
        dev = jnp.bitwise_xor(me, mask)
        return remote(duw, duw_all.at[dev if arrived else me], duw_send.at[mask], duw_recv.at[mask], dev)

    for mask in range(1, 8):
        duw_copy(mask, False).start()
    duw_all[me] = duw[...]

    pass_on(2)
    for k in range(3):
        hop_arrived(k, 1).wait_recv()
        hop_arrived(k, 2).wait_recv()
        relay(k, 3).start()

    for mask in range(1, 8):
        duw_copy(mask, False).wait_send()
        duw_copy(mask, True).wait_recv()
    for h in range(12):
        both = duw_all[2 * (h // 3), h % 3] + duw_all[2 * (h // 3) + 1, h % 3]
        du_out[h:h + 1] = both[0:1]
        dw_out[h:h + 1] = both[1:2]

    def finish(n, _):
        for mask in range(1, 8):
            dev = jnp.bitwise_xor(me, mask)
            in_wait(n, mask).wait_send()
            remote(rin.at[n, dev], rin.at[n, dev], out_send.at[n, dev], out_recv.at[n, mask], dev).wait()
        return 0

    lax.fori_loop(0, NU, finish, 0)
    for k in range(3):
        fin_copy(k, 0).wait_send()
        theirs = drk_out.at[3 * chip + k, pl.ds(4 * (1 - core), 4)]
        remote(theirs, theirs, fin_send.at[k, 0], fin_recv.at[k, 0], jnp.bitwise_xor(me, 1)).wait_recv()
        for s in (1, 2):
            fin_copy(k, s).wait_send()
            hop(k, s).wait_send()
        for s in (1, 2, 3):
            relay(k, s).wait_send()
            relay_arrived(k, s).wait_recv()


def exchange_attend(xq, xk, xv, xd, bias_u, bias_w, rel):
    any_spec = pl.BlockSpec(memory_space=pl.ANY)
    vmem_spec = pl.BlockSpec(memory_space=pltpu.VMEM)
    dma = pltpu.SemaphoreType.DMA
    act = pltpu.VMEM((4, 12, T, D), BF)
    bias = pltpu.VMEM((12, D), F32)
    return pl.pallas_call(
        kernel,
        out_shape=(act, act, act, act, pltpu.VMEM((12, NT, T, D), F32), bias, bias),
        in_specs=[any_spec] * 4 + [vmem_spec] * 2 + [any_spec],
        out_specs=(vmem_spec,) * 7,
        scratch_shapes=[
            pltpu.VMEM((NU, 8, 4, T, D), BF), pltpu.VMEM((3, NT, D, T), F32),
            pltpu.VMEM((3, 4, D, T), F32), pltpu.VMEM((3, 8, D), F32), pltpu.VMEM((8, 3, 8, D), F32),
            pltpu.VMEM((3, NT, T, D), BF), pltpu.VMEM((3, NT, T, D), BF), pltpu.VMEM((12, D), F32), pltpu.VMEM((12, D), F32),
            dma((NU, 8)), dma((NU, 8)), dma((NU,)), dma((NU, 8)), dma((NU, 8)), dma((3,)), dma((3,)),
            dma((3, 3)), dma((3, 3)), dma((3, 3)), dma((3, 3)), dma((3, 4)), dma((3, 4)), dma((8,)), dma((8,)), dma(())]
        + UNIT_SCRATCH,
        compiler_params=pltpu.CompilerParams(has_side_effects=True, vmem_limit_bytes=VMEM_LIMIT),
    )(xq, xk, xv, xd, bias_u, bias_w, rel)


def solution(mesh):
    seq_spec = P(None, 'cp', None, None)

    def local(query, key_in, value, bias_u, bias_w, rel_k, d_out):
        def by_head(arr):
            return arr.transpose(0, 2, 1, 3)

        rel = rel_k.transpose(1, 0, 2).reshape(12, NT, T, D)
        res = exchange_attend(by_head(query), by_head(key_in), by_head(value), by_head(d_out), bias_u, bias_w, rel)
        d_rel = res[4].reshape(12, NT * T, D).transpose(1, 0, 2)
        return tuple(by_head(arr) for arr in res[:4]) + (res[5], res[6], d_rel)

    return jax.shard_map(local, mesh=mesh,
                         in_specs=(seq_spec, seq_spec, seq_spec, P(), P(), P(), seq_spec),
                         out_specs=(seq_spec, seq_spec, seq_spec, seq_spec, P(), P(), P()),
                         check_vma=False)
```

```python
import jax
import jax.numpy as jnp
from jax import lax
from jax.experimental import pallas as pl
from jax.experimental.pallas import tpu as pltpu
from jax.sharding import PartitionSpec as P

T = 256
D = 128
H = 128
NT = 8
NU = 6
VMEM_LIMIT = 36 * 1024 * 1024
F32 = jnp.float32
BF = jnp.bfloat16
MESH = pl.DeviceIdType.MESH


def dot_nt(lhs, rhs):
    return lax.dot_general(lhs, rhs, (((1,), (1,)), ((), ())), preferred_element_type=F32)


def dot_nn(lhs, rhs):
    return lax.dot_general(lhs, rhs, (((1,), (0,)), ((), ())), preferred_element_type=F32)


def unit(x, rk, rkr, u, w, drk, duw, scratch, after_tile):
    (s_ref, dp_ref, r_ref, mx_ref, l_ref, d_ref, u_ref, dk_ref, dv_ref, a_ref, c_ref, t_ref,
     oacc, qc_acc, qr_acc) = scratch
    nt = NT
    scale = D ** -0.5
    c2 = scale * 1.4426950408889634
    low = lax.broadcasted_iota(jnp.int32, (H, H), 1) <= lax.broadcasted_iota(jnp.int32, (H, H), 0)
    idx = (lax.broadcasted_iota(jnp.int32, (T, H), 0) - lax.broadcasted_iota(jnp.int32, (T, H), 1)) & (H - 1)

    def gather(t):
        return jnp.take_along_axis(t, idx, axis=1, mode="promise_in_bounds")
    dk_ref[...] = jnp.zeros_like(dk_ref)
    dv_ref[...] = jnp.zeros_like(dv_ref)


    def prep(i, sl):
        q = x[i, 0].astype(F32)
        a_ref[sl] = (q + u).astype(BF)
        c_ref[sl] = (q + w).astype(BF)
        mx_ref[...] = jnp.full((T, H), -jnp.inf, F32)
        r_ref[...] = jnp.full((2, T, H), -jnp.inf, F32)


    def logits(i, sl, n):
        j = i - n
        by = dot_nt(c_ref[sl], rkr[n])
        sc = dot_nt(a_ref[sl], x[j, 1])
        dp_ref[sl, j] = dot_nt(x[i, 3], x[j, 2])
        r0 = pltpu.roll(by[:, :H], 1, 1, stride=1, stride_axis=0)
        r1 = pltpu.roll(by[:, H:], 1, 1, stride=1, stride_axis=0)
        lo = sc[:, :H] + jnp.concatenate([jnp.where(low, r1[:H], r_ref[0, :H]), jnp.where(low, r0[H:], r1[H:])], 0)
        hi = sc[:, H:] + jnp.concatenate([jnp.where(low, r_ref[0, :H], r_ref[1, :H]), jnp.where(low, r1[H:], r_ref[0, H:])], 0)
        r_ref[0] = r0
        r_ref[1] = r1
        s_ref[sl, j, :, :H] = lo
        s_ref[sl, j, :, H:] = hi
        mx_ref[...] = jnp.maximum(mx_ref[...], jnp.maximum(lo, hi))


    def softmax(i, sl):
        m = jnp.max(mx_ref[...], axis=1, keepdims=True)
        l_ref[...] = jnp.zeros_like(l_ref)
        d_ref[...] = jnp.zeros_like(d_ref)
        def body(j, _):
            p = jnp.exp2((s_ref[sl, j] - m) * c2)
            s_ref[sl, j] = p
            pd = p * dp_ref[sl, j]
            l_ref[...] += p[:, :H] + p[:, H:]
            d_ref[...] += pd[:, :H] + pd[:, H:]
            return 0
        lax.fori_loop(0, i + 1, body, 0)
        inv = 1.0 / jnp.sum(l_ref[...], axis=1, keepdims=True)
        rd = jnp.sum(d_ref[...], axis=1, keepdims=True) * inv
        return inv, rd


    def grads(i, sl, j, inv, rd):
        pn = s_ref[sl, j] * inv
        pb = pn.astype(BF)
        ds = pn * (dp_ref[sl, j] - rd) * scale
        dsb = ds.astype(BF)
        oacc[...] += dot_nn(pb, x[j, 2])
        dv_ref[j] += dot_nn(t_ref[0], pb)
        qc_acc[...] += dot_nn(dsb, x[j, 1])
        dk_ref[j] += dot_nn(t_ref[1], dsb)
        g0 = gather(ds[:, :H])
        g1 = gather(ds[:, H:])
        d0 = jnp.concatenate([jnp.where(low, g0[:H], u_ref[1, :H]), jnp.where(low, g1[H:], g0[H:])], 0)
        d1 = jnp.concatenate([jnp.where(low, u_ref[1, :H], u_ref[0, :H]), jnp.where(low, g0[H:], u_ref[1, H:])], 0)
        dist = jnp.concatenate([d0, d1], 1).astype(BF)
        u_ref[0] = g0
        u_ref[1] = g1
        qr_acc[...] += dot_nn(dist, rk[i - j])
        drk[i - j] += dot_nn(t_ref[2], dist)

    prep(nt - 1, (nt - 1) % 2)

    def first(n, _):
        logits(nt - 1, (nt - 1) % 2, n)
        return 0
    lax.fori_loop(0, nt, first, 0)


    def tile(ii, _):
        i = nt - 1 - ii
        sl = i % 2
        inv, rd = softmax(i, sl)
        nxt = jnp.maximum(i - 1, 0)
        t_ref[0] = x[i, 3].T
        t_ref[1] = a_ref[sl].T
        t_ref[2] = c_ref[sl].T
        oacc[...] = jnp.zeros_like(oacc)
        qc_acc[...] = jnp.zeros_like(qc_acc)
        qr_acc[...] = jnp.zeros_like(qr_acc)
        u_ref[...] = jnp.zeros_like(u_ref)
        prep(nxt, 1 - sl)
        def both(n, _):
            grads(i, sl, n, inv, rd)
            logits(nxt, 1 - sl, n)
            return 0
        lax.fori_loop(0, i, both, 0)
        grads(i, sl, i, inv, rd)
        qc = qc_acc[...]
        qr = qr_acc[...]
        duw[0:1] += jnp.sum(qc, axis=0, keepdims=True)
        duw[1:2] += jnp.sum(qr, axis=0, keepdims=True)
        x[i, 0] = oacc[...].astype(BF)
        x[i, 1] = (qc + qr).astype(BF)
        x[i, 2] = dk_ref[i].T.astype(BF)
        x[i, 3] = dv_ref[i].T.astype(BF)
        after_tile(i)
        return 0
    lax.fori_loop(0, nt, tile, 0)


UNIT_SCRATCH = [
    pltpu.VMEM((2, NT, T, T), F32), pltpu.VMEM((2, NT, T, T), F32), pltpu.VMEM((2, T, H), F32), pltpu.VMEM((T, H), F32),
    pltpu.VMEM((T, H), F32), pltpu.VMEM((T, H), F32), pltpu.VMEM((2, T, H), F32), pltpu.VMEM((NT, D, T), F32),
    pltpu.VMEM((NT, D, T), F32), pltpu.VMEM((2, T, D), BF), pltpu.VMEM((2, T, D), BF), pltpu.VMEM((3, D, T), BF),
    pltpu.VMEM((T, D), F32), pltpu.VMEM((T, D), F32), pltpu.VMEM((T, D), F32)]


def kernel(xq, xk, xv, xd, bias_u, bias_w, rel, oq, odq, odk, odv, drk_out, du_out, dw_out,
           rin, drk, pbuf, duw, duw_all, rk, rkr, bu, bw,
           in_send, in_recv, in_loc, out_send, out_recv, half_send, half_recv,
           fin_send, fin_recv, hop_send, hop_recv, rel_send, rel_recv, duw_send, duw_recv, rk_sem, *scratch):
    me = lax.axis_index('cp')
    chip = me // 2
    core = me % 2
    ins = (xq, xk, xv, xd)
    outs = (oq, odq, odk, odv)

    def remote(src, dst, ssem, rsem, dev):
        return pltpu.make_async_remote_copy(src_ref=src, dst_ref=dst, send_sem=ssem, recv_sem=rsem,
                                            device_id=(dev,), device_id_type=MESH)

    def spot(arr, dev, n):
        return arr.at[2 * (dev % 2) + n % 2, 3 * (dev // 2) + n // 2]

    def send_in(n, mask):
        dev = jnp.bitwise_xor(me, mask)
        for a in range(4):
            remote(spot(ins[a], dev, n), rin.at[n, me, a], in_send.at[n, mask], in_recv.at[n, mask], dev).start()

    def in_wait(n, mask):
        dev = jnp.bitwise_xor(me, mask)
        return remote(rin.at[n, dev], rin.at[n, dev], in_send.at[n, mask], in_recv.at[n, mask], dev)

    rk_copy = pltpu.make_async_copy(rel.at[pl.ds(3 * chip, 3)], rk, rk_sem)
    rk_copy.start()
    for n in range(NU):
        for a in range(4):
            pltpu.make_async_copy(spot(ins[a], me, n), rin.at[n, me, a], in_loc.at[n]).start()
        for mask in (6, 2, 4, 7, 3, 5, 1):
            send_in(n, mask)

    bu[...] = bias_u[...].astype(F32)
    bw[...] = bias_w[...].astype(F32)
    drk[...] = jnp.zeros_like(drk)
    duw[...] = jnp.zeros_like(duw)
    rk_copy.wait()
    flip = (lax.broadcasted_iota(jnp.int32, (T, T), 0) + lax.broadcasted_iota(jnp.int32, (T, T), 1) == T - 1).astype(BF)
    for k in range(3):
        for n in range(NT):
            rkr[k, n] = dot_nn(flip, rk[k, n]).astype(BF)

    def half_copy(k):
        return remote(drk.at[k, pl.ds(4 * (1 - core), 4)], pbuf.at[k], half_send.at[k], half_recv.at[k],
                      jnp.bitwise_xor(me, 1))

    def part(src_chip, k, lo, size):
        return drk_out.at[3 * src_chip + k, pl.ds(4 * core + lo, size)]

    def fin_copy(k, s):
        mine = part(chip, k, 0, 4)
        return remote(mine, mine, fin_send.at[k, s], fin_recv.at[k, s], jnp.bitwise_xor(me, (1, 2, 4)[s]))

    def fin_arrived(k, s):
        theirs = part(jnp.bitwise_xor(chip, s), k, 0, 4)
        return remote(theirs, theirs, fin_send.at[k, s], fin_recv.at[k, s], jnp.bitwise_xor(me, (1, 2, 4)[s]))

    def hop(k, s):
        piece = part(jnp.bitwise_xor(chip, s), k, 2 * (s - 1), 2)
        return remote(piece, piece, hop_send.at[k, s], hop_recv.at[k, s], jnp.bitwise_xor(me, (1, 4, 2)[s]))

    def hop_arrived(k, s):
        piece = part(jnp.bitwise_xor(chip, 3), k, 2 * (s - 1), 2)
        return remote(piece, piece, hop_send.at[k, s], hop_recv.at[k, s], jnp.bitwise_xor(me, (1, 4, 2)[s]))

    def relay(k, s):
        piece = part(jnp.bitwise_xor(chip, s), k, 0, 4)
        return remote(piece, piece, rel_send.at[k, s], rel_recv.at[k, s], jnp.bitwise_xor(me, 1))

    def relay_arrived(k, s):
        piece = drk_out.at[3 * jnp.bitwise_xor(chip, s) + k, pl.ds(4 * (1 - core), 4)]
        return remote(piece, piece, rel_send.at[k, s], rel_recv.at[k, s], jnp.bitwise_xor(me, 1))

    def pass_on(k):
        for s in (1, 2):
            fin_arrived(k, s).wait_recv()
            hop(k, s).start()
            relay(k, s).start()

    def run_unit(n, _):
        k = n // 2
        pltpu.make_async_copy(rin.at[n, me], rin.at[n, me], in_loc.at[n]).wait()
        for mask in range(1, 8):
            in_wait(n, mask).wait_recv()

        def after_tile(i):
            mask = jnp.bitwise_xor(me, i)

            @pl.when(mask != 0)
            def _():
                for a in range(4):
                    remote(rin.at[n, i, a], spot(outs[a], me, n), out_send.at[n, i], out_recv.at[n, mask], i).start()

            @pl.when(mask == 0)
            def _():
                for a in range(4):
                    spot(outs[a], me, n)[...] = rin[n, i, a]

        head = pl.ds(3 * chip + k, 1)
        unit(rin.at[n], rk.at[k], rkr.at[k], bu[head], bw[head], drk.at[k], duw.at[k], scratch, after_tile)

        @pl.when(n % 2 == 1)
        def _():
            copy = half_copy(k)
            copy.start()
            copy.wait()
            for r in range(4):
                part(chip, k, r, 1)[0] = (drk[k, 4 * core + r] + pbuf[k, r]).T
            for s in range(3):
                fin_copy(k, s).start()

        @pl.when((n % 2 == 1) & (n > 1))
        def _():
            pass_on(k - 1)
        return 0

    lax.fori_loop(0, NU, run_unit, 0)

    def duw_copy(mask, arrived):
        dev = jnp.bitwise_xor(me, mask)
        return remote(duw, duw_all.at[dev if arrived else me], duw_send.at[mask], duw_recv.at[mask], dev)

    for mask in range(1, 8):
        duw_copy(mask, False).start()
    duw_all[me] = duw[...]

    pass_on(2)
    for k in range(3):
        hop_arrived(k, 1).wait_recv()
        hop_arrived(k, 2).wait_recv()
        relay(k, 3).start()

    for mask in range(1, 8):
        duw_copy(mask, False).wait_send()
        duw_copy(mask, True).wait_recv()
    for h in range(12):
        both = duw_all[2 * (h // 3), h % 3] + duw_all[2 * (h // 3) + 1, h % 3]
        du_out[h:h + 1] = both[0:1]
        dw_out[h:h + 1] = both[1:2]

    def finish(n, _):
        for mask in range(1, 8):
            dev = jnp.bitwise_xor(me, mask)
            in_wait(n, mask).wait_send()
            remote(rin.at[n, dev], rin.at[n, dev], out_send.at[n, dev], out_recv.at[n, mask], dev).wait()
        return 0

    lax.fori_loop(0, NU, finish, 0)
    for k in range(3):
        fin_copy(k, 0).wait_send()
        theirs = drk_out.at[3 * chip + k, pl.ds(4 * (1 - core), 4)]
        remote(theirs, theirs, fin_send.at[k, 0], fin_recv.at[k, 0], jnp.bitwise_xor(me, 1)).wait_recv()
        for s in (1, 2):
            fin_copy(k, s).wait_send()
            hop(k, s).wait_send()
        for s in (1, 2, 3):
            relay(k, s).wait_send()
            relay_arrived(k, s).wait_recv()


def exchange_attend(xq, xk, xv, xd, bias_u, bias_w, rel):
    any_spec = pl.BlockSpec(memory_space=pl.ANY)
    vmem_spec = pl.BlockSpec(memory_space=pltpu.VMEM)
    dma = pltpu.SemaphoreType.DMA
    act = pltpu.VMEM((4, 12, T, D), BF)
    bias = pltpu.VMEM((12, D), F32)
    return pl.pallas_call(
        kernel,
        out_shape=(act, act, act, act, pltpu.VMEM((12, NT, T, D), F32), bias, bias),
        in_specs=[any_spec] * 4 + [vmem_spec] * 2 + [any_spec],
        out_specs=(vmem_spec,) * 7,
        scratch_shapes=[
            pltpu.VMEM((NU, 8, 4, T, D), BF), pltpu.VMEM((3, NT, D, T), F32),
            pltpu.VMEM((3, 4, D, T), F32), pltpu.VMEM((3, 8, D), F32), pltpu.VMEM((8, 3, 8, D), F32),
            pltpu.VMEM((3, NT, T, D), BF), pltpu.VMEM((3, NT, T, D), BF), pltpu.VMEM((12, D), F32), pltpu.VMEM((12, D), F32),
            dma((NU, 8)), dma((NU, 8)), dma((NU,)), dma((NU, 8)), dma((NU, 8)), dma((3,)), dma((3,)),
            dma((3, 3)), dma((3, 3)), dma((3, 3)), dma((3, 3)), dma((3, 4)), dma((3, 4)), dma((8,)), dma((8,)), dma(())]
        + UNIT_SCRATCH,
        compiler_params=pltpu.CompilerParams(has_side_effects=True, vmem_limit_bytes=VMEM_LIMIT),
    )(xq, xk, xv, xd, bias_u, bias_w, rel)


def write_kernel(*refs):
    half = len(refs) // 2
    sem = refs[-1]
    copies = [pltpu.make_async_copy(refs[n], refs[half + n], sem.at[n]) for n in range(half)]
    for copy in copies:
        copy.start()
    for copy in copies:
        copy.wait()


def write_out(arrs):
    return pl.pallas_call(
        write_kernel,
        out_shape=tuple(jax.ShapeDtypeStruct(arr.shape, arr.dtype) for arr in arrs),
        in_specs=[pl.BlockSpec(memory_space=pltpu.VMEM)] * len(arrs),
        out_specs=(pl.BlockSpec(memory_space=pl.ANY),) * len(arrs),
        scratch_shapes=[pltpu.SemaphoreType.DMA((len(arrs),))],
        compiler_params=pltpu.CompilerParams(vmem_limit_bytes=1024 * 1024),
    )(*[pltpu.with_memory_space_constraint(arr, pltpu.VMEM) for arr in arrs])


def solution(mesh):
    seq_spec = P(None, 'cp', None, None)

    def local(query, key_in, value, bias_u, bias_w, rel_k, d_out):
        def by_head(arr):
            return arr.transpose(0, 2, 1, 3)

        rel = rel_k.transpose(1, 0, 2).reshape(12, NT, T, D)
        res = exchange_attend(by_head(query), by_head(key_in), by_head(value), by_head(d_out), bias_u, bias_w, rel)
        res = write_out(res)
        d_rel = res[4].reshape(12, NT * T, D).transpose(1, 0, 2)
        return tuple(by_head(arr) for arr in res[:4]) + (res[5], res[6], d_rel)

    return jax.shard_map(local, mesh=mesh,
                         in_specs=(seq_spec, seq_spec, seq_spec, P(), P(), P(), seq_spec),
                         out_specs=(seq_spec, seq_spec, seq_spec, seq_spec, P(), P(), P()),
                         check_vma=False)
```

```python
import jax
import jax.numpy as jnp
from jax import lax
from jax.experimental import pallas as pl
from jax.experimental.pallas import tpu as pltpu
from jax.sharding import PartitionSpec as P

T = 256
D = 128
H = 128
NT = 8
NU = 6
EARLY = 6
HOLD = 4
VMEM_LIMIT = 38 * 1024 * 1024
F32 = jnp.float32
BF = jnp.bfloat16
SCALE = D ** -0.5
C2 = SCALE * 1.4426950408889634
MESH = pl.DeviceIdType.MESH


def dot_nt(lhs, rhs):
    return lax.dot_general(lhs, rhs, (((1,), (1,)), ((), ())), preferred_element_type=F32)


def row_max(arr):
    return jnp.max(arr, axis=1, keepdims=True)


def row_sum(arr):
    return jnp.sum(arr, axis=1, keepdims=True)


def dot_nn(lhs, rhs):
    return lax.dot_general(lhs, rhs, (((1,), (0,)), ((), ())), preferred_element_type=F32)


def unit(x, rk, rkr, u, w, drk, duw, scratch, after_softmax, after_tile):
    (s_ref, dp_ref, r_ref, mx_ref, l_ref, d_ref, u_ref, dk_ref, dv_ref, a_ref, c_ref, t_ref,
     oacc, qc_acc, qr_acc) = scratch
    nt = NT
    low = lower_mask()
    gather = gather_fn()
    dk_ref[:] = jnp.zeros_like(dk_ref)
    dv_ref[:] = jnp.zeros_like(dv_ref)


    def prep(i, sl):
        q = x[i, 0].astype(F32)
        a_ref[sl] = (q + u).astype(BF)
        c_ref[sl] = (q + w).astype(BF)
        mx_ref[:] = jnp.full((T, H), -jnp.inf, F32)
        r_ref[:] = jnp.full((2, T, H), -jnp.inf, F32)


    def logits(i, sl, n):
        j = i - n
        by = dot_nt(c_ref[sl], rkr[n])
        sc = dot_nt(a_ref[sl], x[j, 1])
        dp_ref[sl, j] = dot_nt(x[i, 3], x[j, 2])
        r0 = pltpu.roll(by[:, :H], 1, 1, stride=1, stride_axis=0)
        r1 = pltpu.roll(by[:, H:], 1, 1, stride=1, stride_axis=0)
        sc += shifted(low, r1, r0, r_ref[1], r_ref[0])
        r_ref[0] = r0
        r_ref[1] = r1
        s_ref[sl, j] = sc
        mx_ref[:] = jnp.maximum(mx_ref[:], jnp.maximum(sc[:, :H], sc[:, H:]))


    def softmax(i, sl):
        m = row_max(mx_ref[:])
        l_ref[:] = jnp.zeros_like(l_ref)
        d_ref[:] = jnp.zeros_like(d_ref)
        def body(j, _):
            p = jnp.exp2((s_ref[sl, j] - m) * C2)
            s_ref[sl, j] = p
            pd = p * dp_ref[sl, j]
            l_ref[:] += p[:, :H] + p[:, H:]
            d_ref[:] += pd[:, :H] + pd[:, H:]
            return 0
        lax.fori_loop(0, i + 1, body, 0)
        inv = 1.0 / row_sum(l_ref[:])
        rd = row_sum(d_ref[:]) * inv
        after_softmax(i, m, inv, rd)
        return inv, rd


    def grads(i, sl, j, inv, rd):
        pn = s_ref[sl, j] * inv
        pb = pn.astype(BF)
        ds = pn * (dp_ref[sl, j] - rd) * SCALE
        dsb = ds.astype(BF)
        oacc[:] += dot_nn(pb, x[j, 2])
        dv_ref[j] += dot_nn(t_ref[0], pb)
        qc_acc[:] += dot_nn(dsb, x[j, 1])
        dk_ref[j] += dot_nn(t_ref[1], dsb)
        g0 = gather(ds[:, :H])
        g1 = gather(ds[:, H:])
        dist = shifted(low, g0, g1, u_ref[0], u_ref[1]).astype(BF)
        u_ref[0] = g0
        u_ref[1] = g1
        qr_acc[:] += dot_nn(dist, rk[i - j])
        drk[i - j] += dot_nn(t_ref[2], dist)

    prep(nt - 1, (nt - 1) % 2)

    def first(n, _):
        logits(nt - 1, (nt - 1) % 2, n)
        return 0
    lax.fori_loop(0, nt, first, 0)


    def tile(ii, _):
        i = nt - 1 - ii
        sl = i % 2
        inv, rd = softmax(i, sl)
        nxt = jnp.maximum(i - 1, 0)
        t_ref[0] = x[i, 3].T
        t_ref[1] = a_ref[sl].T
        t_ref[2] = c_ref[sl].T
        oacc[:] = jnp.zeros_like(oacc)
        qc_acc[:] = jnp.zeros_like(qc_acc)
        qr_acc[:] = jnp.zeros_like(qr_acc)
        u_ref[:] = jnp.zeros_like(u_ref)
        prep(nxt, 1 - sl)
        def both(n, _):
            grads(i, sl, n, inv, rd)
            logits(nxt, 1 - sl, n)
            return 0
        lax.fori_loop(0, i, both, 0)
        grads(i, sl, i, inv, rd)
        qc = qc_acc[:]
        qr = qr_acc[:]
        duw[0:1] += jnp.sum(qc, axis=0, keepdims=True)
        duw[1:2] += jnp.sum(qr, axis=0, keepdims=True)
        x[i, 0] = oacc[:].astype(BF)
        x[i, 1] = (qc + qr).astype(BF)
        x[i, 2] = dk_ref[i].T.astype(BF)
        x[i, 3] = dv_ref[i].T.astype(BF)
        after_tile(i)
        return 0
    lax.fori_loop(0, nt, tile, 0)


def gather_fn():
    idx = (lax.broadcasted_iota(jnp.int32, (T, H), 0) - lax.broadcasted_iota(jnp.int32, (T, H), 1)) & (H - 1)
    return lambda arr: jnp.take_along_axis(arr, idx, axis=1, mode="promise_in_bounds")


def lower_mask():
    return lax.broadcasted_iota(jnp.int32, (H, H), 1) <= lax.broadcasted_iota(jnp.int32, (H, H), 0)


def shifted(low, n0, n1, p0, p1):
    lo = jnp.concatenate([jnp.where(low, n0[:H], p1[:H]), jnp.where(low, n1[H:], n0[H:])], 0)
    hi = jnp.concatenate([jnp.where(low, p1[:H], p0[:H]), jnp.where(low, n0[H:], p1[H:])], 0)
    return jnp.concatenate([lo, hi], 1)


def block_scores(q, key, rk, u, w, gather, low):
    qf = jnp.concatenate([q[0].astype(F32), q[1].astype(F32)], 0)
    a = (qf + u).astype(BF)
    c = (qf + w).astype(BF)
    by0 = dot_nt(c, rk[0])
    by1 = dot_nt(c[T:], rk[1])
    s0 = dot_nt(a, key[0])
    s11 = dot_nt(a[T:], key[1])
    g00, g01 = gather(by0[:T, :H]), gather(by0[:T, H:])
    g10, g11 = gather(by0[T:, :H]), gather(by0[T:, H:])
    h10, h11 = gather(by1[:, :H]), gather(by1[:, H:])
    none = jnp.full((T, H), -jnp.inf, F32)
    s00 = s0[:T] + shifted(low, g00, g01, none, none)
    s11 = s11 + shifted(low, g10, g11, none, none)
    s10 = s0[T:] + shifted(low, h10, h11, g10, g11)
    return a, c, s00, s10, s11


def row_block(q, d_out, key, val, rk, u, w, outs, d_qs):
    low = lower_mask()
    gather = gather_fn()
    a, c, s00, s10, s11 = block_scores(q, key, rk, u, w, gather, low)
    dob = jnp.concatenate([d_out[0], d_out[1]], 0)
    dp0 = dot_nt(dob, val[0])
    dp11 = dot_nt(d_out[1], val[1])
    m0 = row_max(s00)
    m1 = row_max(jnp.maximum(s10, s11))
    p00 = jnp.exp2((s00 - m0) * C2)
    p10 = jnp.exp2((s10 - m1) * C2)
    p11 = jnp.exp2((s11 - m1) * C2)
    i0 = 1.0 / row_sum(p00)
    i1 = 1.0 / row_sum(p10 + p11)
    r0 = row_sum(p00 * dp0[:T]) * i0
    r1 = row_sum(p10 * dp0[T:] + p11 * dp11) * i1
    p00 *= i0
    p10 *= i1
    p11 *= i1
    d00 = p00 * (dp0[:T] - r0) * SCALE
    d10 = p10 * (dp0[T:] - r1) * SCALE
    d11 = p11 * (dp11 - r1) * SCALE
    o = dot_nn(jnp.concatenate([p00, p10], 0).astype(BF), val[0])
    o1 = o[T:] + dot_nn(p11.astype(BF), val[1])
    outs[0][:] = o[:T].astype(BF)
    outs[1][:] = o1.astype(BF)
    dq = dot_nn(jnp.concatenate([d00, d10], 0).astype(BF), key[0])
    dq1 = dot_nn(d11.astype(BF), key[1])
    zero = jnp.zeros((T, H), F32)
    a0, a1 = gather(d00[:, :H]), gather(d00[:, H:])
    b0, b1 = gather(d10[:, :H]), gather(d10[:, H:])
    e0, e1 = gather(d11[:, :H]), gather(d11[:, H:])
    t00 = shifted(low, a0, a1, zero, zero)
    t11 = shifted(low, b0, b1, zero, zero)
    t10 = shifted(low, e0, e1, b0, b1)
    dr = dot_nn(jnp.concatenate([t00, t10], 0).astype(BF), rk[0])
    dr1 = dot_nn(t11.astype(BF), rk[1])
    d_qs[0][:] = (dq[:T] + dr[:T]).astype(BF)
    d_qs[1][:] = (dq[T:] + dq1 + dr[T:] + dr1).astype(BF)


def col_block(q, d_out, key, val, rk, stats, u, w, d_ks, d_vs):
    low = lower_mask()
    gather = gather_fn()
    a, c, s00, s10, s11 = block_scores(q, key, rk, u, w, gather, low)
    dob = jnp.concatenate([d_out[0], d_out[1]], 0)
    dp0 = dot_nt(dob, val[0])
    dp11 = dot_nt(d_out[1], val[1])
    z = jnp.zeros((H - 8, T), F32)
    t0 = jnp.concatenate([stats[0], z], 0).T
    t1 = jnp.concatenate([stats[1], z], 0).T
    p00 = jnp.exp2((s00 - t0[:, 0:1]) * C2) * t0[:, 1:2]
    p10 = jnp.exp2((s10 - t1[:, 0:1]) * C2) * t1[:, 1:2]
    p11 = jnp.exp2((s11 - t1[:, 0:1]) * C2) * t1[:, 1:2]
    d00 = p00 * (dp0[:T] - t0[:, 2:3]) * SCALE
    d10 = p10 * (dp0[T:] - t1[:, 2:3]) * SCALE
    d11 = p11 * (dp11 - t1[:, 2:3]) * SCALE
    at = a.T
    dot = dob.T
    dv0 = dot_nn(dot, jnp.concatenate([p00, p10], 0).astype(BF))
    dk0 = dot_nn(at, jnp.concatenate([d00, d10], 0).astype(BF))
    dv1 = dot_nn(dot[:, T:], p11.astype(BF))
    dk1 = dot_nn(at[:, T:], d11.astype(BF))
    d_ks[0][:] = dk0.T.astype(BF)
    d_vs[0][:] = dv0.T.astype(BF)
    d_ks[1][:] = dk1.T.astype(BF)
    d_vs[1][:] = dv1.T.astype(BF)


UNIT_SCRATCH = [
    pltpu.VMEM((2, NT, T, T), F32), pltpu.VMEM((2, NT, T, T), F32), pltpu.VMEM((2, T, H), F32), pltpu.VMEM((T, H), F32),
    pltpu.VMEM((T, H), F32), pltpu.VMEM((T, H), F32), pltpu.VMEM((2, T, H), F32), pltpu.VMEM((NT, D, T), F32),
    pltpu.VMEM((NT, D, T), F32), pltpu.VMEM((2, T, D), BF), pltpu.VMEM((2, T, D), BF), pltpu.VMEM((3, D, T), BF),
    pltpu.VMEM((T, D), F32), pltpu.VMEM((T, D), F32), pltpu.VMEM((T, D), F32)]


def kernel(xq, xk, xv, xd, bias_u, bias_w, rel, oq, odq, odk, odv, drk_out, du_out, dw_out, lx,
           rin, drk, pbuf, duw, duw_all, rk, rkr, bu, bw, lblk, lrk, lres, st_out, st_in,
           in_send, in_recv, in_loc, out_send, out_recv, half_send, half_recv,
           fin_send, fin_recv, hop_send, hop_recv, rel_send, rel_recv, duw_send, duw_recv, rk_sem, px_send, px_recv,
           st_send, st_recv, l_sem, lr_send, lr_recv, *scratch):
    me = lax.axis_index('cp')
    chip = me // 2
    core = me % 2
    ins = (xq, xk, xv, xd)
    outs = (oq, odq, odk, odv)

    def remote(src, dst, ssem, rsem, dev):
        return pltpu.make_async_remote_copy(src_ref=src, dst_ref=dst, send_sem=ssem, recv_sem=rsem,
                                            device_id=(dev,), device_id_type=MESH)

    def spot(arr, dev, n):
        return arr.at[2 * (dev % 2) + n % 2, 3 * (dev // 2) + n // 2]

    def send_in(n, mask):
        dev = jnp.bitwise_xor(me, mask)
        for a in range(4):
            remote(spot(ins[a], dev, n), rin.at[n, me, a], in_send.at[n, mask], in_recv.at[n, mask], dev).start()

    def in_wait(n, mask):
        dev = jnp.bitwise_xor(me, mask)
        return remote(rin.at[n, dev], rin.at[n, dev], in_send.at[n, mask], in_recv.at[n, mask], dev)

    rk_copy = pltpu.make_async_copy(rel.at[pl.ds(3 * chip, 3)], rk, rk_sem)
    rk_copy.start()
    rows_here = chip == 0
    cols_here = chip == 3
    partner = jnp.bitwise_xor(me, 1)

    def pair_copies(low_end):
        heads = pl.ds(3 if low_end else 0, 9)
        return [remote(ins[a].at[pl.ds(2 * (1 - core), 2), heads], lx.at[a, :, heads], px_send.at[a], px_recv.at[a], partner)
                for a in range(4)]

    def pair(act):
        for low_end in (True, False):
            @pl.when(rows_here if low_end else cols_here)
            def _():
                for copy in pair_copies(low_end):
                    getattr(copy, act)()

    for n in range(NU):
        for a in range(4):
            pltpu.make_async_copy(spot(ins[a], me, n), rin.at[n, me, a], in_loc.at[n]).start()
        for mask in (6, 2, 4, 7, 3, 5, 1):
            send_in(n, mask)
        if n == 0:
            pair("start")

    bu[:] = bias_u[:].astype(F32)
    bw[:] = bias_w[:].astype(F32)
    drk[:] = jnp.zeros_like(drk)
    duw[:] = jnp.zeros_like(duw)
    rk_copy.wait()
    flip = (lax.broadcasted_iota(jnp.int32, (T, T), 0) + lax.broadcasted_iota(jnp.int32, (T, T), 1) == T - 1).astype(BF)
    for k in range(3):
        for n in range(NT):
            rkr[k, n] = dot_nn(flip, rk[k, n]).astype(BF)

    def half_copy(k):
        return remote(drk.at[k, pl.ds(4 * (1 - core), 4)], pbuf.at[k], half_send.at[k], half_recv.at[k],
                      jnp.bitwise_xor(me, 1))

    def part(src_chip, k, lo, size):
        return drk_out.at[3 * src_chip + k, pl.ds(4 * core + lo, size)]

    def fin_copy(k, s):
        mine = part(chip, k, 0, 4)
        return remote(mine, mine, fin_send.at[k, s], fin_recv.at[k, s], jnp.bitwise_xor(me, (1, 2, 4)[s]))

    def fin_arrived(k, s):
        theirs = part(jnp.bitwise_xor(chip, s), k, 0, 4)
        return remote(theirs, theirs, fin_send.at[k, s], fin_recv.at[k, s], jnp.bitwise_xor(me, (1, 2, 4)[s]))

    outer = (chip == 0) | (chip == 3)
    hop_from = jnp.where(outer, 2, 1)
    hop_to = jnp.bitwise_xor(me, jnp.where(outer, 2, 4))
    hop_via = jnp.bitwise_xor(me, jnp.where(outer, 4, 2))

    def hop(k):
        piece = part(jnp.bitwise_xor(chip, hop_from), k, 0, 4)
        return remote(piece, piece, hop_send.at[k], hop_recv.at[k], hop_to)

    def hop_arrived(k):
        piece = part(jnp.bitwise_xor(chip, 3), k, 0, 4)
        return remote(piece, piece, hop_send.at[k], hop_recv.at[k], hop_via)

    def relay(k, s):
        piece = part(jnp.bitwise_xor(chip, s), k, 0, 4)
        return remote(piece, piece, rel_send.at[k, s], rel_recv.at[k, s], jnp.bitwise_xor(me, 1))

    def relay_arrived(k, s):
        piece = drk_out.at[3 * jnp.bitwise_xor(chip, s) + k, pl.ds(4 * (1 - core), 4)]
        return remote(piece, piece, rel_send.at[k, s], rel_recv.at[k, s], jnp.bitwise_xor(me, 1))

    def pass_on(k):
        for first in (True, False):
            for s in (1, 2):
                @pl.when((hop_from == s) == first)
                def _():
                    fin_arrived(k, s).wait_recv()
                    if first:
                        hop(k).start()
                    relay(k, s).start()

    def made_there(a, dev, owner):
        if a < 2:
            return (dev < 2) & (owner != 0)
        return (dev >= 6) & (owner != 3)

    def stat_copy(n):
        return remote(st_out.at[n], st_in.at[chip, n], st_send.at[n], st_recv.at[chip, n], 6 + core)

    def after_softmax(n, i, m, inv, rd):
        @pl.when((i >= 6) & (chip != 3))
        def _():
            lane = lax.broadcasted_iota(jnp.int32, (T, H), 1)
            table = jnp.where(lane == 0, m, jnp.where(lane == 1, inv, jnp.where(lane == 2, rd, 0.0)))
            st_out[n, i - 6] = table.T[:8]

        @pl.when((i == 6) & (chip != 3))
        def _():
            stat_copy(n).start()

    def local_pair(x):
        owner = jnp.where(rows_here, 1, 0) + x % 3
        return owner, 2 * core + (x // 3) % 2, 3 * owner + x // 6

    def local_loads(x, sl):
        _, bat, head = local_pair(x)
        copies = [pltpu.make_async_copy(rel.at[head, pl.ds(0, 2)], lrk.at[sl], l_sem.at[sl, 0])]
        for a in range(4):
            copies.append(pltpu.make_async_copy(ins[a].at[bat, head], lblk.at[sl, core, a], l_sem.at[sl, 1 + a]))
            copies.append(pltpu.make_async_copy(lx.at[a, bat % 2, head], lblk.at[sl, 1 - core, a], l_sem.at[sl, 5 + a]))
        return copies

    def local_sends(x, sl, low_end):
        _, bat, head = local_pair(x)
        dsts = outs[:2] if low_end else outs[2:]
        return [remote(lres.at[sl, 1 - core, a], dsts[a].at[bat, head], lr_send.at[sl, a], lr_recv, partner)
                for a in range(2)]

    def local_work(lo, hi, low_end):
        for copy in local_loads(lo, lo % 2):
            copy.start()

        def one(x, _):
            sl = x % 2

            @pl.when(x + 1 < hi)
            def _():
                for copy in local_loads(x + 1, 1 - sl):
                    copy.start()

            for copy in local_loads(x, sl):
                copy.wait()
            owner, bat, head = local_pair(x)
            u = bu[pl.ds(head, 1)]
            w = bw[pl.ds(head, 1)]

            @pl.when(x > 1)
            def _():
                for copy in local_sends(x, sl, low_end):
                    copy.wait_send()

            q, key, val, do = [[lblk[sl, r, a] for r in range(2)] for a in range(4)]
            res = [[lres.at[sl, r, a] for r in range(2)] for a in range(2)]
            if low_end:
                row_block(q, do, key, val, lrk[sl], u, w, *res)
            else:
                n = x // 3
                piece = st_in.at[owner, n]
                remote(piece, piece, st_send.at[n], st_recv.at[owner, n], 2 * owner + core).wait_recv()
                col_block(q, do, key, val, lrk[sl], piece, u, w, *res)
            for copy in local_sends(x, sl, low_end):
                copy.start()
            dsts = outs[:2] if low_end else outs[2:]
            for a in range(2):
                dsts[a][bat, head] = lres[sl, core, a]
            return 0

        lax.fori_loop(lo, hi, one, 0)

    @pl.when(rows_here)
    def _():
        for copy in pair_copies(True):
            copy.wait_recv()
        local_work(0, EARLY, True)

    def send_tile(n, i):
        mask = jnp.bitwise_xor(me, i)

        def send(a):
            remote(rin.at[n, i, a], spot(outs[a], me, n), out_send.at[n, i, a // 2], out_recv.at[n, mask, a // 2],
                       i).start()

        for first in (0, 2):
            @pl.when((mask != 0) & ~made_there(first, i, chip))
            def _():
                send(first)
                send(first + 1)

        @pl.when(mask == 0)
        def _():
            for a in range(4):
                spot(outs[a], me, n)[:] = rin[n, i, a]

    def run_unit(n, _):
        k = n // 2
        pltpu.make_async_copy(rin.at[n, me], rin.at[n, me], in_loc.at[n]).wait()
        for mask in range(1, 8):
            in_wait(n, mask).wait_recv()

        def after_tile(i):
            @pl.when(n < HOLD)
            def _():
                send_tile(n, i)

        head = pl.ds(3 * chip + k, 1)
        unit(rin.at[n], rk.at[k], rkr.at[k], bu[head], bw[head], drk.at[k], duw.at[k], scratch,
             lambda i, m, inv, rd: after_softmax(n, i, m, inv, rd), after_tile)

        @pl.when(n % 2 == 1)
        def _():
            copy = half_copy(k)
            copy.start()
            copy.wait()
            for r in range(4):
                part(chip, k, r, 1)[0] = (drk[k, 4 * core + r] + pbuf[k, r]).T
            for s in range(3):
                fin_copy(k, s).start()

        return 0

    lax.fori_loop(0, NU, run_unit, 0)

    def late_sends(x, _):
        send_tile(HOLD + x // NT, NT - 1 - x % NT)
        return 0

    lax.fori_loop(0, (NU - HOLD) * NT, late_sends, 0)
    pass_on(0)
    pass_on(1)

    def duw_copy(mask, arrived):
        dev = jnp.bitwise_xor(me, mask)
        return remote(duw, duw_all.at[dev if arrived else me], duw_send.at[mask], duw_recv.at[mask], dev)

    for mask in range(1, 8):
        duw_copy(mask, False).start()
    duw_all[me] = duw[:]

    @pl.when(rows_here)
    def _():
        local_work(EARLY, 18, True)

    @pl.when(cols_here)
    def _():
        for copy in pair_copies(False):
            copy.wait_recv()
        local_work(0, 18, False)

    pass_on(2)
    for k in range(3):
        hop_arrived(k).wait_recv()
        relay(k, 3).start()

    for mask in range(1, 8):
        duw_copy(mask, False).wait_send()
        duw_copy(mask, True).wait_recv()
    for h in range(12):
        both = duw_all[2 * (h // 3), h % 3] + duw_all[2 * (h // 3) + 1, h % 3]
        du_out[h:h + 1] = both[0:1]
        dw_out[h:h + 1] = both[1:2]

    def finish(n, _):
        for mask in range(1, 8):
            dev = jnp.bitwise_xor(me, mask)
            in_wait(n, mask).wait_send()
            for first in (0, 2):
                both = rin.at[n, dev, pl.ds(first, 2)]
                copy = remote(both, both, out_send.at[n, dev, first // 2], out_recv.at[n, mask, first // 2], dev)

                @pl.when(~made_there(first, dev, chip))
                def _():
                    copy.wait_send()

                @pl.when(~made_there(first, me, dev // 2))
                def _():
                    copy.wait_recv()

        @pl.when(chip != 3)
        def _():
            stat_copy(n).wait_send()
        return 0

    lax.fori_loop(0, NU, finish, 0)
    pair("wait_send")
    for low_end in (True, False):
        @pl.when(rows_here if low_end else cols_here)
        def _():
            for x in (16, 17):
                for copy in local_sends(x, x % 2, low_end):
                    copy.wait_send()
            whole = oq.at[pl.ds(0, 3)]
            remote(whole, whole, lr_send.at[0, 0], lr_recv, partner).wait_recv()

    for k in range(3):
        fin_copy(k, 0).wait_send()
        theirs = drk_out.at[3 * chip + k, pl.ds(4 * (1 - core), 4)]
        remote(theirs, theirs, fin_send.at[k, 0], fin_recv.at[k, 0], jnp.bitwise_xor(me, 1)).wait_recv()
        for s in (1, 2):
            fin_copy(k, s).wait_send()
        hop(k).wait_send()
        for s in (1, 2, 3):
            relay(k, s).wait_send()
            relay_arrived(k, s).wait_recv()


def exchange_attend(xq, xk, xv, xd, bias_u, bias_w, rel):
    any_spec = pl.BlockSpec(memory_space=pl.ANY)
    vmem_spec = pl.BlockSpec(memory_space=pltpu.VMEM)
    dma = pltpu.SemaphoreType.DMA
    act = pltpu.VMEM((4, 12, T, D), BF)
    bias = pltpu.VMEM((12, D), F32)
    return pl.pallas_call(
        kernel,
        out_shape=(act, act, act, act, pltpu.VMEM((12, NT, T, D), F32), bias, bias,
                   jax.ShapeDtypeStruct((4, 2, 12, T, D), BF)),
        in_specs=[any_spec] * 4 + [vmem_spec] * 2 + [any_spec],
        out_specs=(vmem_spec,) * 7 + (any_spec,),
        scratch_shapes=[
            pltpu.VMEM((NU, 8, 4, T, D), BF), pltpu.VMEM((3, NT, D, T), F32),
            pltpu.VMEM((3, 4, D, T), F32), pltpu.VMEM((3, 8, D), F32), pltpu.VMEM((8, 3, 8, D), F32),
            pltpu.VMEM((3, NT, T, D), BF), pltpu.VMEM((3, NT, T, D), BF), pltpu.VMEM((12, D), F32), pltpu.VMEM((12, D), F32),
            pltpu.VMEM((2, 2, 4, T, D), BF), pltpu.VMEM((2, 2, T, D), BF), pltpu.VMEM((2, 2, 2, T, D), BF),
            pltpu.VMEM((NU, 2, 8, T), F32), pltpu.VMEM((3, NU, 2, 8, T), F32),
            dma((NU, 8)), dma((NU, 8)), dma((NU,)), dma((NU, 8, 2)), dma((NU, 8, 2)), dma((3,)), dma((3,)),
            dma((3, 3)), dma((3, 3)), dma((3,)), dma((3,)), dma((3, 4)), dma((3, 4)), dma((8,)), dma((8,)), dma(()), dma((4,)), dma((4,)),
            dma((NU,)), dma((3, NU)), dma((2, 9)), dma((2, 2)), dma(())]
        + UNIT_SCRATCH,
        compiler_params=pltpu.CompilerParams(has_side_effects=True, vmem_limit_bytes=VMEM_LIMIT),
    )(xq, xk, xv, xd, bias_u, bias_w, rel)


def write_kernel(*refs):
    half = len(refs) // 2
    sem = refs[-1]
    copies = [pltpu.make_async_copy(refs[n], refs[half + n], sem.at[n]) for n in range(half)]
    for copy in copies:
        copy.start()
    for copy in copies:
        copy.wait()


def write_out(arrs):
    return pl.pallas_call(
        write_kernel,
        out_shape=tuple(jax.ShapeDtypeStruct(arr.shape, arr.dtype) for arr in arrs),
        in_specs=[pl.BlockSpec(memory_space=pltpu.VMEM)] * len(arrs),
        out_specs=(pl.BlockSpec(memory_space=pl.ANY),) * len(arrs),
        scratch_shapes=[pltpu.SemaphoreType.DMA((len(arrs),))],
        compiler_params=pltpu.CompilerParams(vmem_limit_bytes=1024 * 1024),
    )(*[pltpu.with_memory_space_constraint(arr, pltpu.VMEM) for arr in arrs])


def solution(mesh):
    seq_spec = P(None, 'cp', None, None)

    def local(query, key_in, value, bias_u, bias_w, rel_k, d_out):
        def by_head(arr):
            return arr.transpose(0, 2, 1, 3)

        rel = rel_k.transpose(1, 0, 2).reshape(12, NT, T, D)
        res = exchange_attend(by_head(query), by_head(key_in), by_head(value), by_head(d_out), bias_u, bias_w, rel)
        res = write_out(res[:7])
        d_rel = res[4].reshape(12, NT * T, D).transpose(1, 0, 2)
        return tuple(by_head(arr) for arr in res[:4]) + (res[5], res[6], d_rel)

    return jax.shard_map(local, mesh=mesh,
                         in_specs=(seq_spec, seq_spec, seq_spec, P(), P(), P(), seq_spec),
                         out_specs=(seq_spec, seq_spec, seq_spec, seq_spec, P(), P(), P()),
                         check_vma=False)
```

```python
import jax
import jax.numpy as jnp
from jax import lax
from jax.experimental import pallas as pl
from jax.experimental.pallas import tpu as pltpu
from jax.sharding import PartitionSpec as P

T = 256
D = 128
H = 128
NT = 8
NU = 6
NA = 4
HC = 3
NH = 12
EARLY = 6
AHEAD = 3
VMEM_LIMIT = 39 * 1024 * 1024
F32 = jnp.float32
BF = jnp.bfloat16
SCALE = D ** -0.5
C2 = SCALE * 1.4426950408889634
MESH = pl.DeviceIdType.MESH


def dot_nt(lhs, rhs):
    return lax.dot_general(lhs, rhs, (((1,), (1,)), ((), ())), preferred_element_type=F32)


def row_max(arr):
    return jnp.max(arr, axis=1, keepdims=True)


def row_sum(arr):
    return jnp.sum(arr, axis=1, keepdims=True)


def dot_nn(lhs, rhs):
    return lax.dot_general(lhs, rhs, (((1,), (0,)), ((), ())), preferred_element_type=F32)


def unit(x, rk, rkr, u, w, drk, duw, scratch, after_softmax, after_tile):
    (s_ref, dp_ref, r_ref, mx_ref, l_ref, d_ref, u_ref, dk_ref, dv_ref, a_ref, c_ref, t_ref,
     oacc, qc_acc, qr_acc) = scratch
    nt = NT
    low = lower_mask()
    gather = gather_fn()
    dk_ref[:] = jnp.zeros_like(dk_ref)
    dv_ref[:] = jnp.zeros_like(dv_ref)

    def prep(i, sl):
        q = x[i, 0].astype(F32)
        a_ref[sl] = (q + u).astype(BF)
        c_ref[sl] = (q + w).astype(BF)
        mx_ref[:] = jnp.full((T, H), -jnp.inf, F32)
        r_ref[:] = jnp.full((2, T, H), -jnp.inf, F32)

    def logits(i, sl, n):
        j = i - n
        by = dot_nt(c_ref[sl], rkr[n])
        sc = dot_nt(a_ref[sl], x[j, 2])
        dp_ref[sl, j] = dot_nt(x[i, 1], x[j, 3])
        r0, r1 = [pltpu.roll(half, 1, 1, stride=1, stride_axis=0) for half in (by[:, :H], by[:, H:])]
        sc += shifted(low, r1, r0, r_ref[1], r_ref[0])
        r_ref[0] = r0
        r_ref[1] = r1
        s_ref[sl, j] = sc
        mx_ref[:] = jnp.maximum(mx_ref[:], jnp.maximum(sc[:, :H], sc[:, H:]))

    def softmax(i, sl):
        m = row_max(mx_ref[:])
        l_ref[:] = jnp.zeros_like(l_ref)
        d_ref[:] = jnp.zeros_like(d_ref)

        def body(j, _):
            p = jnp.exp2((s_ref[sl, j] - m) * C2)
            s_ref[sl, j] = p
            pd = p * dp_ref[sl, j]
            l_ref[:] += p[:, :H] + p[:, H:]
            d_ref[:] += pd[:, :H] + pd[:, H:]
            return 0

        lax.fori_loop(0, i + 1, body, 0)
        inv = 1.0 / row_sum(l_ref[:])
        rd = row_sum(d_ref[:]) * inv
        after_softmax(i, m, inv, rd)
        return inv, rd

    def grads(i, sl, j, inv, rd):
        pn = s_ref[sl, j] * inv
        pb = pn.astype(BF)
        ds = pn * (dp_ref[sl, j] - rd) * SCALE
        dsb = ds.astype(BF)
        oacc[:] += dot_nn(pb, x[j, 3])
        dv_ref[j] += dot_nn(t_ref[0], pb)
        qc_acc[:] += dot_nn(dsb, x[j, 2])
        dk_ref[j] += dot_nn(t_ref[1], dsb)
        g0, g1 = gather(ds)
        dist = shifted(low, g0, g1, u_ref[0], u_ref[1]).astype(BF)
        u_ref[0] = g0
        u_ref[1] = g1
        qr_acc[:] += dot_nn(dist, rk[i - j])
        drk[i - j] += dot_nn(t_ref[2], dist)

    prep(nt - 1, (nt - 1) % 2)

    def first(n, _):
        logits(nt - 1, (nt - 1) % 2, n)
        return 0

    lax.fori_loop(0, nt, first, 0)

    def tile(ii, _):
        i = nt - 1 - ii
        sl = i % 2
        inv, rd = softmax(i, sl)
        nxt = jnp.maximum(i - 1, 0)
        t_ref[0] = x[i, 1].T
        t_ref[1] = a_ref[sl].T
        t_ref[2] = c_ref[sl].T
        for acc in (oacc, qc_acc, qr_acc, u_ref):
            acc[:] = jnp.zeros_like(acc)
        prep(nxt, 1 - sl)

        def both(n, _):
            grads(i, sl, n, inv, rd)
            logits(nxt, 1 - sl, n)
            return 0

        lax.fori_loop(0, i, both, 0)
        grads(i, sl, i, inv, rd)
        qc = qc_acc[:]
        qr = qr_acc[:]
        for r, part in enumerate((qc, qr)):
            duw[r:r + 1] += jnp.sum(part, axis=0, keepdims=True)
        for r, res in enumerate((oacc[:], qc + qr, dk_ref[i].T, dv_ref[i].T)):
            x[i, r] = res.astype(BF)
        after_tile(i)
        return 0

    lax.fori_loop(0, nt, tile, 0)


def gather_fn():
    idx = (lax.broadcasted_iota(jnp.int32, (T, H), 0) - lax.broadcasted_iota(jnp.int32, (T, H), 1)) & (H - 1)

    def gather(arr):
        return [jnp.take_along_axis(half, idx, axis=1, mode="promise_in_bounds") for half in (arr[:, :H], arr[:, H:])]

    return gather


def lower_mask():
    return lax.broadcasted_iota(jnp.int32, (H, H), 1) <= lax.broadcasted_iota(jnp.int32, (H, H), 0)


def shifted(low, n0, n1, p0, p1):
    lo = jnp.concatenate([jnp.where(low, n0[:H], p1[:H]), jnp.where(low, n1[H:], n0[H:])], 0)
    hi = jnp.concatenate([jnp.where(low, p1[:H], p0[:H]), jnp.where(low, n0[H:], p1[H:])], 0)
    return jnp.concatenate([lo, hi], 1)


def row_tile(q, d_out, keys, vals, rk, u, w):
    last = len(keys) - 1
    low = lower_mask()
    gather = gather_fn()
    qf = q.astype(F32)
    a = (qf + u).astype(BF)
    c = (qf + w).astype(BF)
    by = [gather(dot_nt(c, rk[n])) for n in range(last + 1)]
    none = [jnp.full((T, H), -jnp.inf, F32)] * 2
    s = [dot_nt(a, key) + shifted(low, *by[last - j], *(by[last - j - 1] if j < last else none)) for j, key in enumerate(keys)]
    top = s[0]
    for other in s[1:]:
        top = jnp.maximum(top, other)
    m = row_max(top)
    p = [jnp.exp2((sj - m) * C2) for sj in s]
    dp = [dot_nt(d_out, val) for val in vals]
    inv = 1.0 / row_sum(sum(p))
    row_dot = row_sum(sum(pj * dj for pj, dj in zip(p, dp))) * inv
    out, d_q, prev = 0.0, 0.0, [jnp.zeros((T, H), F32)] * 2
    for j in range(last + 1):
        pn = p[j] * inv
        ds = pn * (dp[j] - row_dot) * SCALE
        out += dot_nn(pn.astype(BF), vals[j])
        mine = gather(ds)
        dist = shifted(low, *mine, *prev).astype(BF)
        prev = mine
        d_q += dot_nn(ds.astype(BF), keys[j]) + dot_nn(dist, rk[last - j])
    return out.astype(BF), d_q.astype(BF)


def col_tiles(qs, d_outs, keys, vals, rk, stats, u, w):
    low = lower_mask()
    gather = gather_fn()
    none = [jnp.full((T, H), -jnp.inf, F32)] * 2
    d_keys, d_vals = [0.0, 0.0], [0.0, 0.0]
    for i in range(len(qs)):
        qf = qs[i].astype(F32)
        a = (qf + u).astype(BF)
        c = (qf + w).astype(BF)
        by = {n: gather(dot_nt(c, rk[n])) for n in range(max(i - 2, 0), i + 1)}
        cols = jnp.concatenate([stats[i], jnp.zeros((H - 8, T), F32)], 0).T
        m, inv, row_dot = cols[:, 0:1], cols[:, 1:2], cols[:, 2:3]
        at, dot = a.T, d_outs[i].T
        for r in range(min(i + 1, 2)):
            n = i - r
            s = dot_nt(a, keys[r]) + shifted(low, *by[n], *(by[n - 1] if n else none))
            pn = jnp.exp2((s - m) * C2) * inv
            ds = pn * (dot_nt(d_outs[i], vals[r]) - row_dot) * SCALE
            d_vals[r] += dot_nn(dot, pn.astype(BF))
            d_keys[r] += dot_nn(at, ds.astype(BF))
    return [dk.T.astype(BF) for dk in d_keys], [dv.T.astype(BF) for dv in d_vals]


UNIT_SCRATCH = (
    [pltpu.VMEM((2, NT, T, T), F32)] * 2 + [pltpu.VMEM((2, T, H), F32)] + [pltpu.VMEM((T, H), F32)] * 3
    + [pltpu.VMEM((2, T, H), F32)] + [pltpu.VMEM((NT, D, T), F32)] * 2 + [pltpu.VMEM((2, T, D), BF)] * 2
    + [pltpu.VMEM((3, D, T), BF)] + [pltpu.VMEM((T, D), F32)] * 3)


def kernel(xq, xd, xk, xv, bias_u, bias_w, rel, oq, odq, odk, odv, drk_out, du_out, dw_out, lx,
           rin, rl, drk, pbuf, duw, duw_all, rk, rkr, bu, bw, lblk, lrk, lres, st_out, st_in,
           in_send, in_recv, in_loc, rl_recv, fw_send, fw_recv, out_send, out_recv, half_send, half_recv,
           fin_send, fin_recv, hop_send, hop_recv, rel_send, rel_recv, duw_send, duw_recv, rk_sem, px_send, px_recv,
           st_send, st_recv, l_sem, lr_send, lr_recv, *scratch):
    me = lax.axis_index('cp')
    chip = me // 2
    core = me % 2
    last = NA - 1
    partner = jnp.bitwise_xor(me, 1)
    outer = (chip == 0) | (chip == last)
    ins = (xq, xd, xk, xv)
    outs = (oq, odq, odk, odv)
    neighbours = (1, 2, 4)

    def remote(src, dst, ssem, rsem, dev):
        return pltpu.make_async_remote_copy(src_ref=src, dst_ref=dst, send_sem=ssem, recv_sem=rsem,
                                            device_id=(dev,), device_id_type=MESH)

    def spot(arr, dev, n):
        return arr.at[2 * (dev % 2) + n % 2, HC * (dev // 2) + n // 2]

    def send_in(n, mask):
        dev = jnp.bitwise_xor(me, mask)

        def send(first, via):
            for a in (first, first + 1):
                if via:
                    dst, rsem, to = rl.at[n, core, a % 2], rl_recv.at[n], jnp.bitwise_xor(dev, 4)
                else:
                    dst, rsem, to = rin.at[n, me, a], in_recv.at[n, mask], dev
                remote(spot(ins[a], dev, n), dst, in_send.at[n, mask], rsem, to).start()

        for first in (0, 2):
            if mask < NU:
                send(first, False)
            else:
                through = chip == (0 if first else last)
                for via in (True, False):
                    @pl.when(through == via)
                    def _():
                        send(first, via)

    def send_pair(n):
        for mask in (6, 2, 4, 7, 3, 5, 1):
            send_in(n, mask)

    def in_wait(n, mask, size=NA):
        dev = jnp.bitwise_xor(me, mask)
        piece = rin.at[n, dev, pl.ds(0, size)]
        return remote(piece, piece, in_send.at[n, mask], in_recv.at[n, mask], dev)

    def forward(n):
        dst = rin.at[n, pl.ds(2 * jnp.bitwise_xor(chip, 1), 2), pl.ds(2 * (chip % 2), 2)]
        return remote(rl.at[n], dst, fw_send.at[n], fw_recv.at[n], jnp.bitwise_xor(me, 4))

    def pass_forward(n):
        remote(rl.at[n], rl.at[n], fw_send.at[n], rl_recv.at[n], jnp.bitwise_xor(me, 2)).wait_recv()
        forward(n).start()

    def at_chip(act):
        for c, heads in enumerate(((3, 9), (9, 3), (0, 3), (0, 9))):
            @pl.when(chip == c)
            def _():
                act(c, pl.ds(*heads))

    def pair_copies(heads):
        return [remote(ins[a].at[pl.ds(2 * (1 - core), 2), heads], lx.at[a, :, heads], px_send.at[a], px_recv.at[a], partner)
                for a in range(NA)]

    rk_copy = pltpu.make_async_copy(rel.at[pl.ds(HC * chip, HC)], rk, rk_sem)
    rk_copy.start()
    for n in range(NU):
        for a in range(NA):
            pltpu.make_async_copy(spot(ins[a], me, n), rin.at[n, me, a], in_loc.at[n]).start()
        if n < AHEAD:
            send_pair(n)
        if n == 0:
            at_chip(lambda c, heads: [copy.start() for copy in pair_copies(heads)])

    bu[:] = bias_u[:].astype(F32)
    bw[:] = bias_w[:].astype(F32)
    drk[:] = jnp.zeros_like(drk)
    duw[:] = jnp.zeros_like(duw)
    rk_copy.wait()
    flip = (lax.broadcasted_iota(jnp.int32, (T, T), 0) + lax.broadcasted_iota(jnp.int32, (T, T), 1) == T - 1).astype(BF)
    for k in range(HC):
        for n in range(NT):
            rkr[k, n] = dot_nn(flip, rk[k, n]).astype(BF)

    def half_copy(k):
        return remote(drk.at[k, pl.ds(NA * (1 - core), NA)], pbuf.at[k], half_send.at[k], half_recv.at[k], partner)

    def part(src_chip, k, lo, size):
        return drk_out.at[HC * src_chip + k, pl.ds(NA * core + lo, size)]

    def fin_copy(k, s, arrived=False):
        piece = part(jnp.bitwise_xor(chip, s) if arrived else chip, k, 0, NA)
        return remote(piece, piece, fin_send.at[k, s], fin_recv.at[k, s], jnp.bitwise_xor(me, neighbours[s]))

    def hop(k, s, arrived=False):
        piece = part(jnp.bitwise_xor(chip, last if arrived else s), k, 2 * (s - 1), 2)
        return remote(piece, piece, hop_send.at[k, s], hop_recv.at[k, s], jnp.bitwise_xor(me, neighbours[-s]))

    def relay(k, s, arrived=False):
        half = 1 - core if arrived else core
        piece = drk_out.at[HC * jnp.bitwise_xor(chip, s) + k, pl.ds(NA * half, NA)]
        return remote(piece, piece, rel_send.at[k, s], rel_recv.at[k, s], partner)

    def pass_on(k):
        for s in (1, 2):
            fin_copy(k, s, True).wait_recv()
            hop(k, s).start()
            relay(k, s).start()

    def made_there(first, dev, owner):
        there = dev // 2
        if first:
            return ((there == last) & (owner != last)) | ((there == 2) & (owner == 0))
        return ((there == 0) & (owner != 0)) | ((there == 1) & (owner == last))

    def stat_copy(n, whole):
        if whole:
            return remote(st_out.at[n], st_in.at[0, n], st_send.at[n, 1], st_recv.at[0, n], 4 + core)
        piece = pl.ds(2, 2)
        return remote(st_out.at[n, piece], st_in.at[chip, n, piece], st_send.at[n, 0], st_recv.at[chip, n], 6 + core)

    def after_softmax(n, i, m, inv, rd):
        first = jnp.where(chip == 0, 4, 6)

        @pl.when((i >= first) & (chip != last))
        def _():
            lane = lax.broadcasted_iota(jnp.int32, (T, H), 1)
            table = jnp.where(lane == 0, m, jnp.where(lane == 1, inv, jnp.where(lane == 2, rd, 0.0)))
            st_out[n, i - 4] = table.T[:8]

        @pl.when((i == 6) & (chip != last))
        def _():
            stat_copy(n, False).start()

        @pl.when((i == 4) & (chip == 0))
        def _():
            stat_copy(n, True).start()

    def local_pair(x):
        owner = jnp.where(outer, x % HC + jnp.where(chip == 0, 1, 0), jnp.where(chip == 1, last, 0))
        n = jnp.where(outer, x // HC, x)
        return owner, n, 2 * core + n % 2, HC * owner + n // 2

    def local_loads(x, sl):
        _, n, bat, head = local_pair(x)
        copies = [pltpu.make_async_copy(rel.at[head, pl.ds(0, NA)], lrk.at[sl], l_sem.at[sl, 0, 2])]
        for a in range(NA):
            for r, src in enumerate((ins[a].at[bat, head], lx.at[a, n % 2, head])):
                where = core if r == 0 else 1 - core
                copies.append(pltpu.make_async_copy(src, lblk.at[sl, where, a], l_sem.at[sl, a, r]))
        return copies

    def local_sends(x, c):
        sl = x % 2
        _, _, bat, head = local_pair(x)
        dsts = outs[2 * (c // 2):]
        return [remote(lres.at[sl, 1 - core, a], dsts[a].at[bat, head], lr_send.at[sl, a], lr_recv, partner)
                for a in range(2)]

    def local_work(lo, hi, c):
        for copy in local_loads(lo, lo % 2):
            copy.start()

        def one(x, _):
            sl = x % 2

            @pl.when(x + 1 < hi)
            def _():
                for copy in local_loads(x + 1, 1 - sl):
                    copy.start()

            for copy in local_loads(x, sl):
                copy.wait()

            @pl.when(x > 1)
            def _():
                for copy in local_sends(x, c):
                    copy.wait_send()

            owner, n, bat, head = local_pair(x)
            u = bu[pl.ds(head, 1)]
            w = bw[pl.ds(head, 1)]
            q, do, key, val = [[lblk[sl, r, a] for r in range(2)] for a in range(NA)]
            table = lrk[sl]
            if c < 2:
                if c:
                    key = [rl[n, r, 0] for r in range(2)] + key
                    val = [rl[n, r, 1] for r in range(2)] + val
                for r in range(2):
                    upto = len(key) - 1 + r
                    res = row_tile(q[r], do[r], key[:upto], val[:upto], table, u, w)
                    for a in range(2):
                        lres[sl, r, a] = res[a]
            else:
                piece = st_in.at[owner, n]
                if c == last:
                    piece = st_in.at[owner, n, pl.ds(2, 2)]
                else:
                    q = q + [rl[n, r, 0] for r in range(2)]
                    do = do + [rl[n, r, 1] for r in range(2)]
                remote(piece, piece, st_send.at[n, 0], st_recv.at[owner, n], 2 * owner + core).wait_recv()
                for a, res in enumerate(col_tiles(q, do, key, val, table, piece, u, w)):
                    for r in range(2):
                        lres[sl, r, a] = res[r]
            for copy in local_sends(x, c):
                copy.start()
            for a in range(2):
                outs[2 * (c // 2) + a][bat, head] = lres[sl, core, a]
            return 0

        lax.fori_loop(lo, hi, one, 0)

    def local_count(c):
        return NU if c in (1, 2) else NU * HC

    @pl.when(chip == 0)
    def _():
        for copy in pair_copies(pl.ds(3, 9)):
            copy.wait_recv()
        local_work(0, EARLY, 0)

    def send_tile(n, i):
        mask = jnp.bitwise_xor(me, i)
        for first in (0, 2):
            @pl.when((mask != 0) & ~made_there(first, i, chip))
            def _():
                for a in (first, first + 1):
                    remote(rin.at[n, i, a], spot(outs[a], me, n), out_send.at[n, i, first // 2],
                           out_recv.at[n, mask, first // 2], i).start()

        @pl.when(mask == 0)
        def _():
            for a in range(NA):
                spot(outs[a], me, n)[:] = rin[n, i, a]

    def run_unit(n, _):
        k = n // 2

        @pl.when(n + AHEAD < NU)
        def _():
            send_pair(n + AHEAD)

        @pl.when(~outer & (n == 0))
        def _():
            pass_forward(0)

        @pl.when(~outer & (n + 1 < NU))
        def _():
            pass_forward(n + 1)

        pltpu.make_async_copy(rin.at[n, me], rin.at[n, me], in_loc.at[n]).wait()
        for mask in range(1, NT):
            if mask < NU:
                in_wait(n, mask).wait_recv()
            else:
                for split in (True, False):
                    @pl.when(outer == split)
                    def _():
                        in_wait(n, mask, 2 if split else NA).wait_recv()

        @pl.when(outer)
        def _():
            piece = rin.at[n, pl.ds(0, 2), pl.ds(0, 2)]
            remote(piece, piece, fw_send.at[n], fw_recv.at[n], jnp.bitwise_xor(me, 4)).wait_recv()

        head = pl.ds(HC * chip + k, 1)
        unit(rin.at[n], rk.at[k], rkr.at[k], bu[head], bw[head], drk.at[k], duw.at[k], scratch,
             lambda i, m, inv, rd: after_softmax(n, i, m, inv, rd), lambda i: send_tile(n, i))

        @pl.when(n % 2 == 1)
        def _():
            copy = half_copy(k)
            copy.start()
            copy.wait()
            for r in range(NA):
                part(chip, k, r, 1)[0] = (drk[k, NA * core + r] + pbuf[k, r]).T
            for s in range(3):
                fin_copy(k, s).start()

        return 0

    lax.fori_loop(0, NU, run_unit, 0)

    pass_on(0)
    pass_on(1)

    def duw_copy(mask, arrived):
        dev = jnp.bitwise_xor(me, mask)
        return remote(duw, duw_all.at[dev if arrived else me], duw_send.at[mask], duw_recv.at[mask], dev)

    for mask in range(1, NT):
        duw_copy(mask, False).start()
    duw_all[me] = duw[:]

    def late_work(c, heads):
        if c:
            for copy in pair_copies(heads):
                copy.wait_recv()
        local_work(0 if c else EARLY, local_count(c), c)

    at_chip(late_work)
    pass_on(2)
    for k in range(HC):
        for s in (1, 2):
            hop(k, s, True).wait_recv()
        relay(k, last).start()

    for mask in range(1, NT):
        duw_copy(mask, False).wait_send()
        duw_copy(mask, True).wait_recv()
    for h in range(NH):
        both = duw_all[2 * (h // HC), h % HC] + duw_all[2 * (h // HC) + 1, h % HC]
        for r, out in enumerate((du_out, dw_out)):
            out[h:h + 1] = both[r:r + 1]

    def finish(n, _):
        for mask in range(1, NT):
            dev = jnp.bitwise_xor(me, mask)
            in_wait(n, mask).wait_send()
            for first in (0, 2):
                both = rin.at[n, dev, pl.ds(first, 2)]
                copy = remote(both, both, out_send.at[n, dev, first // 2], out_recv.at[n, mask, first // 2], dev)

                @pl.when(~made_there(first, dev, chip))
                def _():
                    copy.wait_send()

                @pl.when(~made_there(first, me, dev // 2))
                def _():
                    copy.wait_recv()

        @pl.when(~outer)
        def _():
            forward(n).wait_send()

        @pl.when(chip != last)
        def _():
            stat_copy(n, False).wait_send()

        @pl.when(chip == 0)
        def _():
            stat_copy(n, True).wait_send()
        return 0

    lax.fori_loop(0, NU, finish, 0)

    def end_local(c, heads):
        for copy in pair_copies(heads):
            copy.wait_send()
        count = local_count(c)
        for x in (count - 2, count - 1):
            for copy in local_sends(x, c):
                copy.wait_send()
        whole = oq.at[pl.ds(0, count // NU)]
        remote(whole, whole, lr_send.at[0, 0], lr_recv, partner).wait_recv()

    at_chip(end_local)
    for k in range(HC):
        fin_copy(k, 0).wait_send()
        theirs = drk_out.at[HC * chip + k, pl.ds(NA * (1 - core), NA)]
        remote(theirs, theirs, fin_send.at[k, 0], fin_recv.at[k, 0], partner).wait_recv()
        for s in (1, 2):
            fin_copy(k, s).wait_send()
            hop(k, s).wait_send()
        for s in (1, 2, last):
            relay(k, s).wait_send()
            relay(k, s, True).wait_recv()


def exchange_attend(xq, xd, xk, xv, bias_u, bias_w, rel):
    any_spec = pl.BlockSpec(memory_space=pl.ANY)
    vmem_spec = pl.BlockSpec(memory_space=pltpu.VMEM)
    dma = pltpu.SemaphoreType.DMA
    act = pltpu.VMEM((NA, NH, T, D), BF)
    bias = pltpu.VMEM((NH, D), F32)
    heads = pltpu.VMEM((HC, NT, T, D), BF)
    per_head = dma((HC, NA))
    per_pair = dma((NU,))
    per_peer = dma((NU, NT))
    per_half = dma((NU, NT, 2))
    return pl.pallas_call(
        kernel,
        out_shape=(act, act, act, act, pltpu.VMEM((NH, NT, T, D), F32), bias, bias,
                   jax.ShapeDtypeStruct((NA, 2, NH, T, D), BF)),
        in_specs=[any_spec] * 4 + [vmem_spec] * 2 + [any_spec],
        out_specs=(vmem_spec,) * 7 + (any_spec,),
        scratch_shapes=[
            pltpu.VMEM((NU, NT, NA, T, D), BF), pltpu.VMEM((NU, 2, 2, T, D), BF), pltpu.VMEM((HC, NT, D, T), F32),
            pltpu.VMEM((HC, NA, D, T), F32), pltpu.VMEM((HC, 8, D), F32), pltpu.VMEM((NT, HC, 8, D), F32),
            heads, heads, bias, bias,
            pltpu.VMEM((2, 2, NA, T, D), BF), pltpu.VMEM((2, NA, T, D), BF), pltpu.VMEM((2, 2, 2, T, D), BF),
            pltpu.VMEM((NU, NA, 8, T), F32), pltpu.VMEM((HC, NU, NA, 8, T), F32),
            per_peer, per_peer, per_pair, per_pair, per_pair, per_pair, per_half, per_half, dma((HC,)), dma((HC,)),
            per_head, per_head, per_head, per_head, per_head, per_head, dma((NT,)), dma((NT,)), dma(()), dma((NA,)),
            dma((NA,)), dma((NU, 2)), dma((HC, NU)), dma((2, NA, HC)), dma((2, 2)), dma(())]
        + UNIT_SCRATCH,
        compiler_params=pltpu.CompilerParams(has_side_effects=True, vmem_limit_bytes=VMEM_LIMIT),
    )(xq, xd, xk, xv, bias_u, bias_w, rel)


def write_kernel(*refs):
    half = len(refs) // 2
    sem = refs[-1]
    copies = [pltpu.make_async_copy(refs[n], refs[half + n], sem.at[n]) for n in range(half)]
    for copy in copies:
        copy.start()
    for copy in copies:
        copy.wait()


def write_out(arrs):
    return pl.pallas_call(
        write_kernel,
        out_shape=tuple(jax.ShapeDtypeStruct(arr.shape, arr.dtype) for arr in arrs),
        in_specs=[pl.BlockSpec(memory_space=pltpu.VMEM)] * len(arrs),
        out_specs=(pl.BlockSpec(memory_space=pl.ANY),) * len(arrs),
        scratch_shapes=[pltpu.SemaphoreType.DMA((len(arrs),))],
        compiler_params=pltpu.CompilerParams(vmem_limit_bytes=1024 * 1024),
    )(*[pltpu.with_memory_space_constraint(arr, pltpu.VMEM) for arr in arrs])


def solution(mesh):
    seq_spec = P(None, 'cp', None, None)

    def local(query, key_in, value, bias_u, bias_w, rel_k, d_out):
        def by_head(arr):
            return arr.transpose(0, 2, 1, 3)

        rel = rel_k.transpose(1, 0, 2).reshape(NH, NT, T, D)
        acts = [by_head(arr) for arr in (query, d_out, key_in, value)]
        res = write_out(exchange_attend(*acts, bias_u, bias_w, rel)[:7])
        d_rel = res[4].reshape(NH, NT * T, D).transpose(1, 0, 2)
        return tuple(by_head(arr) for arr in res[:4]) + (res[5], res[6], d_rel)

    return jax.shard_map(local, mesh=mesh,
                         in_specs=(seq_spec, seq_spec, seq_spec, P(), P(), P(), seq_spec),
                         out_specs=(seq_spec, seq_spec, seq_spec, seq_spec, P(), P(), P()),
                         check_vma=False)
```

```python
import jax
import jax.numpy as jnp
from jax import lax
from jax.experimental import pallas as pl
from jax.experimental.pallas import tpu as pltpu
from jax.sharding import PartitionSpec as P

T = 256
D = 128
H = 128
NT = 8
NU = 6
NA = 4
HC = 3
NH = 12
EARLY = 6
AHEAD = 3
VMEM_LIMIT = 39 * 1024 * 1024
F32 = jnp.float32
BF = jnp.bfloat16
SCALE = D ** -0.5
C2 = SCALE * 1.4426950408889634
MESH = pl.DeviceIdType.MESH


def dot_nt(lhs, rhs):
    return lax.dot_general(lhs, rhs, (((1,), (1,)), ((), ())), preferred_element_type=F32)


def row_max(arr):
    return jnp.max(arr, axis=1, keepdims=True)


def row_sum(arr):
    return jnp.sum(arr, axis=1, keepdims=True)


def dot_nn(lhs, rhs):
    return lax.dot_general(lhs, rhs, (((1,), (0,)), ((), ())), preferred_element_type=F32)


def unit(x, rk, rkr, u, w, drk, duw, scratch, after_softmax, after_tile):
    (s_ref, dp_ref, r_ref, mx_ref, l_ref, d_ref, u_ref, dk_ref, dv_ref, a_ref, c_ref, t_ref,
     oacc, qc_acc, qr_acc) = scratch
    nt = NT
    low = lower_mask()
    gather = gather_fn()
    dk_ref[:] = jnp.zeros_like(dk_ref)
    dv_ref[:] = jnp.zeros_like(dv_ref)

    def prep(i, sl):
        q = x[i, 0].astype(F32)
        a_ref[sl] = (q + u).astype(BF)
        c_ref[sl] = (q + w).astype(BF)
        mx_ref[:] = jnp.full((T, H), -jnp.inf, F32)
        r_ref[:] = jnp.full((2, T, H), -jnp.inf, F32)

    def logits(i, sl, n):
        j = i - n
        by = dot_nt(c_ref[sl], rkr[n])
        sc = dot_nt(a_ref[sl], x[j, 2])
        dp_ref[sl, j] = dot_nt(x[i, 1], x[j, 3])
        r0, r1 = [pltpu.roll(half, 1, 1, stride=1, stride_axis=0) for half in (by[:, :H], by[:, H:])]
        sc += shifted(low, r1, r0, r_ref[1], r_ref[0])
        r_ref[0] = r0
        r_ref[1] = r1
        s_ref[sl, j] = sc
        mx_ref[:] = jnp.maximum(mx_ref[:], jnp.maximum(sc[:, :H], sc[:, H:]))

    def softmax(i, sl):
        m = row_max(mx_ref[:])
        l_ref[:] = jnp.zeros_like(l_ref)
        d_ref[:] = jnp.zeros_like(d_ref)

        def body(j, _):
            p = jnp.exp2((s_ref[sl, j] - m) * C2)
            s_ref[sl, j] = p
            pd = p * dp_ref[sl, j]
            l_ref[:] += p[:, :H] + p[:, H:]
            d_ref[:] += pd[:, :H] + pd[:, H:]
            return 0

        lax.fori_loop(0, i + 1, body, 0)
        inv = 1.0 / row_sum(l_ref[:])
        rd = row_sum(d_ref[:]) * inv
        after_softmax(i, m, inv, rd)
        return inv, rd

    def grads(i, sl, j, inv, rd):
        pn = s_ref[sl, j] * inv
        pb = pn.astype(BF)
        ds = pn * (dp_ref[sl, j] - rd) * SCALE
        dsb = ds.astype(BF)
        oacc[:] += dot_nn(pb, x[j, 3])
        dv_ref[j] += dot_nn(t_ref[0], pb)
        qc_acc[:] += dot_nn(dsb, x[j, 2])
        dk_ref[j] += dot_nn(t_ref[1], dsb)
        g0, g1 = gather(ds)
        dist = shifted(low, g0, g1, u_ref[0], u_ref[1]).astype(BF)
        u_ref[0] = g0
        u_ref[1] = g1
        qr_acc[:] += dot_nn(dist, rk[i - j])
        drk[i - j] += dot_nn(t_ref[2], dist)

    prep(nt - 1, (nt - 1) % 2)

    def first(n, _):
        logits(nt - 1, (nt - 1) % 2, n)
        return 0

    lax.fori_loop(0, nt, first, 0)

    def tile(ii, _):
        i = nt - 1 - ii
        sl = i % 2
        inv, rd = softmax(i, sl)
        nxt = jnp.maximum(i - 1, 0)
        t_ref[0] = x[i, 1].T
        t_ref[1] = a_ref[sl].T
        t_ref[2] = c_ref[sl].T
        for acc in (oacc, qc_acc, qr_acc, u_ref):
            acc[:] = jnp.zeros_like(acc)
        prep(nxt, 1 - sl)

        def both(n, _):
            grads(i, sl, n, inv, rd)
            logits(nxt, 1 - sl, n)
            return 0

        lax.fori_loop(0, i, both, 0)
        grads(i, sl, i, inv, rd)
        qc = qc_acc[:]
        qr = qr_acc[:]
        for r, part in enumerate((qc, qr)):
            duw[r:r + 1] += jnp.sum(part, axis=0, keepdims=True)
        for r, res in enumerate((oacc[:], qc + qr, dk_ref[i].T, dv_ref[i].T)):
            x[i, r] = res.astype(BF)
        after_tile(i)
        return 0

    lax.fori_loop(0, nt, tile, 0)


def gather_fn():
    idx = (lax.broadcasted_iota(jnp.int32, (T, H), 0) - lax.broadcasted_iota(jnp.int32, (T, H), 1)) & (H - 1)

    def gather(arr):
        return [jnp.take_along_axis(half, idx, axis=1, mode="promise_in_bounds") for half in (arr[:, :H], arr[:, H:])]

    return gather


def lower_mask():
    return lax.broadcasted_iota(jnp.int32, (H, H), 1) <= lax.broadcasted_iota(jnp.int32, (H, H), 0)


def shifted(low, n0, n1, p0, p1):
    lo = jnp.concatenate([jnp.where(low, n0[:H], p1[:H]), jnp.where(low, n1[H:], n0[H:])], 0)
    hi = jnp.concatenate([jnp.where(low, p1[:H], p0[:H]), jnp.where(low, n0[H:], p1[H:])], 0)
    return jnp.concatenate([lo, hi], 1)


def row_tile(q, d_out, keys, vals, rk, u, w):
    last = len(keys) - 1
    low = lower_mask()
    gather = gather_fn()
    qf = q.astype(F32)
    a = (qf + u).astype(BF)
    c = (qf + w).astype(BF)
    by = [gather(dot_nt(c, rk[n])) for n in range(last + 1)]
    none = [jnp.full((T, H), -jnp.inf, F32)] * 2
    s = [dot_nt(a, key) + shifted(low, *by[last - j], *(by[last - j - 1] if j < last else none)) for j, key in enumerate(keys)]
    top = s[0]
    for other in s[1:]:
        top = jnp.maximum(top, other)
    m = row_max(top)
    p = [jnp.exp2((sj - m) * C2) for sj in s]
    dp = [dot_nt(d_out, val) for val in vals]
    inv = 1.0 / row_sum(sum(p))
    row_dot = row_sum(sum(pj * dj for pj, dj in zip(p, dp))) * inv
    out, d_q, prev = 0.0, 0.0, [jnp.zeros((T, H), F32)] * 2
    for j in range(last + 1):
        pn = p[j] * inv
        ds = pn * (dp[j] - row_dot) * SCALE
        out += dot_nn(pn.astype(BF), vals[j])
        mine = gather(ds)
        dist = shifted(low, *mine, *prev).astype(BF)
        prev = mine
        d_q += dot_nn(ds.astype(BF), keys[j]) + dot_nn(dist, rk[last - j])
    return out.astype(BF), d_q.astype(BF)


def col_tiles(qs, d_outs, keys, vals, rk, stats, u, w):
    low = lower_mask()
    gather = gather_fn()
    none = [jnp.full((T, H), -jnp.inf, F32)] * 2
    d_keys, d_vals = [0.0, 0.0], [0.0, 0.0]
    for i in range(len(qs)):
        qf = qs[i].astype(F32)
        a = (qf + u).astype(BF)
        c = (qf + w).astype(BF)
        by = {n: gather(dot_nt(c, rk[n])) for n in range(max(i - 2, 0), i + 1)}
        if i % 2 == 0:
            cols = jnp.concatenate([stats[i // 2], jnp.zeros((H - 8, T), F32)], 0).T
        m, inv, row_dot = [cols[:, r:r + 1] for r in range(HC * (i % 2), HC * (i % 2 + 1))]
        at, dot = a.T, d_outs[i].T
        for r in range(min(i + 1, 2)):
            n = i - r
            s = dot_nt(a, keys[r]) + shifted(low, *by[n], *(by[n - 1] if n else none))
            pn = jnp.exp2((s - m) * C2) * inv
            ds = pn * (dot_nt(d_outs[i], vals[r]) - row_dot) * SCALE
            d_vals[r] += dot_nn(dot, pn.astype(BF))
            d_keys[r] += dot_nn(at, ds.astype(BF))
    return [dk.T.astype(BF) for dk in d_keys], [dv.T.astype(BF) for dv in d_vals]


UNIT_SCRATCH = (
    [pltpu.VMEM((2, NT, T, T), F32)] * 2 + [pltpu.VMEM((2, T, H), F32)] + [pltpu.VMEM((T, H), F32)] * 3
    + [pltpu.VMEM((2, T, H), F32)] + [pltpu.VMEM((NT, D, T), F32)] * 2 + [pltpu.VMEM((2, T, D), BF)] * 2
    + [pltpu.VMEM((3, D, T), BF)] + [pltpu.VMEM((T, D), F32)] * 3)


def kernel(xq, xd, xk, xv, bias_u, bias_w, rel, out, drk_out, du_out, dw_out, lx,
           rin, rl, drk, pbuf, duw, duw_all, rk, rkr, bu, bw, lblk, lrk, lres, st_out, st_in,
           in_send, in_recv, in_loc, rl_recv, fw_send, fw_recv, out_send, out_recv, half_send, half_recv,
           fin_send, fin_recv, hop_send, hop_recv, rel_send, rel_recv, duw_send, duw_recv, rk_sem, px_send, px_recv,
           st_send, st_recv, l_sem, lr_send, lr_recv, *scratch):
    me = lax.axis_index('cp')
    chip = me // 2
    core = me % 2
    last = NA - 1
    partner = jnp.bitwise_xor(me, 1)
    outer = (chip == 0) | (chip == last)
    ins = (xq, xd, xk, xv)
    neighbours = (1, 2, 4)

    def remote(src, dst, ssem, rsem, dev):
        return pltpu.make_async_remote_copy(src_ref=src, dst_ref=dst, send_sem=ssem, recv_sem=rsem,
                                            device_id=(dev,), device_id_type=MESH)

    def pair_of(dev, n):
        return 2 * (dev % 2) + n % 2, HC * (dev // 2) + n // 2

    def spot(a, dev, n):
        return ins[a].at[pair_of(dev, n)]

    def send_in(n, mask):
        dev = jnp.bitwise_xor(me, mask)

        def send(first, via):
            for a in (first, first + 1):
                if via:
                    dst, rsem, to = rl.at[n, core, a % 2], rl_recv.at[n], jnp.bitwise_xor(dev, 4)
                else:
                    dst, rsem, to = rin.at[n, me, a], in_recv.at[n, mask], dev
                remote(spot(a, dev, n), dst, in_send.at[n, mask], rsem, to).start()

        for first in (0, 2):
            if mask < NU:
                send(first, False)
            else:
                through = chip == (0 if first else last)
                for via in (True, False):
                    @pl.when(through == via)
                    def _():
                        send(first, via)

    def send_pair(n):
        for mask in (6, 2, 4, 7, 3, 5, 1):
            send_in(n, mask)

    def in_wait(n, mask, size=NA):
        dev = jnp.bitwise_xor(me, mask)
        piece = rin.at[n, dev, pl.ds(0, size)]
        return remote(piece, piece, in_send.at[n, mask], in_recv.at[n, mask], dev)

    def forward(n):
        dst = rin.at[n, pl.ds(2 * jnp.bitwise_xor(chip, 1), 2), pl.ds(2 * (chip % 2), 2)]
        return remote(rl.at[n], dst, fw_send.at[n], fw_recv.at[n], jnp.bitwise_xor(me, 4))

    def pass_forward(n):
        remote(rl.at[n], rl.at[n], fw_send.at[n], rl_recv.at[n], jnp.bitwise_xor(me, 2)).wait_recv()
        forward(n).start()

    def at_chip(act):
        for c, heads in enumerate(((3, 9), (9, 3), (0, 3), (0, 9))):
            @pl.when(chip == c)
            def _():
                act(c, pl.ds(*heads))

    def pair_copies(heads):
        return [remote(ins[a].at[pl.ds(2 * (1 - core), 2), heads], lx.at[a, :, heads], px_send.at[a], px_recv.at[a], partner)
                for a in range(NA)]

    barrier = pltpu.get_barrier_semaphore()
    for mask in range(1, NT):
        pl.semaphore_signal(barrier, inc=1, device_id=(jnp.bitwise_xor(me, mask),), device_id_type=MESH)
    rk_copy = pltpu.make_async_copy(rel.at[pl.ds(HC * chip, HC)], rk, rk_sem)
    rk_copy.start()
    for n in range(NU):
        for a in range(NA):
            pltpu.make_async_copy(spot(a, me, n), rin.at[n, me, a], in_loc.at[n]).start()
    pl.semaphore_wait(barrier, NT - 1)
    for n in range(NU):
        if n < AHEAD:
            send_pair(n)
        if n == 0:
            at_chip(lambda c, heads: [copy.start() for copy in pair_copies(heads)])

    bu[:] = bias_u[:].astype(F32)
    bw[:] = bias_w[:].astype(F32)
    drk[:] = jnp.zeros_like(drk)
    duw[:] = jnp.zeros_like(duw)
    st_out[:] = jnp.zeros_like(st_out)
    rk_copy.wait()
    flip = (lax.broadcasted_iota(jnp.int32, (T, T), 0) + lax.broadcasted_iota(jnp.int32, (T, T), 1) == T - 1).astype(BF)
    for k in range(HC):
        for n in range(NT):
            rkr[k, n] = dot_nn(flip, rk[k, n]).astype(BF)

    def half_copy(k):
        return remote(drk.at[k, pl.ds(NA * (1 - core), NA)], pbuf.at[k], half_send.at[k], half_recv.at[k], partner)

    def part(src_chip, k, lo, size):
        return drk_out.at[HC * src_chip + k, pl.ds(NA * core + lo, size)]

    def fin_copy(k, s, arrived=False):
        piece = part(jnp.bitwise_xor(chip, s) if arrived else chip, k, 0, NA)
        return remote(piece, piece, fin_send.at[k, s], fin_recv.at[k, s], jnp.bitwise_xor(me, neighbours[s]))

    def hop(k, s, whole, arrived=False):
        span = (0, NA) if whole else (2 * (s - 1), 2)
        piece = part(jnp.bitwise_xor(chip, last if arrived else s), k, *span)
        return remote(piece, piece, hop_send.at[k, s], hop_recv.at[k, s], jnp.bitwise_xor(me, neighbours[-s]))

    def hops(k, s, sender, act):
        @pl.when(sender)
        def _():
            act(k, s, False)

        if s == 1:
            @pl.when(~sender)
            def _():
                act(k, s, True)

    def relay(k, s, arrived=False):
        half = 1 - core if arrived else core
        piece = drk_out.at[HC * jnp.bitwise_xor(chip, s) + k, pl.ds(NA * half, NA)]
        return remote(piece, piece, rel_send.at[k, s], rel_recv.at[k, s], partner)

    def pass_on(k):
        for s in (1, 2):
            fin_copy(k, s, True).wait_recv()
            hops(k, s, outer, lambda *args: hop(*args).start())
            relay(k, s).start()

    def made_there(first, dev, owner):
        there = dev // 2
        if first:
            return ((there == last) & (owner != last)) | ((there == 2) & (owner == 0))
        return ((there == 0) & (owner != 0)) | ((there == 1) & (owner == last))

    def stat_copy(n, whole):
        if whole:
            return remote(st_out.at[n], st_in.at[0, n], st_send.at[n, 1], st_recv.at[0, n], 4 + core)
        return remote(st_out.at[n, 1], st_in.at[chip, n, 1], st_send.at[n, 0], st_recv.at[chip, n], 6 + core)

    def after_softmax(n, i, m, inv, rd):
        first = jnp.where(chip == 0, 4, 6)

        @pl.when((i >= first) & (chip != last))
        def _():
            lane = lax.broadcasted_iota(jnp.int32, (T, H), 1)
            table = jnp.where(lane == 0, m, jnp.where(lane == 1, inv, rd)).T
            for r in range(2):
                @pl.when(i % 2 == r)
                def _():
                    st_out[n, i // 2 - 2, HC * r:HC * (r + 1)] = table[:HC]

        @pl.when((i == 6) & (chip != last))
        def _():
            stat_copy(n, False).start()

        @pl.when((i == 4) & (chip == 0))
        def _():
            stat_copy(n, True).start()

    def local_pair(x):
        owner = jnp.where(outer, x % HC + jnp.where(chip == 0, 1, 0), jnp.where(chip == 1, last, 0))
        n = jnp.where(outer, x // HC, x)
        return owner, n, 2 * core + n % 2, HC * owner + n // 2

    def local_loads(x, sl):
        _, n, bat, head = local_pair(x)
        copies = [pltpu.make_async_copy(rel.at[head, pl.ds(0, NA)], lrk.at[sl], l_sem.at[sl, 0, 2])]
        for a in range(NA):
            for r, src in enumerate((ins[a].at[bat, head], lx.at[a, n % 2, head])):
                where = core if r == 0 else 1 - core
                copies.append(pltpu.make_async_copy(src, lblk.at[sl, where, a], l_sem.at[sl, a, r]))
        return copies

    def local_send(x, c):
        sl = x % 2
        _, _, bat, head = local_pair(x)
        dst = out.at[pl.ds(2 * (c // 2), 2), bat, head]
        return remote(lres.at[sl, 1 - core], dst, lr_send.at[sl], lr_recv, partner)

    def local_work(lo, hi, c):
        for copy in local_loads(lo, lo % 2):
            copy.start()

        def one(x, _):
            sl = x % 2

            @pl.when(x + 1 < hi)
            def _():
                for copy in local_loads(x + 1, 1 - sl):
                    copy.start()

            for copy in local_loads(x, sl):
                copy.wait()

            @pl.when(x > 1)
            def _():
                local_send(x, c).wait_send()

            owner, n, bat, head = local_pair(x)
            u = bu[pl.ds(head, 1)]
            w = bw[pl.ds(head, 1)]
            q, do, key, val = [[lblk[sl, r, a] for r in range(2)] for a in range(NA)]
            table = lrk[sl]
            if c < 2:
                if c:
                    key = [rl[n, r, 0] for r in range(2)] + key
                    val = [rl[n, r, 1] for r in range(2)] + val
                for r in range(2):
                    upto = len(key) - 1 + r
                    res = row_tile(q[r], do[r], key[:upto], val[:upto], table, u, w)
                    for a in range(2):
                        lres[sl, r, a] = res[a]
            else:
                groups = (1,)
                piece = st_in.at[owner, n, 1]
                if c != last:
                    groups = (0, 1)
                    piece = st_in.at[owner, n]
                    q = q + [rl[n, r, 0] for r in range(2)]
                    do = do + [rl[n, r, 1] for r in range(2)]
                remote(piece, piece, st_send.at[n, 0], st_recv.at[owner, n], 2 * owner + core).wait_recv()
                stats = [st_in[owner, n, g] for g in groups]
                for a, res in enumerate(col_tiles(q, do, key, val, table, stats, u, w)):
                    for r in range(2):
                        lres[sl, r, a] = res[r]
            local_send(x, c).start()
            for a in range(2):
                out[2 * (c // 2) + a, bat, head] = lres[sl, core, a]
            return 0

        lax.fori_loop(lo, hi, one, 0)

    def local_count(c):
        return NU if c in (1, 2) else NU * HC

    @pl.when(chip == 0)
    def _():
        for copy in pair_copies(pl.ds(3, 9)):
            copy.wait_recv()
        local_work(0, EARLY, 0)

    def send_tile(n, i):
        mask = jnp.bitwise_xor(me, i)
        for first in (0, 2):
            @pl.when((mask != 0) & ~made_there(first, i, chip))
            def _():
                two = pl.ds(first, 2)
                remote(rin.at[n, i, two], out.at[(two,) + pair_of(me, n)], out_send.at[n, i, first // 2],
                       out_recv.at[n, mask, first // 2], i).start()

        @pl.when(mask == 0)
        def _():
            for a in range(NA):
                out[(a,) + pair_of(me, n)] = rin[n, i, a]

    def run_unit(n, _):
        k = n // 2

        @pl.when(n + AHEAD < NU)
        def _():
            send_pair(n + AHEAD)

        @pl.when(~outer & (n == 0))
        def _():
            pass_forward(0)

        @pl.when(~outer & (n + 1 < NU))
        def _():
            pass_forward(n + 1)

        pltpu.make_async_copy(rin.at[n, me], rin.at[n, me], in_loc.at[n]).wait()
        for mask in range(1, NT):
            if mask < NU:
                in_wait(n, mask).wait_recv()
            else:
                for split in (True, False):
                    @pl.when(outer == split)
                    def _():
                        in_wait(n, mask, 2 if split else NA).wait_recv()

        @pl.when(outer)
        def _():
            piece = rin.at[n, pl.ds(0, 2), pl.ds(0, 2)]
            remote(piece, piece, fw_send.at[n], fw_recv.at[n], jnp.bitwise_xor(me, 4)).wait_recv()

        head = pl.ds(HC * chip + k, 1)
        unit(rin.at[n], rk.at[k], rkr.at[k], bu[head], bw[head], drk.at[k], duw.at[k], scratch,
             lambda i, m, inv, rd: after_softmax(n, i, m, inv, rd), lambda i: send_tile(n, i))

        @pl.when(n % 2 == 1)
        def _():
            copy = half_copy(k)
            copy.start()
            copy.wait()
            for r in range(NA):
                part(chip, k, r, 1)[0] = (drk[k, NA * core + r] + pbuf[k, r]).T
            for s in range(3):
                fin_copy(k, s).start()

        return 0

    lax.fori_loop(0, NU, run_unit, 0)

    pass_on(0)
    pass_on(1)

    def duw_copy(mask, arrived):
        dev = jnp.bitwise_xor(me, mask)
        return remote(duw, duw_all.at[dev if arrived else me], duw_send.at[mask], duw_recv.at[mask], dev)

    for mask in range(1, NT):
        duw_copy(mask, False).start()
    duw_all[me] = duw[:]

    def late_work(c, heads):
        if c:
            for copy in pair_copies(heads):
                copy.wait_recv()
        local_work(0 if c else EARLY, local_count(c), c)

    at_chip(late_work)
    pass_on(2)
    for k in range(HC):
        for s in (1, 2):
            hops(k, s, ~outer, lambda *args: hop(*args, True).wait_recv())
        relay(k, last).start()

    for mask in range(1, NT):
        duw_copy(mask, False).wait_send()
        duw_copy(mask, True).wait_recv()
    for h in range(NH):
        both = duw_all[2 * (h // HC), h % HC] + duw_all[2 * (h // HC) + 1, h % HC]
        for r, bias_out in enumerate((du_out, dw_out)):
            bias_out[h:h + 1] = both[r:r + 1]

    def finish(n, _):
        for mask in range(1, NT):
            dev = jnp.bitwise_xor(me, mask)
            in_wait(n, mask).wait_send()
            for first in (0, 2):
                both = rin.at[n, dev, pl.ds(first, 2)]
                copy = remote(both, both, out_send.at[n, dev, first // 2], out_recv.at[n, mask, first // 2], dev)

                @pl.when(~made_there(first, dev, chip))
                def _():
                    copy.wait_send()

                @pl.when(~made_there(first, me, dev // 2))
                def _():
                    copy.wait_recv()

        @pl.when(~outer)
        def _():
            forward(n).wait_send()

        @pl.when(chip != last)
        def _():
            stat_copy(n, False).wait_send()

        @pl.when(chip == 0)
        def _():
            stat_copy(n, True).wait_send()
        return 0

    lax.fori_loop(0, NU, finish, 0)

    def end_local(c, heads):
        for copy in pair_copies(heads):
            copy.wait_send()
        count = local_count(c)
        for x in (count - 2, count - 1):
            local_send(x, c).wait_send()
        whole = out.at[0, pl.ds(0, count // NU)]
        remote(whole, whole, lr_send.at[0], lr_recv, partner).wait_recv()

    at_chip(end_local)
    for k in range(HC):
        fin_copy(k, 0).wait_send()
        theirs = drk_out.at[HC * chip + k, pl.ds(NA * (1 - core), NA)]
        remote(theirs, theirs, fin_send.at[k, 0], fin_recv.at[k, 0], partner).wait_recv()
        for s in (1, 2):
            fin_copy(k, s).wait_send()
            hops(k, s, outer, lambda *args: hop(*args).wait_send())
        for s in (1, 2, last):
            relay(k, s).wait_send()
            relay(k, s, True).wait_recv()


def exchange_attend(xq, xd, xk, xv, bias_u, bias_w, rel):
    any_spec = pl.BlockSpec(memory_space=pl.ANY)
    vmem_spec = pl.BlockSpec(memory_space=pltpu.VMEM)
    dma = pltpu.SemaphoreType.DMA
    acts = pltpu.VMEM((NA, NA, NH, T, D), BF)
    bias = pltpu.VMEM((NH, D), F32)
    heads = pltpu.VMEM((HC, NT, T, D), BF)
    per_head = dma((HC, NA))
    per_pair = dma((NU,))
    per_peer = dma((NU, NT))
    per_half = dma((NU, NT, 2))
    return pl.pallas_call(
        kernel,
        out_shape=(acts, pltpu.VMEM((NH, NT, T, D), F32), bias, bias,
                   jax.ShapeDtypeStruct((NA, 2, NH, T, D), BF)),
        in_specs=[any_spec] * 4 + [vmem_spec] * 2 + [any_spec],
        out_specs=(vmem_spec,) * 4 + (any_spec,),
        scratch_shapes=[
            pltpu.VMEM((NU, NT, NA, T, D), BF), pltpu.VMEM((NU, 2, 2, T, D), BF), pltpu.VMEM((HC, NT, D, T), F32),
            pltpu.VMEM((HC, NA, D, T), F32), pltpu.VMEM((HC, 8, D), F32), pltpu.VMEM((NT, HC, 8, D), F32),
            heads, heads, bias, bias,
            pltpu.VMEM((2, 2, NA, T, D), BF), pltpu.VMEM((2, NA, T, D), BF), pltpu.VMEM((2, 2, 2, T, D), BF),
            pltpu.VMEM((NU, 2, 8, T), F32), pltpu.VMEM((HC, NU, 2, 8, T), F32),
            per_peer, per_peer, per_pair, per_pair, per_pair, per_pair, per_half, per_half, dma((HC,)), dma((HC,)),
            per_head, per_head, per_head, per_head, per_head, per_head, dma((NT,)), dma((NT,)), dma(()), dma((NA,)),
            dma((NA,)), dma((NU, 2)), dma((HC, NU)), dma((2, NA, HC)), dma((2,)), dma(())]
        + UNIT_SCRATCH,
        compiler_params=pltpu.CompilerParams(collective_id=0, has_side_effects=True, vmem_limit_bytes=VMEM_LIMIT),
    )(xq, xd, xk, xv, bias_u, bias_w, rel)


def write_kernel(acts, table, bias_u, bias_w, *refs):
    sem = refs[-1]
    srcs = [acts.at[a] for a in range(NA)] + [table, bias_u, bias_w]
    copies = [pltpu.make_async_copy(src, dst, sem.at[n]) for n, (src, dst) in enumerate(zip(srcs, refs[:-1]))]
    for copy in copies:
        copy.start()
    for copy in copies:
        copy.wait()


def write_out(arrs):
    shapes = [arrs[0].shape[1:]] * NA + [arr.shape for arr in arrs[1:]]
    types = [arrs[0].dtype] * NA + [arr.dtype for arr in arrs[1:]]
    return pl.pallas_call(
        write_kernel,
        out_shape=tuple(map(jax.ShapeDtypeStruct, shapes, types)),
        in_specs=[pl.BlockSpec(memory_space=pltpu.VMEM)] * len(arrs),
        out_specs=(pl.BlockSpec(memory_space=pl.ANY),) * len(shapes),
        scratch_shapes=[pltpu.SemaphoreType.DMA((len(shapes),))],
        compiler_params=pltpu.CompilerParams(vmem_limit_bytes=1024 * 1024),
    )(*[pltpu.with_memory_space_constraint(arr, pltpu.VMEM) for arr in arrs])


def solution(mesh):
    seq_spec = P(None, 'cp', None, None)

    def local(query, key_in, value, bias_u, bias_w, rel_k, d_out):
        def by_head(arr):
            return arr.transpose(0, 2, 1, 3)

        rel = rel_k.transpose(1, 0, 2).reshape(NH, NT, T, D)
        acts = [by_head(arr) for arr in (query, d_out, key_in, value)]
        res = write_out(exchange_attend(*acts, bias_u, bias_w, rel)[:4])
        d_rel = res[4].reshape(NH, NT * T, D).transpose(1, 0, 2)
        return tuple(by_head(arr) for arr in res[:4]) + (res[5], res[6], d_rel)

    return jax.shard_map(local, mesh=mesh,
                         in_specs=(seq_spec, seq_spec, seq_spec, P(), P(), P(), seq_spec),
                         out_specs=(seq_spec, seq_spec, seq_spec, seq_spec, P(), P(), P()),
                         check_vma=False)
```

```python
import jax
import jax.numpy as jnp
from jax import lax
from jax.experimental import pallas as pl
from jax.experimental.pallas import tpu as pltpu
from jax.sharding import PartitionSpec as P

T = 256
D = 128
H = 128
NT = 8
NU = 6
NA = 4
HC = 3
NH = 12
EARLY = 6
GROUPS = ((0, 1), (1, 1), (2, 2), (4, 2))
AHEAD = 3
SEND_AT = 1
FORWARD_AT = (0, 0, 1, 3)
VMEM_LIMIT = 39 * 1024 * 1024
F32 = jnp.float32
BF = jnp.bfloat16
SCALE = D ** -0.5
C2 = SCALE * 1.4426950408889634
MESH = pl.DeviceIdType.MESH


def dot_nt(lhs, rhs):
    return lax.dot_general(lhs, rhs, (((1,), (1,)), ((), ())), preferred_element_type=F32)


def row_max(arr):
    return jnp.max(arr, axis=1, keepdims=True)


def row_sum(arr):
    return jnp.sum(arr, axis=1, keepdims=True)


def dot_nn(lhs, rhs):
    return lax.dot_general(lhs, rhs, (((1,), (0,)), ((), ())), preferred_element_type=F32)


def unit(x, rk, rkr, u, w, drk, duw, scratch, after_softmax, after_tile):
    (s_ref, dp_ref, r_ref, mx_ref, l_ref, d_ref, u_ref, dk_ref, dv_ref, a_ref, c_ref, t_ref,
     oacc, qc_acc, qr_acc) = scratch
    nt = NT
    low = lower_mask()
    gather = gather_fn()
    dk_ref[:] = jnp.zeros_like(dk_ref)
    dv_ref[:] = jnp.zeros_like(dv_ref)

    def prep(i, sl):
        q = x[i, 0].astype(F32)
        a_ref[sl] = (q + u).astype(BF)
        c_ref[sl] = (q + w).astype(BF)
        mx_ref[:] = jnp.full((T, H), -jnp.inf, F32)
        r_ref[:] = jnp.full((2, T, H), -jnp.inf, F32)

    def logits(i, sl, n):
        j = i - n
        by = dot_nt(c_ref[sl], rkr[n])
        sc = dot_nt(a_ref[sl], x[j, 2])
        dp_ref[sl, j] = dot_nt(x[i, 1], x[j, 3])
        r0, r1 = [pltpu.roll(half, 1, 1, stride=1, stride_axis=0) for half in (by[:, :H], by[:, H:])]
        sc += shifted(low, r1, r0, r_ref[1], r_ref[0])
        r_ref[0] = r0
        r_ref[1] = r1
        s_ref[sl, j] = sc
        mx_ref[:] = jnp.maximum(mx_ref[:], jnp.maximum(sc[:, :H], sc[:, H:]))

    def softmax(i, sl):
        m = row_max(mx_ref[:])
        l_ref[:] = jnp.zeros_like(l_ref)
        d_ref[:] = jnp.zeros_like(d_ref)

        def body(j, _):
            p = jnp.exp2((s_ref[sl, j] - m) * C2)
            s_ref[sl, j] = p
            pd = p * dp_ref[sl, j]
            l_ref[:] += p[:, :H] + p[:, H:]
            d_ref[:] += pd[:, :H] + pd[:, H:]
            return 0

        lax.fori_loop(0, i + 1, body, 0)
        inv = 1.0 / row_sum(l_ref[:])
        rd = row_sum(d_ref[:]) * inv
        after_softmax(i, m, inv, rd)
        return inv, rd

    def grads(i, sl, j, inv, rd):
        pn = s_ref[sl, j] * inv
        pb = pn.astype(BF)
        ds = pn * (dp_ref[sl, j] - rd) * SCALE
        dsb = ds.astype(BF)
        oacc[:] += dot_nn(pb, x[j, 3])
        dv_ref[j] += dot_nn(t_ref[0], pb)
        qc_acc[:] += dot_nn(dsb, x[j, 2])
        dk_ref[j] += dot_nn(t_ref[1], dsb)
        g0, g1 = gather(ds)
        dist = shifted(low, g0, g1, u_ref[0], u_ref[1]).astype(BF)
        u_ref[0] = g0
        u_ref[1] = g1
        qr_acc[:] += dot_nn(dist, rk[i - j])
        drk[i - j] += dot_nn(t_ref[2], dist)

    prep(nt - 1, (nt - 1) % 2)

    def first(n, _):
        logits(nt - 1, (nt - 1) % 2, n)
        return 0

    lax.fori_loop(0, nt, first, 0)

    def tile(ii, _):
        i = nt - 1 - ii
        sl = i % 2
        inv, rd = softmax(i, sl)
        nxt = jnp.maximum(i - 1, 0)
        t_ref[0] = x[i, 1].T
        t_ref[1] = a_ref[sl].T
        t_ref[2] = c_ref[sl].T
        for acc in (oacc, qc_acc, qr_acc, u_ref):
            acc[:] = jnp.zeros_like(acc)
        prep(nxt, 1 - sl)

        def both(n, _):
            grads(i, sl, n, inv, rd)
            logits(nxt, 1 - sl, n)
            return 0

        lax.fori_loop(0, i, both, 0)
        grads(i, sl, i, inv, rd)
        qc = qc_acc[:]
        qr = qr_acc[:]
        for r, part in enumerate((qc, qr)):
            duw[r:r + 1] += jnp.sum(part, axis=0, keepdims=True)
        for r, res in enumerate((oacc[:], qc + qr, dk_ref[i].T, dv_ref[i].T)):
            x[i, r] = res.astype(BF)
        after_tile(i)
        return 0

    lax.fori_loop(0, nt, tile, 0)


def gather_fn():
    idx = (lax.broadcasted_iota(jnp.int32, (T, H), 0) - lax.broadcasted_iota(jnp.int32, (T, H), 1)) & (H - 1)

    def gather(arr):
        return [jnp.take_along_axis(half, idx, axis=1, mode="promise_in_bounds") for half in (arr[:, :H], arr[:, H:])]

    return gather


def lower_mask():
    return lax.broadcasted_iota(jnp.int32, (H, H), 1) <= lax.broadcasted_iota(jnp.int32, (H, H), 0)


def shifted(low, n0, n1, p0, p1):
    lo = jnp.concatenate([jnp.where(low, n0[:H], p1[:H]), jnp.where(low, n1[H:], n0[H:])], 0)
    hi = jnp.concatenate([jnp.where(low, p1[:H], p0[:H]), jnp.where(low, n0[H:], p1[H:])], 0)
    return jnp.concatenate([lo, hi], 1)


def row_tile(q, d_out, keys, vals, rk, u, w):
    last = len(keys) - 1
    low = lower_mask()
    gather = gather_fn()
    qf = q.astype(F32)
    a = (qf + u).astype(BF)
    c = (qf + w).astype(BF)
    by = [gather(dot_nt(c, rk[n])) for n in range(last + 1)]
    none = [jnp.full((T, H), -jnp.inf, F32)] * 2
    s = [dot_nt(a, key) + shifted(low, *by[last - j], *(by[last - j - 1] if j < last else none)) for j, key in enumerate(keys)]
    top = s[0]
    for other in s[1:]:
        top = jnp.maximum(top, other)
    m = row_max(top)
    p = [jnp.exp2((sj - m) * C2) for sj in s]
    dp = [dot_nt(d_out, val) for val in vals]
    inv = 1.0 / row_sum(sum(p))
    row_dot = row_sum(sum(pj * dj for pj, dj in zip(p, dp))) * inv
    out, d_q, prev = 0.0, 0.0, [jnp.zeros((T, H), F32)] * 2
    for j in range(last + 1):
        pn = p[j] * inv
        ds = pn * (dp[j] - row_dot) * SCALE
        out += dot_nn(pn.astype(BF), vals[j])
        mine = gather(ds)
        dist = shifted(low, *mine, *prev).astype(BF)
        prev = mine
        d_q += dot_nn(ds.astype(BF), keys[j]) + dot_nn(dist, rk[last - j])
    return out.astype(BF), d_q.astype(BF)


def col_tiles(qs, d_outs, keys, vals, rk, stats, u, w):
    low = lower_mask()
    gather = gather_fn()
    none = [jnp.full((T, H), -jnp.inf, F32)] * 2
    d_keys, d_vals = [0.0, 0.0], [0.0, 0.0]
    for i in range(len(qs)):
        qf = qs[i].astype(F32)
        a = (qf + u).astype(BF)
        c = (qf + w).astype(BF)
        by = {n: gather(dot_nt(c, rk[n])) for n in range(max(i - 2, 0), i + 1)}
        if i % 2 == 0:
            cols = jnp.concatenate([stats[i // 2], jnp.zeros((H - 8, T), F32)], 0).T
        m, inv, row_dot = [cols[:, r:r + 1] for r in range(HC * (i % 2), HC * (i % 2 + 1))]
        at, dot = a.T, d_outs[i].T
        for r in range(min(i + 1, 2)):
            n = i - r
            s = dot_nt(a, keys[r]) + shifted(low, *by[n], *(by[n - 1] if n else none))
            pn = jnp.exp2((s - m) * C2) * inv
            ds = pn * (dot_nt(d_outs[i], vals[r]) - row_dot) * SCALE
            d_vals[r] += dot_nn(dot, pn.astype(BF))
            d_keys[r] += dot_nn(at, ds.astype(BF))
    return [dk.T.astype(BF) for dk in d_keys], [dv.T.astype(BF) for dv in d_vals]


UNIT_SCRATCH = (
    [pltpu.VMEM((2, NT, T, T), F32)] * 2 + [pltpu.VMEM((2, T, H), F32)] + [pltpu.VMEM((T, H), F32)] * 3
    + [pltpu.VMEM((2, T, H), F32)] + [pltpu.VMEM((NT, D, T), F32)] * 2 + [pltpu.VMEM((2, T, D), BF)] * 2
    + [pltpu.VMEM((3, D, T), BF)] + [pltpu.VMEM((T, D), F32)] * 3)


def kernel(xq, xd, xk, xv, bias_u, bias_w, rel, out, drk_out, du_out, dw_out, lx,
           rin, rl, drk, pbuf, duw, duw_all, rk, rkr, bias, bu, bw, lblk, lrk, lres, st_out, st_in,
           in_recv, rl_recv, st_recv, half_send, half_recv, fin_recv, hop_recv, l_sem, lr_send,
           in_send, in_loc, fw_send, out_send, out_recv, table_send, table_recv, duw_send, duw_recv, rk_sem, px_send,
           px_recv, st_send, st_send_all, lr_recv, *scratch):
    me = lax.axis_index('cp')
    chip = me // 2
    core = me % 2
    last = NA - 1
    partner = jnp.bitwise_xor(me, 1)
    outer = (chip == 0) | (chip == last)
    ins = (xq, xd, xk, xv)
    neighbours = (1, 2, 4)

    def remote(src, dst, ssem, rsem, dev):
        return pltpu.make_async_remote_copy(src_ref=src, dst_ref=dst, send_sem=ssem, recv_sem=rsem,
                                            device_id=(dev,), device_id_type=MESH)

    def pair_of(dev, n):
        return 2 * (dev % 2) + n % 2, HC * (dev // 2) + n // 2

    def spot(a, dev, n):
        return ins[a].at[pair_of(dev, n)]

    def pairs(n, count):
        return pl.ds(n, count) if count > 1 else n

    def send_in(n, count, mask):
        dev = jnp.bitwise_xor(me, mask)
        bat, head = pair_of(dev, n)

        def send(first, via):
            for a in (first, first + 1):
                if via:
                    dst, rsem, to = rl.at[pairs(n, count), core, a % 2], rl_recv.at[n], jnp.bitwise_xor(dev, 4)
                else:
                    dst, rsem, to = rin.at[pairs(n, count), me, a], in_recv.at[n], dev
                remote(ins[a].at[pairs(bat, count), head], dst, in_send, rsem, to).start()

        for first in (0, 2):
            if mask < NU:
                send(first, False)
            else:
                through = chip == (0 if first else last)
                for via in (True, False):
                    @pl.when(through == via)
                    def _():
                        send(first, via)

    def send_group(n, count):
        for mask in (6, 2, 4, 7, 3, 5, 1):
            send_in(n, count, mask)

    def forward(n, count):
        dst = rin.at[pairs(n, count), pl.ds(2 * jnp.bitwise_xor(chip, 1), 2), pl.ds(2 * (chip % 2), 2)]
        return remote(rl.at[pairs(n, count)], dst, fw_send, in_recv.at[n], jnp.bitwise_xor(me, 4))

    def pass_forward(n, count):
        piece = rl.at[pairs(n, count)]
        remote(piece, piece, fw_send, rl_recv.at[n], jnp.bitwise_xor(me, 2)).wait_recv()
        forward(n, count).start()

    def arrive(n, count):
        piece = rin.at[pairs(n, count), pl.ds(0, NT - 1)]
        remote(piece, piece, in_send, in_recv.at[n], partner).wait_recv()

    def at_chip(act):
        for c, heads in enumerate(((3, 9), (9, 3), (0, 3), (0, 9))):
            @pl.when(chip == c)
            def _():
                act(c, pl.ds(*heads))

    def pair_wait(heads, wait):
        piece = lx.at[:, :, heads]
        getattr(remote(piece, piece, px_send, px_recv, partner), wait)()

    def pair_copies(heads):
        return [remote(ins[a].at[pl.ds(2 * (1 - core), 2), heads], lx.at[a, :, heads], px_send, px_recv, partner)
                for a in range(NA)]

    barrier = pltpu.get_barrier_semaphore()
    for mask in range(1, NT):
        pl.semaphore_signal(barrier, inc=1, device_id=(jnp.bitwise_xor(me, mask),), device_id_type=MESH)
    copies = [pltpu.make_async_copy(bias_u, bias.at[0], rk_sem.at[0]), pltpu.make_async_copy(bias_w, bias.at[1], rk_sem.at[1]),
              pltpu.make_async_copy(rel.at[pl.ds(HC * chip, HC)], rk, rk_sem.at[2])]
    for copy in copies:
        copy.start()
    for n in range(NU):
        for a in range(NA):
            pltpu.make_async_copy(spot(a, me, n), rin.at[n, me, a], in_loc).start()
    pl.semaphore_wait(barrier, NT - 1)
    for g, (n, count) in enumerate(GROUPS):
        if g < AHEAD:
            send_group(n, count)
        if g == 0:
            at_chip(lambda c, heads: [copy.start() for copy in pair_copies(heads)])

    for copy in copies:
        copy.wait()
    bu[:] = bias[0].astype(F32)
    bw[:] = bias[1].astype(F32)
    drk[:] = jnp.zeros_like(drk)
    duw[:] = jnp.zeros_like(duw)
    st_out[:] = jnp.zeros_like(st_out)
    flip = (lax.broadcasted_iota(jnp.int32, (T, T), 0) + lax.broadcasted_iota(jnp.int32, (T, T), 1) == T - 1).astype(BF)
    for k in range(HC):
        for n in range(NT):
            rkr[k, n] = dot_nn(flip, rk[k, n]).astype(BF)

    def half_copy(k):
        return remote(drk.at[k, pl.ds(NA * (1 - core), NA)], pbuf.at[k], half_send.at[k], half_recv.at[k], partner)

    def part(src_chip, k, lo, size):
        return drk_out.at[HC * src_chip + k, pl.ds(NA * core + lo, size)]

    def fin_copy(k, s, arrived=False):
        piece = part(jnp.bitwise_xor(chip, s) if arrived else chip, k, 0, NA)
        rsem = fin_recv.at[k, s - 1] if s else table_recv
        return remote(piece, piece, table_send, rsem, jnp.bitwise_xor(me, neighbours[s]))

    def hop(k, s, whole):
        piece = part(jnp.bitwise_xor(chip, s), k, *((0, NA) if whole else (2 * (s - 1), 2)))
        return remote(piece, piece, table_send, hop_recv.at[k], jnp.bitwise_xor(me, neighbours[-s]))

    def hops(k, s):
        @pl.when(outer)
        def _():
            hop(k, s, False).start()

        if s == 1:
            @pl.when(~outer)
            def _():
                hop(k, s, True).start()

    def relay(k, s):
        piece = part(jnp.bitwise_xor(chip, s), k, 0, NA)
        return remote(piece, piece, table_send, table_recv, partner)

    def pass_on(k):
        for s in (1, 2):
            fin_copy(k, s, True).wait_recv()
            hops(k, s)
            relay(k, s).start()

    def sent_parts(dev, owner):
        there = dev // 2
        rows = ((there == 0) & (owner != 0)) | ((there == 1) & (owner == last))
        cols = ((there == last) & (owner != last)) | ((there == 2) & (owner == 0))
        return ((0, NA), ~rows & ~cols), ((2, 2), rows), ((0, 2), cols)

    def stat_copy(n, whole):
        if whole:
            return remote(st_out.at[n], st_in.at[0, n], st_send_all, st_recv.at[n], 4 + core)
        return remote(st_out.at[n, 1], st_in.at[chip, n, 1], st_send, st_recv.at[n], 6 + core)

    def after_softmax(n, i, m, inv, rd):
        first = jnp.where(chip == 0, 4, 6)

        @pl.when((i >= first) & (chip != last))
        def _():
            lane = lax.broadcasted_iota(jnp.int32, (T, H), 1)
            table = jnp.where(lane == 0, m, jnp.where(lane == 1, inv, rd)).T
            for r in range(2):
                @pl.when(i % 2 == r)
                def _():
                    st_out[n, i // 2 - 2, HC * r:HC * (r + 1)] = table[:HC]

        @pl.when((i == 6) & (chip != last))
        def _():
            stat_copy(n, False).start()

        @pl.when((i == 4) & (chip == 0))
        def _():
            stat_copy(n, True).start()

    def local_pair(x):
        owner = jnp.where(outer, x % HC + jnp.where(chip == 0, 1, 0), jnp.where(chip == 1, last, 0))
        n = jnp.where(outer, x // HC, x)
        return owner, n, 2 * core + n % 2, HC * owner + n // 2

    def local_loads(x, sl):
        _, n, bat, head = local_pair(x)
        copies = [pltpu.make_async_copy(rel.at[head, pl.ds(0, NA)], lrk.at[sl], l_sem.at[sl])]
        for a in range(NA):
            for r, src in enumerate((ins[a].at[bat, head], lx.at[a, n % 2, head])):
                where = core if r == 0 else 1 - core
                copies.append(pltpu.make_async_copy(src, lblk.at[sl, where, a], l_sem.at[sl]))
        return copies

    def local_send(x, c):
        sl = x % 2
        _, _, bat, head = local_pair(x)
        dst = out.at[pl.ds(2 * (c // 2), 2), bat, head]
        return remote(lres.at[sl, 1 - core], dst, lr_send.at[sl], lr_recv, partner)

    def local_work(lo, hi, c):
        for copy in local_loads(lo, lo % 2):
            copy.start()

        def one(x, _):
            sl = x % 2

            @pl.when(x + 1 < hi)
            def _():
                for copy in local_loads(x + 1, 1 - sl):
                    copy.start()

            pltpu.make_async_copy(rin.at[0, pl.ds(0, HC)], rin.at[0, pl.ds(0, HC)], l_sem.at[sl]).wait()

            @pl.when(x > 1)
            def _():
                local_send(x, c).wait_send()

            owner, n, bat, head = local_pair(x)
            u = bu[pl.ds(head, 1)]
            w = bw[pl.ds(head, 1)]
            q, do, key, val = [[lblk[sl, r, a] for r in range(2)] for a in range(NA)]
            table = lrk[sl]
            if c < 2:
                if c:
                    key = [rl[n, r, 0] for r in range(2)] + key
                    val = [rl[n, r, 1] for r in range(2)] + val
                for r in range(2):
                    upto = len(key) - 1 + r
                    res = row_tile(q[r], do[r], key[:upto], val[:upto], table, u, w)
                    for a in range(2):
                        lres[sl, r, a] = res[a]
            else:
                groups = (1,)
                piece = st_in.at[:, n, 1]
                if c != last:
                    groups = (0, 1)
                    piece = st_in.at[0, n]
                    q = q + [rl[n, r, 0] for r in range(2)]
                    do = do + [rl[n, r, 1] for r in range(2)]

                @pl.when((owner == 0) | (c != last))
                def _():
                    remote(piece, piece, st_send, st_recv.at[n], partner).wait_recv()

                stats = [st_in[owner, n, g] for g in groups]
                for a, res in enumerate(col_tiles(q, do, key, val, table, stats, u, w)):
                    for r in range(2):
                        lres[sl, r, a] = res[r]
            local_send(x, c).start()
            for a in range(2):
                out[2 * (c // 2) + a, bat, head] = lres[sl, core, a]
            return 0

        lax.fori_loop(lo, hi, one, 0)

    def local_count(c):
        return NU if c in (1, 2) else NU * HC

    @pl.when(chip == 0)
    def _():
        pair_wait(pl.ds(3, 9), "wait_recv")
        local_work(0, EARLY, 0)

    def send_tile(n, i):
        mask = jnp.bitwise_xor(me, i)
        for span, sent in sent_parts(i, chip):
            @pl.when((mask != 0) & sent)
            def _():
                some = pl.ds(*span)
                remote(rin.at[n, i, some], out.at[(some,) + pair_of(me, n)], out_send, out_recv, i).start()

        @pl.when(mask == 0)
        def _():
            for a in range(NA):
                out[(a,) + pair_of(me, n)] = rin[n, i, a]

    def run_unit(n, _):
        k = n // 2

        for g, group in enumerate(GROUPS):
            if g >= AHEAD:
                @pl.when(n == SEND_AT)
                def _():
                    send_group(*group)

            @pl.when(~outer & (n == FORWARD_AT[g]))
            def _():
                pass_forward(*group)

        @pl.when(n == 0)
        def _():
            pltpu.make_async_copy(rin.at[:, me], rin.at[:, me], in_loc).wait()

        for group in GROUPS:
            @pl.when(n == group[0])
            def _():
                arrive(*group)

        head = pl.ds(HC * chip + k, 1)
        unit(rin.at[n], rk.at[k], rkr.at[k], bu[head], bw[head], drk.at[k], duw.at[k], scratch,
             lambda i, m, inv, rd: after_softmax(n, i, m, inv, rd), lambda i: send_tile(n, i))

        @pl.when(n % 2 == 1)
        def _():
            copy = half_copy(k)
            copy.start()
            copy.wait()
            for r in range(NA):
                part(chip, k, r, 1)[0] = (drk[k, NA * core + r] + pbuf[k, r]).T
            for s in range(3):
                fin_copy(k, s).start()

        return 0

    lax.fori_loop(0, NU, run_unit, 0)

    pass_on(0)
    pass_on(1)

    for mask in range(1, NT):
        remote(duw, duw_all.at[me], duw_send, duw_recv, jnp.bitwise_xor(me, mask)).start()
    duw_all[me] = duw[:]

    def late_work(c, heads):
        if c:
            pair_wait(heads, "wait_recv")
        local_work(0 if c else EARLY, local_count(c), c)

    at_chip(late_work)
    pass_on(2)
    for k in range(HC):
        far = part(jnp.bitwise_xor(chip, last), k, 0, NA)
        remote(far, far, table_send, hop_recv.at[k], partner).wait_recv()
        relay(k, last).start()

    others = duw_all.at[pl.ds(0, NT - 1)]
    remote(others, others, duw_send, duw_recv, partner).wait()
    for h in range(NH):
        both = duw_all[2 * (h // HC), h % HC] + duw_all[2 * (h // HC) + 1, h % HC]
        for r, bias_out in enumerate((du_out, dw_out)):
            bias_out[h:h + 1] = both[r:r + 1]

    sent = rin.at[:, pl.ds(0, NT - 1)]
    remote(sent, sent, in_send, in_recv.at[0], partner).wait_send()
    sent = rin.at[:, pl.ds(0, 5)]
    remote(sent, sent, out_send, out_recv, partner).wait_send()
    for inner, count in ((True, 6), (False, 4)):
        @pl.when(outer != inner)
        def _():
            got = rin.at[:, pl.ds(0, count)]
            remote(got, got, out_send, out_recv, partner).wait_recv()

    @pl.when(~outer)
    def _():
        remote(rl, rl, fw_send, in_recv.at[0], partner).wait_send()

    @pl.when(chip != last)
    def _():
        some = st_out.at[:, 1]
        remote(some, some, st_send, st_recv.at[0], partner).wait_send()

    @pl.when(chip == 0)
    def _():
        remote(st_out, st_out, st_send_all, st_recv.at[0], partner).wait_send()

    def end_local(c, heads):
        pair_wait(heads, "wait_send")
        count = local_count(c)
        for x in (count - 2, count - 1):
            local_send(x, c).wait_send()
        whole = out.at[0, pl.ds(0, count // NU)]
        remote(whole, whole, lr_send.at[0], lr_recv, partner).wait_recv()

    at_chip(end_local)
    sent, got = drk_out.at[:, pl.ds(0, NT - 1)], drk_out.at[:, pl.ds(0, NA)]
    remote(sent, sent, table_send, table_recv, partner).wait_send()
    remote(got, got, table_send, table_recv, partner).wait_recv()


def exchange_attend(xq, xd, xk, xv, bias_u, bias_w, rel):
    any_spec = pl.BlockSpec(memory_space=pl.ANY)
    vmem_spec = pl.BlockSpec(memory_space=pltpu.VMEM)
    dma = pltpu.SemaphoreType.DMA
    acts = pltpu.VMEM((NA, NA, NH, T, D), BF)
    bias = pltpu.VMEM((NH, D), F32)
    heads = pltpu.VMEM((HC, NT, T, D), BF)
    per_pair = dma((NU,))
    per_head = dma((HC,))
    two = dma((2,))
    one = dma(())
    return pl.pallas_call(
        kernel,
        out_shape=(acts, pltpu.VMEM((NH, NT, T, D), F32), bias, bias,
                   jax.ShapeDtypeStruct((NA, 2, NH, T, D), BF)),
        in_specs=[any_spec] * 7,
        out_specs=(vmem_spec,) * 4 + (any_spec,),
        scratch_shapes=[
            pltpu.VMEM((NU, NT, NA, T, D), BF), pltpu.VMEM((NU, 2, 2, T, D), BF), pltpu.VMEM((HC, NT, D, T), F32),
            pltpu.VMEM((HC, NA, D, T), F32), pltpu.VMEM((HC, 8, D), F32), pltpu.VMEM((NT, HC, 8, D), F32),
            heads, heads, pltpu.VMEM((2, NH, D), BF), bias, bias,
            pltpu.VMEM((2, 2, NA, T, D), BF), pltpu.VMEM((2, NA, T, D), BF), pltpu.VMEM((2, 2, 2, T, D), BF),
            pltpu.VMEM((NU, 2, 8, T), F32), pltpu.VMEM((HC, NU, 2, 8, T), F32),
            per_pair, per_pair, per_pair, per_head, per_head, dma((HC, 2)), per_head, two, two]
        + [one] * 9 + [per_head] + [one] * 5
        + UNIT_SCRATCH,
        compiler_params=pltpu.CompilerParams(collective_id=0, has_side_effects=True, vmem_limit_bytes=VMEM_LIMIT),
    )(xq, xd, xk, xv, bias_u, bias_w, rel)


def write_kernel(acts, table, bias_u, bias_w, *refs):
    sem = refs[-1]
    srcs = [acts.at[a] for a in range(NA)] + [table, bias_u, bias_w]
    copies = [pltpu.make_async_copy(src, dst, sem.at[n]) for n, (src, dst) in enumerate(zip(srcs, refs[:-1]))]
    for copy in copies:
        copy.start()
    for copy in copies:
        copy.wait()


def write_out(arrs):
    shapes = [arrs[0].shape[1:]] * NA + [arr.shape for arr in arrs[1:]]
    types = [arrs[0].dtype] * NA + [arr.dtype for arr in arrs[1:]]
    return pl.pallas_call(
        write_kernel,
        out_shape=tuple(map(jax.ShapeDtypeStruct, shapes, types)),
        in_specs=[pl.BlockSpec(memory_space=pltpu.VMEM)] * len(arrs),
        out_specs=(pl.BlockSpec(memory_space=pl.ANY),) * len(shapes),
        scratch_shapes=[pltpu.SemaphoreType.DMA((len(shapes),))],
        compiler_params=pltpu.CompilerParams(vmem_limit_bytes=1024 * 1024),
    )(*[pltpu.with_memory_space_constraint(arr, pltpu.VMEM) for arr in arrs])


def solution(mesh):
    seq_spec = P(None, 'cp', None, None)

    def local(query, key_in, value, bias_u, bias_w, rel_k, d_out):
        def by_head(arr):
            return arr.transpose(0, 2, 1, 3)

        rel = rel_k.transpose(1, 0, 2).reshape(NH, NT, T, D)
        acts = [by_head(arr) for arr in (query, d_out, key_in, value)]
        res = write_out(exchange_attend(*acts, bias_u, bias_w, rel)[:4])
        d_rel = res[4].reshape(NH, NT * T, D).transpose(1, 0, 2)
        return tuple(by_head(arr) for arr in res[:4]) + (res[5], res[6], d_rel)

    return jax.shard_map(local, mesh=mesh,
                         in_specs=(seq_spec, seq_spec, seq_spec, P(), P(), P(), seq_spec),
                         out_specs=(seq_spec, seq_spec, seq_spec, seq_spec, P(), P(), P()),
                         check_vma=False)
```

```python
import jax
import jax.numpy as jnp
from jax import lax
from jax.experimental import pallas as pl
from jax.experimental.pallas import tpu as pltpu
from jax.sharding import PartitionSpec as P

T = 256
D = 128
H = 128
NT = 8
NU = 6
NA = 4
HC = 3
NH = 12
EARLY = 6
GROUPS = ((0, 1), (1, 1), (2, 2), (4, 2))
AHEAD = 3
SEND_AT = 1
FORWARD_AT = (0, 0, 1, 3)
VMEM_LIMIT = 39 * 1024 * 1024
F32 = jnp.float32
BF = jnp.bfloat16
SCALE = D ** -0.5
C2 = SCALE * 1.4426950408889634
MESH = pl.DeviceIdType.MESH


def dot_nt(lhs, rhs):
    return lax.dot_general(lhs, rhs, (((1,), (1,)), ((), ())), preferred_element_type=F32)


def row_max(arr):
    return jnp.max(arr, axis=1, keepdims=True)


def row_sum(arr):
    return jnp.sum(arr, axis=1, keepdims=True)


def dot_nn(lhs, rhs):
    return lax.dot_general(lhs, rhs, (((1,), (0,)), ((), ())), preferred_element_type=F32)


def unit(x, rk, rkr, u, w, drk, duw, scratch, after_softmax, after_tile):
    (s_ref, dp_ref, r_ref, mx_ref, l_ref, d_ref, u_ref, dk_ref, dv_ref, a_ref, c_ref, t_ref,
     oacc, qc_acc, qr_acc) = scratch
    nt = NT
    low = lower_mask()
    gather = gather_fn()
    dk_ref[:] = jnp.zeros_like(dk_ref)
    dv_ref[:] = jnp.zeros_like(dv_ref)

    def prep(i, sl):
        q = x[i, 0].astype(F32)
        a_ref[sl] = (q + u).astype(BF)
        c_ref[sl] = (q + w).astype(BF)
        mx_ref[:] = jnp.full((T, H), -jnp.inf, F32)
        r_ref[:] = jnp.full((2, T, H), -jnp.inf, F32)

    def logits(i, sl, n):
        j = i - n
        by = dot_nt(c_ref[sl], rkr[n])
        sc = dot_nt(a_ref[sl], x[j, 2])
        dp_ref[sl, j] = dot_nt(x[i, 1], x[j, 3])
        r0, r1 = [pltpu.roll(half, 1, 1, stride=1, stride_axis=0) for half in (by[:, :H], by[:, H:])]
        sc += shifted(low, r1, r0, r_ref[1], r_ref[0])
        r_ref[0] = r0
        r_ref[1] = r1
        s_ref[sl, j] = sc
        mx_ref[:] = jnp.maximum(mx_ref[:], jnp.maximum(sc[:, :H], sc[:, H:]))

    def softmax(i, sl):
        m = row_max(mx_ref[:])
        l_ref[:] = jnp.zeros_like(l_ref)
        d_ref[:] = jnp.zeros_like(d_ref)

        def body(j, _):
            p = jnp.exp2((s_ref[sl, j] - m) * C2)
            s_ref[sl, j] = p
            pd = p * dp_ref[sl, j]
            l_ref[:] += p[:, :H] + p[:, H:]
            d_ref[:] += pd[:, :H] + pd[:, H:]
            return 0

        lax.fori_loop(0, i + 1, body, 0)
        inv = 1.0 / row_sum(l_ref[:])
        rd = row_sum(d_ref[:]) * inv
        after_softmax(i, m, inv, rd)
        return inv, rd

    def grads(i, sl, j, inv, rd):
        pn = s_ref[sl, j] * inv
        pb = pn.astype(BF)
        ds = pn * (dp_ref[sl, j] - rd) * SCALE
        dsb = ds.astype(BF)
        oacc[:] += dot_nn(pb, x[j, 3])
        dv_ref[j] += dot_nn(t_ref[0], pb)
        qc_acc[:] += dot_nn(dsb, x[j, 2])
        dk_ref[j] += dot_nn(t_ref[1], dsb)
        g0, g1 = gather(ds)
        dist = shifted(low, g0, g1, u_ref[0], u_ref[1]).astype(BF)
        u_ref[0] = g0
        u_ref[1] = g1
        qr_acc[:] += dot_nn(dist, rk[i - j])
        drk[i - j] += dot_nn(t_ref[2], dist)

    prep(nt - 1, (nt - 1) % 2)

    def first(n, _):
        logits(nt - 1, (nt - 1) % 2, n)
        return 0

    lax.fori_loop(0, nt, first, 0)

    def tile(ii, _):
        i = nt - 1 - ii
        sl = i % 2
        inv, rd = softmax(i, sl)
        nxt = jnp.maximum(i - 1, 0)
        t_ref[0] = x[i, 1].T
        t_ref[1] = a_ref[sl].T
        t_ref[2] = c_ref[sl].T
        for acc in (oacc, qc_acc, qr_acc, u_ref):
            acc[:] = jnp.zeros_like(acc)
        prep(nxt, 1 - sl)

        def both(n, _):
            grads(i, sl, n, inv, rd)
            logits(nxt, 1 - sl, n)
            return 0

        lax.fori_loop(0, i, both, 0)
        grads(i, sl, i, inv, rd)
        qc = qc_acc[:]
        qr = qr_acc[:]
        for r, part in enumerate((qc, qr)):
            duw[r:r + 1] += jnp.sum(part, axis=0, keepdims=True)
        for r, res in enumerate((oacc[:], qc + qr, dk_ref[i].T, dv_ref[i].T)):
            x[i, r] = res.astype(BF)
        after_tile(i)
        return 0

    lax.fori_loop(0, nt, tile, 0)


def gather_fn():
    idx = (lax.broadcasted_iota(jnp.int32, (T, H), 0) - lax.broadcasted_iota(jnp.int32, (T, H), 1)) & (H - 1)

    def gather(arr):
        return [jnp.take_along_axis(half, idx, axis=1, mode="promise_in_bounds") for half in (arr[:, :H], arr[:, H:])]

    return gather


def lower_mask():
    return lax.broadcasted_iota(jnp.int32, (H, H), 1) <= lax.broadcasted_iota(jnp.int32, (H, H), 0)


def shifted(low, n0, n1, p0, p1):
    lo = jnp.concatenate([jnp.where(low, n0[:H], p1[:H]), jnp.where(low, n1[H:], n0[H:])], 0)
    hi = jnp.concatenate([jnp.where(low, p1[:H], p0[:H]), jnp.where(low, n0[H:], p1[H:])], 0)
    return jnp.concatenate([lo, hi], 1)


def row_tile(q, d_out, keys, vals, rk, u, w):
    last = len(keys) - 1
    low = lower_mask()
    gather = gather_fn()
    qf = q.astype(F32)
    a = (qf + u).astype(BF)
    c = (qf + w).astype(BF)
    by = [gather(dot_nt(c, rk[n])) for n in range(last + 1)]
    none = [jnp.full((T, H), -jnp.inf, F32)] * 2
    s = [dot_nt(a, key) + shifted(low, *by[last - j], *(by[last - j - 1] if j < last else none)) for j, key in enumerate(keys)]
    top = s[0]
    for other in s[1:]:
        top = jnp.maximum(top, other)
    m = row_max(top)
    p = [jnp.exp2((sj - m) * C2) for sj in s]
    dp = [dot_nt(d_out, val) for val in vals]
    inv = 1.0 / row_sum(sum(p))
    row_dot = row_sum(sum(pj * dj for pj, dj in zip(p, dp))) * inv
    out, d_q, prev = 0.0, 0.0, [jnp.zeros((T, H), F32)] * 2
    for j in range(last + 1):
        pn = p[j] * inv
        ds = pn * (dp[j] - row_dot) * SCALE
        out += dot_nn(pn.astype(BF), vals[j])
        mine = gather(ds)
        dist = shifted(low, *mine, *prev).astype(BF)
        prev = mine
        d_q += dot_nn(ds.astype(BF), keys[j]) + dot_nn(dist, rk[last - j])
    return out.astype(BF), d_q.astype(BF)


def col_tiles(qs, d_outs, keys, vals, rk, stats, u, w):
    low = lower_mask()
    gather = gather_fn()
    none = [jnp.full((T, H), -jnp.inf, F32)] * 2
    d_keys, d_vals = [0.0, 0.0], [0.0, 0.0]
    for i in range(len(qs)):
        qf = qs[i].astype(F32)
        a = (qf + u).astype(BF)
        c = (qf + w).astype(BF)
        by = {n: gather(dot_nt(c, rk[n])) for n in range(max(i - 2, 0), i + 1)}
        if i % 2 == 0:
            cols = jnp.concatenate([stats[i // 2], jnp.zeros((H - 8, T), F32)], 0).T
        m, inv, row_dot = [cols[:, r:r + 1] for r in range(HC * (i % 2), HC * (i % 2 + 1))]
        at, dot = a.T, d_outs[i].T
        for r in range(min(i + 1, 2)):
            n = i - r
            s = dot_nt(a, keys[r]) + shifted(low, *by[n], *(by[n - 1] if n else none))
            pn = jnp.exp2((s - m) * C2) * inv
            ds = pn * (dot_nt(d_outs[i], vals[r]) - row_dot) * SCALE
            d_vals[r] += dot_nn(dot, pn.astype(BF))
            d_keys[r] += dot_nn(at, ds.astype(BF))
    return [dk.T.astype(BF) for dk in d_keys], [dv.T.astype(BF) for dv in d_vals]


UNIT_SCRATCH = (
    [pltpu.VMEM((2, NT, T, T), F32)] * 2 + [pltpu.VMEM((2, T, H), F32)] + [pltpu.VMEM((T, H), F32)] * 3
    + [pltpu.VMEM((2, T, H), F32)] + [pltpu.VMEM((NT, D, T), F32)] * 2 + [pltpu.VMEM((2, T, D), BF)] * 2
    + [pltpu.VMEM((3, D, T), BF)] + [pltpu.VMEM((T, D), F32)] * 3)


def kernel(xq, xd, xk, xv, bias_u, bias_w, rel, out, drk_out, du_out, dw_out, lx,
           rin, rl, drk, pbuf, duw, duw_all, rk, rkr, bias, bu, bw, lblk, lrk, lres, st_out, st_in,
           in_recv, rl_recv, st_recv, half_send, half_recv, fin_recv, hop_recv, l_sem, lr_send,
           in_send, in_loc, fw_send, out_send, out_recv, table_send, table_recv, duw_send, duw_recv, rk_sem, px_send,
           px_recv, st_send, st_send_all, lr_recv, *scratch):
    me = lax.axis_index('cp')
    chip = me // 2
    core = me % 2
    last = NA - 1
    partner = jnp.bitwise_xor(me, 1)
    outer = (chip == 0) | (chip == last)
    ins = (xq, xd, xk, xv)
    neighbours = (1, 2, 4)

    def remote(src, dst, ssem, rsem, dev):
        return pltpu.make_async_remote_copy(src_ref=src, dst_ref=dst, send_sem=ssem, recv_sem=rsem,
                                            device_id=(dev,), device_id_type=MESH)

    def pair_of(dev, n):
        return 2 * (dev % 2) + n % 2, HC * (dev // 2) + n // 2

    def spot(a, dev, n):
        return ins[a].at[pair_of(dev, n)]

    def pairs(n, count):
        return pl.ds(n, count) if count > 1 else n

    def send_in(n, count, mask):
        dev = jnp.bitwise_xor(me, mask)
        bat, head = pair_of(dev, n)

        def send(first, via):
            for a in (first, first + 1):
                if via:
                    dst, rsem, to = rl.at[pairs(n, count), core, a % 2], rl_recv.at[n], jnp.bitwise_xor(dev, 4)
                else:
                    dst, rsem, to = rin.at[pairs(n, count), me, a], in_recv.at[n], dev
                remote(ins[a].at[pairs(bat, count), head], dst, in_send, rsem, to).start()

        for first in (0, 2):
            if mask < NU:
                send(first, False)
            else:
                through = chip == (0 if first else last)
                for via in (True, False):
                    @pl.when(through == via)
                    def _():
                        send(first, via)

    def send_group(n, count):
        for mask in (6, 2, 4, 7, 3, 5, 1):
            send_in(n, count, mask)

    def forward(n, count):
        dst = rin.at[pairs(n, count), pl.ds(2 * jnp.bitwise_xor(chip, 1), 2), pl.ds(2 * (chip % 2), 2)]
        return remote(rl.at[pairs(n, count)], dst, fw_send, in_recv.at[n], jnp.bitwise_xor(me, 4))

    def pass_forward(n, count):
        piece = rl.at[pairs(n, count)]
        remote(piece, piece, fw_send, rl_recv.at[n], jnp.bitwise_xor(me, 2)).wait_recv()
        forward(n, count).start()

    def arrive(n, count):
        piece = rin.at[pairs(n, count), pl.ds(0, NT - 1)]
        remote(piece, piece, in_send, in_recv.at[n], partner).wait_recv()

    def at_chip(act):
        for c, heads in enumerate(((3, 9), (9, 3), (0, 3), (0, 9))):
            @pl.when(chip == c)
            def _():
                act(c, pl.ds(*heads))

    def pair_wait(heads, wait):
        piece = lx.at[:, :, heads]
        getattr(remote(piece, piece, px_send, px_recv, partner), wait)()

    def pair_copies(heads):
        return [remote(ins[a].at[pl.ds(2 * (1 - core), 2), heads], lx.at[a, :, heads], px_send, px_recv, partner)
                for a in range(NA)]

    barrier = pltpu.get_barrier_semaphore()
    for mask in range(1, NT):
        pl.semaphore_signal(barrier, inc=1, device_id=(jnp.bitwise_xor(me, mask),), device_id_type=MESH)
    copies = [pltpu.make_async_copy(bias_u, bias.at[0], rk_sem.at[0]), pltpu.make_async_copy(bias_w, bias.at[1], rk_sem.at[1]),
              pltpu.make_async_copy(rel.at[pl.ds(HC * chip, HC)], rk, rk_sem.at[2])]
    for copy in copies:
        copy.start()
    for n in range(NU):
        for a in range(NA):
            pltpu.make_async_copy(spot(a, me, n), rin.at[n, me, a], in_loc).start()
    pl.semaphore_wait(barrier, NT - 1)
    for g, (n, count) in enumerate(GROUPS):
        if g < AHEAD:
            send_group(n, count)
        if g == 0:
            at_chip(lambda c, heads: [copy.start() for copy in pair_copies(heads)])

    for copy in copies:
        copy.wait()
    bu[:] = bias[0].astype(F32)
    bw[:] = bias[1].astype(F32)
    drk[:] = jnp.zeros_like(drk)
    duw[:] = jnp.zeros_like(duw)
    st_out[:] = jnp.zeros_like(st_out)
    flip = (lax.broadcasted_iota(jnp.int32, (T, T), 0) + lax.broadcasted_iota(jnp.int32, (T, T), 1) == T - 1).astype(BF)
    for k in range(HC):
        for n in range(NT):
            rkr[k, n] = dot_nn(flip, rk[k, n]).astype(BF)

    def half_copy(k):
        return remote(drk.at[k, pl.ds(NA * (1 - core), NA)], pbuf.at[k], half_send.at[k], half_recv.at[k], partner)

    def part(src_chip, k, lo, size):
        return drk_out.at[HC * src_chip + k, pl.ds(NA * core + lo, size)]

    def fin_copy(k, s, arrived=False):
        piece = part(jnp.bitwise_xor(chip, s) if arrived else chip, k, 0, NA)
        rsem = fin_recv.at[k, s - 1] if s else table_recv
        return remote(piece, piece, table_send, rsem, jnp.bitwise_xor(me, neighbours[s]))

    def hop(k, s, whole):
        piece = part(jnp.bitwise_xor(chip, s), k, *((0, NA) if whole else (2 * (s - 1), 2)))
        return remote(piece, piece, table_send, hop_recv.at[k], jnp.bitwise_xor(me, neighbours[-s]))

    def hops(k, s):
        @pl.when(outer)
        def _():
            hop(k, s, False).start()

        if s == 1:
            @pl.when(~outer)
            def _():
                hop(k, s, True).start()

    def relay(k, s):
        piece = part(jnp.bitwise_xor(chip, s), k, 0, NA)
        return remote(piece, piece, table_send, table_recv, partner)

    def pass_on(k):
        for s in (1, 2):
            fin_copy(k, s, True).wait_recv()
            hops(k, s)
            relay(k, s).start()

    def sent_parts(dev, owner):
        there = dev // 2
        rows = ((there == 0) & (owner != 0)) | ((there == 1) & (owner == last))
        cols = ((there == last) & (owner != last)) | ((there == 2) & (owner == 0))
        return ((0, NA), ~rows & ~cols), ((2, 2), rows), ((0, 2), cols)

    def stat_copy(n, whole):
        if whole:
            return remote(st_out.at[n], st_in.at[0, n], st_send_all, st_recv.at[n], 4 + core)
        return remote(st_out.at[n, 1], st_in.at[chip, n, 1], st_send, st_recv.at[n], 6 + core)

    def after_softmax(n, i, m, inv, rd):
        first = jnp.where(chip == 0, 4, 6)

        @pl.when((i >= first) & (chip != last))
        def _():
            lane = lax.broadcasted_iota(jnp.int32, (T, H), 1)
            table = jnp.where(lane == 0, m, jnp.where(lane == 1, inv, rd)).T
            for r in range(2):
                @pl.when(i % 2 == r)
                def _():
                    st_out[n, i // 2 - 2, HC * r:HC * (r + 1)] = table[:HC]

    def local_pair(x):
        owner = jnp.where(outer, x % HC + jnp.where(chip == 0, 1, 0), jnp.where(chip == 1, last, 0))
        n = jnp.where(outer, x // HC, x)
        return owner, n, 2 * core + n % 2, HC * owner + n // 2

    def local_loads(x, sl):
        _, n, bat, head = local_pair(x)
        copies = [pltpu.make_async_copy(rel.at[head, pl.ds(0, NA)], lrk.at[sl], l_sem.at[sl])]
        for a in range(NA):
            for r, src in enumerate((ins[a].at[bat, head], lx.at[a, n % 2, head])):
                where = core if r == 0 else 1 - core
                copies.append(pltpu.make_async_copy(src, lblk.at[sl, where, a], l_sem.at[sl]))
        return copies

    def local_send(x, c):
        sl = x % 2
        _, _, bat, head = local_pair(x)
        dst = out.at[pl.ds(2 * (c // 2), 2), bat, head]
        return remote(lres.at[sl, 1 - core], dst, lr_send.at[sl], lr_recv, partner)

    def local_work(lo, hi, c):
        for copy in local_loads(lo, lo % 2):
            copy.start()

        def one(x, _):
            sl = x % 2

            @pl.when(x + 1 < hi)
            def _():
                for copy in local_loads(x + 1, 1 - sl):
                    copy.start()

            pltpu.make_async_copy(rin.at[0, pl.ds(0, HC)], rin.at[0, pl.ds(0, HC)], l_sem.at[sl]).wait()

            @pl.when(x > 1)
            def _():
                local_send(x, c).wait_send()

            owner, n, bat, head = local_pair(x)
            u = bu[pl.ds(head, 1)]
            w = bw[pl.ds(head, 1)]
            q, do, key, val = [[lblk[sl, r, a] for r in range(2)] for a in range(NA)]
            table = lrk[sl]
            if c < 2:
                if c:
                    key = [rl[n, r, 0] for r in range(2)] + key
                    val = [rl[n, r, 1] for r in range(2)] + val
                for r in range(2):
                    upto = len(key) - 1 + r
                    res = row_tile(q[r], do[r], key[:upto], val[:upto], table, u, w)
                    for a in range(2):
                        lres[sl, r, a] = res[a]
            else:
                groups = (1,)
                piece = st_in.at[:, n, 1]
                if c != last:
                    groups = (0, 1)
                    piece = st_in.at[0, n]
                    q = q + [rl[n, r, 0] for r in range(2)]
                    do = do + [rl[n, r, 1] for r in range(2)]

                @pl.when((owner == 0) | (c != last))
                def _():
                    remote(piece, piece, st_send, st_recv.at[n], partner).wait_recv()

                stats = [st_in[owner, n, g] for g in groups]
                for a, res in enumerate(col_tiles(q, do, key, val, table, stats, u, w)):
                    for r in range(2):
                        lres[sl, r, a] = res[r]
            for a in range(2):
                out[2 * (c // 2) + a, bat, head] = lres[sl, core, a]
            local_send(x, c).start()
            return 0

        lax.fori_loop(lo, hi, one, 0)

    def local_count(c):
        return NU if c in (1, 2) else NU * HC

    @pl.when(chip == 0)
    def _():
        pair_wait(pl.ds(3, 9), "wait_recv")
        local_work(0, EARLY, 0)

    def send_tile(n, i):
        mask = jnp.bitwise_xor(me, i)
        for tile, whole, chips in ((6, False, chip != last), (4, True, chip == 0)):
            @pl.when((i == tile) & chips)
            def _():
                stat_copy(n, whole).start()

        for span, sent in sent_parts(i, chip):
            @pl.when((mask != 0) & sent)
            def _():
                some = pl.ds(*span)
                remote(rin.at[n, i, some], out.at[(some,) + pair_of(me, n)], out_send, out_recv, i).start()

        @pl.when(mask == 0)
        def _():
            for a in range(NA):
                out[(a,) + pair_of(me, n)] = rin[n, i, a]

    def run_unit(n, _):
        k = n // 2

        for g, group in enumerate(GROUPS):
            if g >= AHEAD:
                @pl.when(n == SEND_AT)
                def _():
                    send_group(*group)

            @pl.when(~outer & (n == FORWARD_AT[g]))
            def _():
                pass_forward(*group)

        @pl.when(n == 0)
        def _():
            pltpu.make_async_copy(rin.at[:, me], rin.at[:, me], in_loc).wait()

        for group in GROUPS:
            @pl.when(n == group[0])
            def _():
                arrive(*group)

        head = pl.ds(HC * chip + k, 1)
        unit(rin.at[n], rk.at[k], rkr.at[k], bu[head], bw[head], drk.at[k], duw.at[k], scratch,
             lambda i, m, inv, rd: after_softmax(n, i, m, inv, rd), lambda i: send_tile(n, i))

        @pl.when(n % 2 == 1)
        def _():
            copy = half_copy(k)
            copy.start()
            copy.wait()
            for r in range(NA):
                part(chip, k, r, 1)[0] = (drk[k, NA * core + r] + pbuf[k, r]).T
            for s in range(3):
                fin_copy(k, s).start()

        return 0

    lax.fori_loop(0, NU, run_unit, 0)

    pass_on(0)
    pass_on(1)

    for mask in range(1, NT):
        remote(duw, duw_all.at[me], duw_send, duw_recv, jnp.bitwise_xor(me, mask)).start()
    duw_all[me] = duw[:]

    def late_work(c, heads):
        if c:
            pair_wait(heads, "wait_recv")
        local_work(0 if c else EARLY, local_count(c), c)

    at_chip(late_work)
    pass_on(2)
    for k in range(HC):
        far = part(jnp.bitwise_xor(chip, last), k, 0, NA)
        remote(far, far, table_send, hop_recv.at[k], partner).wait_recv()
        relay(k, last).start()

    others = duw_all.at[pl.ds(0, NT - 1)]
    remote(others, others, duw_send, duw_recv, partner).wait()
    for h in range(NH):
        both = duw_all[2 * (h // HC), h % HC] + duw_all[2 * (h // HC) + 1, h % HC]
        for r, bias_out in enumerate((du_out, dw_out)):
            bias_out[h:h + 1] = both[r:r + 1]

    sent = rin.at[:, pl.ds(0, NT - 1)]
    remote(sent, sent, in_send, in_recv.at[0], partner).wait_send()
    sent = rin.at[:, pl.ds(0, 5)]
    remote(sent, sent, out_send, out_recv, partner).wait_send()
    for inner, count in ((True, 6), (False, 4)):
        @pl.when(outer != inner)
        def _():
            got = rin.at[:, pl.ds(0, count)]
            remote(got, got, out_send, out_recv, partner).wait_recv()

    @pl.when(~outer)
    def _():
        remote(rl, rl, fw_send, in_recv.at[0], partner).wait_send()

    @pl.when(chip != last)
    def _():
        some = st_out.at[:, 1]
        remote(some, some, st_send, st_recv.at[0], partner).wait_send()

    @pl.when(chip == 0)
    def _():
        remote(st_out, st_out, st_send_all, st_recv.at[0], partner).wait_send()

    def end_local(c, heads):
        pair_wait(heads, "wait_send")
        count = local_count(c)
        for x in (count - 2, count - 1):
            local_send(x, c).wait_send()
        whole = out.at[0, pl.ds(0, count // NU)]
        remote(whole, whole, lr_send.at[0], lr_recv, partner).wait_recv()

    at_chip(end_local)
    sent, got = drk_out.at[:, pl.ds(0, NT - 1)], drk_out.at[:, pl.ds(0, NA)]
    remote(sent, sent, table_send, table_recv, partner).wait_send()
    remote(got, got, table_send, table_recv, partner).wait_recv()


def exchange_attend(xq, xd, xk, xv, bias_u, bias_w, rel):
    any_spec = pl.BlockSpec(memory_space=pl.ANY)
    vmem_spec = pl.BlockSpec(memory_space=pltpu.VMEM)
    dma = pltpu.SemaphoreType.DMA
    acts = pltpu.VMEM((NA, NA, NH, T, D), BF)
    bias = pltpu.VMEM((NH, D), F32)
    heads = pltpu.VMEM((HC, NT, T, D), BF)
    per_pair = dma((NU,))
    per_head = dma((HC,))
    two = dma((2,))
    one = dma(())
    return pl.pallas_call(
        kernel,
        out_shape=(acts, pltpu.VMEM((NH, NT, T, D), F32), bias, bias,
                   jax.ShapeDtypeStruct((NA, 2, NH, T, D), BF)),
        in_specs=[any_spec] * 7,
        out_specs=(vmem_spec,) * 4 + (any_spec,),
        scratch_shapes=[
            pltpu.VMEM((NU, NT, NA, T, D), BF), pltpu.VMEM((NU, 2, 2, T, D), BF), pltpu.VMEM((HC, NT, D, T), F32),
            pltpu.VMEM((HC, NA, D, T), F32), pltpu.VMEM((HC, 8, D), F32), pltpu.VMEM((NT, HC, 8, D), F32),
            heads, heads, pltpu.VMEM((2, NH, D), BF), bias, bias,
            pltpu.VMEM((2, 2, NA, T, D), BF), pltpu.VMEM((2, NA, T, D), BF), pltpu.VMEM((2, 2, 2, T, D), BF),
            pltpu.VMEM((NU, 2, 8, T), F32), pltpu.VMEM((HC, NU, 2, 8, T), F32),
            per_pair, per_pair, per_pair, per_head, per_head, dma((HC, 2)), per_head, two, two]
        + [one] * 9 + [per_head] + [one] * 5
        + UNIT_SCRATCH,
        compiler_params=pltpu.CompilerParams(collective_id=0, has_side_effects=True, vmem_limit_bytes=VMEM_LIMIT),
    )(xq, xd, xk, xv, bias_u, bias_w, rel)


def write_kernel(acts, table, bias_u, bias_w, *refs):
    sem = refs[-1]
    srcs = [acts.at[a] for a in range(NA)] + [table, bias_u, bias_w]
    copies = [pltpu.make_async_copy(src, dst, sem.at[n]) for n, (src, dst) in enumerate(zip(srcs, refs[:-1]))]
    for copy in copies:
        copy.start()
    for copy in copies:
        copy.wait()


def write_out(arrs):
    shapes = [arrs[0].shape[1:]] * NA + [arr.shape for arr in arrs[1:]]
    types = [arrs[0].dtype] * NA + [arr.dtype for arr in arrs[1:]]
    return pl.pallas_call(
        write_kernel,
        out_shape=tuple(map(jax.ShapeDtypeStruct, shapes, types)),
        in_specs=[pl.BlockSpec(memory_space=pltpu.VMEM)] * len(arrs),
        out_specs=(pl.BlockSpec(memory_space=pl.ANY),) * len(shapes),
        scratch_shapes=[pltpu.SemaphoreType.DMA((len(shapes),))],
        compiler_params=pltpu.CompilerParams(vmem_limit_bytes=1024 * 1024),
    )(*[pltpu.with_memory_space_constraint(arr, pltpu.VMEM) for arr in arrs])


def solution(mesh):
    seq_spec = P(None, 'cp', None, None)

    def local(query, key_in, value, bias_u, bias_w, rel_k, d_out):
        def by_head(arr):
            return arr.transpose(0, 2, 1, 3)

        rel = rel_k.transpose(1, 0, 2).reshape(NH, NT, T, D)
        acts = [by_head(arr) for arr in (query, d_out, key_in, value)]
        res = write_out(exchange_attend(*acts, bias_u, bias_w, rel)[:4])
        d_rel = res[4].reshape(NH, NT * T, D).transpose(1, 0, 2)
        return tuple(by_head(arr) for arr in res[:4]) + (res[5], res[6], d_rel)

    return jax.shard_map(local, mesh=mesh,
                         in_specs=(seq_spec, seq_spec, seq_spec, P(), P(), P(), seq_spec),
                         out_specs=(seq_spec, seq_spec, seq_spec, seq_spec, P(), P(), P()),
                         check_vma=False)
```

```python
import jax
import jax.numpy as jnp
from jax import lax
from jax.experimental import pallas as pl
from jax.experimental.pallas import tpu as pltpu
from jax.sharding import PartitionSpec as P

T = 256
D = 128
H = 128
NT = 8
NU = 6
NA = 4
HC = 3
HALF = 1024
CUT = 480
NH = 12
EARLY = 6
GROUPS = ((0, 1), (1, 1), (2, 2), (4, 2))
AHEAD = 3
SEND_AT = 1
FORWARD_AT = (0, 0, 1, 3)
VMEM_LIMIT = 39 * 1024 * 1024
F32 = jnp.float32
BF = jnp.bfloat16
SCALE = D ** -0.5
C2 = SCALE * 1.4426950408889634
MESH = pl.DeviceIdType.MESH


def dot_nt(lhs, rhs):
    return lax.dot_general(lhs, rhs, (((1,), (1,)), ((), ())), preferred_element_type=F32)


def row_max(arr):
    return jnp.max(arr, axis=1, keepdims=True)


def row_sum(arr):
    return jnp.sum(arr, axis=1, keepdims=True)


def dot_nn(lhs, rhs):
    return lax.dot_general(lhs, rhs, (((1,), (0,)), ((), ())), preferred_element_type=F32)


def unit(x, rk, rkr, u, w, drk, duw, scratch, after_softmax, after_tile):
    (s_ref, dp_ref, r_ref, mx_ref, l_ref, d_ref, u_ref, dk_ref, dv_ref, a_ref, c_ref, t_ref,
     oacc, qc_acc, qr_acc) = scratch
    nt = NT
    low = lower_mask()
    gather = gather_fn()
    dk_ref[:] = jnp.zeros_like(dk_ref)
    dv_ref[:] = jnp.zeros_like(dv_ref)

    def prep(i, sl):
        q = x[i, 0].astype(F32)
        a_ref[sl] = (q + u).astype(BF)
        c_ref[sl] = (q + w).astype(BF)
        mx_ref[:] = jnp.full((T, H), -jnp.inf, F32)
        r_ref[:] = jnp.full((2, T, H), -jnp.inf, F32)

    def logits(i, sl, n):
        j = i - n
        by = dot_nt(c_ref[sl], rkr[n])
        sc = dot_nt(a_ref[sl], x[j, 2])
        dp_ref[sl, j] = dot_nt(x[i, 1], x[j, 3])
        r0, r1 = [pltpu.roll(half, 1, 1, stride=1, stride_axis=0) for half in (by[:, :H], by[:, H:])]
        sc += shifted(low, r1, r0, r_ref[1], r_ref[0])
        r_ref[0] = r0
        r_ref[1] = r1
        s_ref[sl, j] = sc
        mx_ref[:] = jnp.maximum(mx_ref[:], jnp.maximum(sc[:, :H], sc[:, H:]))

    def softmax(i, sl):
        m = row_max(mx_ref[:])
        l_ref[:] = jnp.zeros_like(l_ref)
        d_ref[:] = jnp.zeros_like(d_ref)

        def body(j, _):
            p = jnp.exp2((s_ref[sl, j] - m) * C2)
            s_ref[sl, j] = p
            pd = p * dp_ref[sl, j]
            l_ref[:] += p[:, :H] + p[:, H:]
            d_ref[:] += pd[:, :H] + pd[:, H:]
            return 0

        lax.fori_loop(0, i + 1, body, 0)
        inv = 1.0 / row_sum(l_ref[:])
        rd = row_sum(d_ref[:]) * inv
        after_softmax(i, m, inv, rd)
        return inv, rd

    def grads(i, sl, j, inv, rd):
        pn = s_ref[sl, j] * inv
        pb = pn.astype(BF)
        ds = pn * (dp_ref[sl, j] - rd) * SCALE
        dsb = ds.astype(BF)
        oacc[:] += dot_nn(pb, x[j, 3])
        dv_ref[j] += dot_nn(t_ref[0], pb)
        qc_acc[:] += dot_nn(dsb, x[j, 2])
        dk_ref[j] += dot_nn(t_ref[1], dsb)
        g0, g1 = gather(ds)
        dist = shifted(low, g0, g1, u_ref[0], u_ref[1]).astype(BF)
        u_ref[0] = g0
        u_ref[1] = g1
        qr_acc[:] += dot_nn(dist, rk[i - j])
        drk[i - j] += dot_nn(t_ref[2], dist)

    prep(nt - 1, (nt - 1) % 2)

    def first(n, _):
        logits(nt - 1, (nt - 1) % 2, n)
        return 0

    lax.fori_loop(0, nt, first, 0)

    def tile(ii, _):
        i = nt - 1 - ii
        sl = i % 2
        inv, rd = softmax(i, sl)
        nxt = jnp.maximum(i - 1, 0)
        t_ref[0] = x[i, 1].T
        t_ref[1] = a_ref[sl].T
        t_ref[2] = c_ref[sl].T
        for acc in (oacc, qc_acc, qr_acc, u_ref):
            acc[:] = jnp.zeros_like(acc)
        prep(nxt, 1 - sl)

        def both(n, _):
            grads(i, sl, n, inv, rd)
            logits(nxt, 1 - sl, n)
            return 0

        lax.fori_loop(0, i, both, 0)
        grads(i, sl, i, inv, rd)
        qc = qc_acc[:]
        qr = qr_acc[:]
        for r, part in enumerate((qc, qr)):
            duw[r:r + 1] += jnp.sum(part, axis=0, keepdims=True)
        for r, res in enumerate((oacc[:], qc + qr, dk_ref[i].T, dv_ref[i].T)):
            x[i, r] = res.astype(BF)
        after_tile(i)
        return 0

    lax.fori_loop(0, nt, tile, 0)


def gather_fn():
    idx = (lax.broadcasted_iota(jnp.int32, (T, H), 0) - lax.broadcasted_iota(jnp.int32, (T, H), 1)) & (H - 1)

    def gather(arr):
        return [jnp.take_along_axis(half, idx, axis=1, mode="promise_in_bounds") for half in (arr[:, :H], arr[:, H:])]

    return gather


def lower_mask():
    return lax.broadcasted_iota(jnp.int32, (H, H), 1) <= lax.broadcasted_iota(jnp.int32, (H, H), 0)


def shifted(low, n0, n1, p0, p1):
    lo = jnp.concatenate([jnp.where(low, n0[:H], p1[:H]), jnp.where(low, n1[H:], n0[H:])], 0)
    hi = jnp.concatenate([jnp.where(low, p1[:H], p0[:H]), jnp.where(low, n0[H:], p1[H:])], 0)
    return jnp.concatenate([lo, hi], 1)


def row_tile(q, d_out, keys, vals, rk, u, w):
    last = len(keys) - 1
    low = lower_mask()
    gather = gather_fn()
    qf = q.astype(F32)
    a = (qf + u).astype(BF)
    c = (qf + w).astype(BF)
    by = [gather(dot_nt(c, rk[n])) for n in range(last + 1)]
    none = [jnp.full((T, H), -jnp.inf, F32)] * 2
    s = [dot_nt(a, key) + shifted(low, *by[last - j], *(by[last - j - 1] if j < last else none)) for j, key in enumerate(keys)]
    top = s[0]
    for other in s[1:]:
        top = jnp.maximum(top, other)
    m = row_max(top)
    p = [jnp.exp2((sj - m) * C2) for sj in s]
    dp = [dot_nt(d_out, val) for val in vals]
    inv = 1.0 / row_sum(sum(p))
    row_dot = row_sum(sum(pj * dj for pj, dj in zip(p, dp))) * inv
    out, d_q, prev = 0.0, 0.0, [jnp.zeros((T, H), F32)] * 2
    for j in range(last + 1):
        pn = p[j] * inv
        ds = pn * (dp[j] - row_dot) * SCALE
        out += dot_nn(pn.astype(BF), vals[j])
        mine = gather(ds)
        dist = shifted(low, *mine, *prev).astype(BF)
        prev = mine
        d_q += dot_nn(ds.astype(BF), keys[j]) + dot_nn(dist, rk[last - j])
    return out.astype(BF), d_q.astype(BF)


def col_tiles(qs, d_outs, keys, vals, rk, stats, u, w):
    low = lower_mask()
    gather = gather_fn()
    none = [jnp.full((T, H), -jnp.inf, F32)] * 2
    d_keys, d_vals = [0.0, 0.0], [0.0, 0.0]
    for i in range(len(qs)):
        qf = qs[i].astype(F32)
        a = (qf + u).astype(BF)
        c = (qf + w).astype(BF)
        by = {n: gather(dot_nt(c, rk[n])) for n in range(max(i - 2, 0), i + 1)}
        if i % 2 == 0:
            cols = jnp.concatenate([stats[i // 2], jnp.zeros((H - 8, T), F32)], 0).T
        m, inv, row_dot = [cols[:, r:r + 1] for r in range(HC * (i % 2), HC * (i % 2 + 1))]
        at, dot = a.T, d_outs[i].T
        for r in range(min(i + 1, 2)):
            n = i - r
            s = dot_nt(a, keys[r]) + shifted(low, *by[n], *(by[n - 1] if n else none))
            pn = jnp.exp2((s - m) * C2) * inv
            ds = pn * (dot_nt(d_outs[i], vals[r]) - row_dot) * SCALE
            d_vals[r] += dot_nn(dot, pn.astype(BF))
            d_keys[r] += dot_nn(at, ds.astype(BF))
    return [dk.T.astype(BF) for dk in d_keys], [dv.T.astype(BF) for dv in d_vals]


UNIT_SCRATCH = (
    [pltpu.VMEM((2, NT, T, T), F32)] * 2 + [pltpu.VMEM((2, T, H), F32)] + [pltpu.VMEM((T, H), F32)] * 3
    + [pltpu.VMEM((2, T, H), F32)] + [pltpu.VMEM((NT, D, T), F32)] * 2 + [pltpu.VMEM((2, T, D), BF)] * 2
    + [pltpu.VMEM((3, D, T), BF)] + [pltpu.VMEM((T, D), F32)] * 3)


def kernel(xq, xd, xk, xv, bias_u, bias_w, rel, out, drk_out, du_out, dw_out, lx,
           rin, rl, drk, pbuf, duw, duw_all, rk, rkr, bias, bu, bw, lblk, lrk, lres, st_out, st_in,
           in_recv, rl_recv, st_recv, half_send, half_recv, fin_recv, hop_recv, l_sem, lr_send,
           in_send, in_loc, fw_send, out_send, out_recv, table_send, table_recv, duw_send, duw_recv, rk_sem, px_send,
           px_recv, st_send, st_send_all, lr_recv, *scratch):
    me = lax.axis_index('cp')
    chip = me // 2
    core = me % 2
    last = NA - 1
    partner = jnp.bitwise_xor(me, 1)
    outer = (chip == 0) | (chip == last)
    ins = (xq, xd, xk, xv)
    neighbours = (1, 2, 4)

    def remote(src, dst, ssem, rsem, dev):
        return pltpu.make_async_remote_copy(src_ref=src, dst_ref=dst, send_sem=ssem, recv_sem=rsem,
                                            device_id=(dev,), device_id_type=MESH)

    def pair_of(dev, n):
        return 2 * (dev % 2) + n % 2, HC * (dev // 2) + n // 2

    def spot(a, dev, n):
        return ins[a].at[pair_of(dev, n)]

    def pairs(n, count):
        return pl.ds(n, count) if count > 1 else n

    def send_in(n, count, mask):
        dev = jnp.bitwise_xor(me, mask)
        bat, head = pair_of(dev, n)

        def send(first, via):
            for a in (first, first + 1):
                if via:
                    dst, rsem, to = rl.at[pairs(n, count), core, a % 2], rl_recv.at[n], jnp.bitwise_xor(dev, 4)
                else:
                    dst, rsem, to = rin.at[pairs(n, count), me, a], in_recv.at[n], dev
                remote(ins[a].at[pairs(bat, count), head], dst, in_send, rsem, to).start()

        for first in (0, 2):
            if mask < NU:
                send(first, False)
            else:
                through = chip == (0 if first else last)
                for via in (True, False):
                    @pl.when(through == via)
                    def _():
                        send(first, via)

    def send_group(n, count):
        for mask in (6, 2, 4, 7, 3, 5, 1):
            send_in(n, count, mask)

    def forward(n, count):
        dst = rin.at[pairs(n, count), pl.ds(2 * jnp.bitwise_xor(chip, 1), 2), pl.ds(2 * (chip % 2), 2)]
        return remote(rl.at[pairs(n, count)], dst, fw_send, in_recv.at[n], jnp.bitwise_xor(me, 4))

    def pass_forward(n, count):
        piece = rl.at[pairs(n, count)]
        remote(piece, piece, fw_send, rl_recv.at[n], jnp.bitwise_xor(me, 2)).wait_recv()
        forward(n, count).start()

    def arrive(n, count):
        piece = rin.at[pairs(n, count), pl.ds(0, NT - 1)]
        remote(piece, piece, in_send, in_recv.at[n], partner).wait_recv()

    def at_chip(act):
        for c, heads in enumerate(((3, 9), (9, 3), (0, 3), (0, 9))):
            @pl.when(chip == c)
            def _():
                act(c, pl.ds(*heads))

    def pair_wait(heads, wait):
        piece = lx.at[:, :, heads]
        getattr(remote(piece, piece, px_send, px_recv, partner), wait)()

    def pair_copies(heads):
        return [remote(ins[a].at[pl.ds(2 * (1 - core), 2), heads], lx.at[a, :, heads], px_send, px_recv, partner)
                for a in range(NA)]

    barrier = pltpu.get_barrier_semaphore()
    for mask in range(1, NT):
        pl.semaphore_signal(barrier, inc=1, device_id=(jnp.bitwise_xor(me, mask),), device_id_type=MESH)
    copies = [pltpu.make_async_copy(bias_u, bias.at[0], rk_sem.at[0]), pltpu.make_async_copy(bias_w, bias.at[1], rk_sem.at[1]),
              pltpu.make_async_copy(rel.at[pl.ds(HC * chip, HC)], rk, rk_sem.at[2])]
    for copy in copies:
        copy.start()
    for n in range(NU):
        for a in range(NA):
            pltpu.make_async_copy(spot(a, me, n), rin.at[n, me, a], in_loc).start()
    pl.semaphore_wait(barrier, NT - 1)
    for g, (n, count) in enumerate(GROUPS):
        if g < AHEAD:
            send_group(n, count)
        if g == 0:
            at_chip(lambda c, heads: [copy.start() for copy in pair_copies(heads)])

    for copy in copies:
        copy.wait()
    bu[:] = bias[0].astype(F32)
    bw[:] = bias[1].astype(F32)
    drk[:] = jnp.zeros_like(drk)
    duw[:] = jnp.zeros_like(duw)
    st_out[:] = jnp.zeros_like(st_out)
    flip = (lax.broadcasted_iota(jnp.int32, (T, T), 0) + lax.broadcasted_iota(jnp.int32, (T, T), 1) == T - 1).astype(BF)
    for k in range(HC):
        for n in range(NT):
            rkr[k, n] = dot_nn(flip, rk[k, n]).astype(BF)

    def half_copy(k):
        return remote(drk.at[k, pl.ds(NA * (1 - core), NA)], pbuf.at[k], half_send.at[k], half_recv.at[k], partner)

    def part(src_chip, k, lo=0, rows=HALF):
        return drk_out.at[HC * src_chip + k, pl.ds(HALF * core + lo, rows)]

    def fin_copy(k, s, arrived=False):
        piece = part(jnp.bitwise_xor(chip, s) if arrived else chip, k)
        rsem = fin_recv.at[k, s - 1] if s else table_recv
        return remote(piece, piece, table_send, rsem, jnp.bitwise_xor(me, neighbours[s]))

    even = ((0, HALF // 2), (HALF // 2, HALF // 2))
    uneven = ((0, CUT), (CUT, HALF - CUT))
    going = ((uneven[0], even[1]), ((0, HALF),), ((0, HALF),), (even[0], uneven[1]))
    coming = (((0, HALF),), even, uneven, ((0, HALF),))

    def each_span(spans, act):
        for c, here in enumerate(spans):
            @pl.when(chip == c)
            def _():
                act(here)

    def hop(k, s, span):
        piece = part(jnp.bitwise_xor(chip, s), k, *span)
        return remote(piece, piece, table_send, hop_recv.at[k, s - 1], jnp.bitwise_xor(me, neighbours[-s]))

    def relay(k, s, *span):
        piece = part(jnp.bitwise_xor(chip, s), k, *span)
        return remote(piece, piece, table_send, table_recv, partner)

    def far_relay(k):
        def act(spans):
            for r, span in enumerate(spans):
                piece = part(jnp.bitwise_xor(chip, last), k, *span)
                remote(piece, piece, table_send, hop_recv.at[k, r], partner).wait_recv()
                relay(k, last, *span).start()

        each_span(coming, act)

    def pass_on(k):
        for s in (1, 2):
            fin_copy(k, s, True).wait_recv()
            each_span(going, lambda spans: [hop(k, s, span).start() for span in spans[s - 1:s]])
            relay(k, s).start()

    def sent_parts(dev, owner):
        there = dev // 2
        rows = ((there == 0) & (owner != 0)) | ((there == 1) & (owner == last))
        cols = ((there == last) & (owner != last)) | ((there == 2) & (owner == 0))
        return ((0, NA), ~rows & ~cols), ((2, 2), rows), ((0, 2), cols)

    def stat_copy(n, whole):
        if whole:
            return remote(st_out.at[n], st_in.at[0, n], st_send_all, st_recv.at[n], 4 + core)
        return remote(st_out.at[n, 1], st_in.at[chip, n, 1], st_send, st_recv.at[n], 6 + core)

    def after_softmax(n, i, m, inv, rd):
        first = jnp.where(chip == 0, 4, 6)

        @pl.when((i >= first) & (chip != last))
        def _():
            lane = lax.broadcasted_iota(jnp.int32, (T, H), 1)
            table = jnp.where(lane == 0, m, jnp.where(lane == 1, inv, rd)).T
            for r in range(2):
                @pl.when(i % 2 == r)
                def _():
                    st_out[n, i // 2 - 2, HC * r:HC * (r + 1)] = table[:HC]

    def local_pair(x):
        owner = jnp.where(outer, x % HC + jnp.where(chip == 0, 1, 0), jnp.where(chip == 1, last, 0))
        n = jnp.where(outer, x // HC, x)
        return owner, n, 2 * core + n % 2, HC * owner + n // 2

    def local_loads(x, sl):
        _, n, bat, head = local_pair(x)
        copies = [pltpu.make_async_copy(rel.at[head, pl.ds(0, NA)], lrk.at[sl], l_sem.at[sl])]
        for a in range(NA):
            for r, src in enumerate((ins[a].at[bat, head], lx.at[a, n % 2, head])):
                where = core if r == 0 else 1 - core
                copies.append(pltpu.make_async_copy(src, lblk.at[sl, where, a], l_sem.at[sl]))
        return copies

    def local_send(x, c):
        sl = x % 2
        _, _, bat, head = local_pair(x)
        dst = out.at[pl.ds(2 * (c // 2), 2), bat, head]
        return remote(lres.at[sl, 1 - core], dst, lr_send.at[sl], lr_recv, partner)

    def local_work(lo, hi, c):
        for copy in local_loads(lo, lo % 2):
            copy.start()

        def one(x, _):
            sl = x % 2

            @pl.when(x + 1 < hi)
            def _():
                for copy in local_loads(x + 1, 1 - sl):
                    copy.start()

            pltpu.make_async_copy(rin.at[0, pl.ds(0, HC)], rin.at[0, pl.ds(0, HC)], l_sem.at[sl]).wait()

            @pl.when(x > 1)
            def _():
                local_send(x, c).wait_send()

            owner, n, bat, head = local_pair(x)
            u = bu[pl.ds(head, 1)]
            w = bw[pl.ds(head, 1)]
            q, do, key, val = [[lblk[sl, r, a] for r in range(2)] for a in range(NA)]
            table = lrk[sl]
            if c < 2:
                if c:
                    key = [rl[n, r, 0] for r in range(2)] + key
                    val = [rl[n, r, 1] for r in range(2)] + val
                for r in range(2):
                    upto = len(key) - 1 + r
                    res = row_tile(q[r], do[r], key[:upto], val[:upto], table, u, w)
                    for a in range(2):
                        lres[sl, r, a] = res[a]
            else:
                groups = (1,)
                piece = st_in.at[:, n, 1]
                if c != last:
                    groups = (0, 1)
                    piece = st_in.at[0, n]
                    q = q + [rl[n, r, 0] for r in range(2)]
                    do = do + [rl[n, r, 1] for r in range(2)]

                @pl.when((owner == 0) | (c != last))
                def _():
                    remote(piece, piece, st_send, st_recv.at[n], partner).wait_recv()

                stats = [st_in[owner, n, g] for g in groups]
                for a, res in enumerate(col_tiles(q, do, key, val, table, stats, u, w)):
                    for r in range(2):
                        lres[sl, r, a] = res[r]
            for a in range(2):
                out[2 * (c // 2) + a, bat, head] = lres[sl, core, a]
            local_send(x, c).start()
            return 0

        lax.fori_loop(lo, hi, one, 0)

    def local_count(c):
        return NU if c in (1, 2) else NU * HC

    @pl.when(chip == 0)
    def _():
        pair_wait(pl.ds(3, 9), "wait_recv")
        local_work(0, EARLY, 0)

    def send_tile(n, i):
        mask = jnp.bitwise_xor(me, i)
        for tile, whole, chips in ((6, False, chip != last), (4, True, chip == 0)):
            @pl.when((i == tile) & chips)
            def _():
                stat_copy(n, whole).start()

        for span, sent in sent_parts(i, chip):
            @pl.when((mask != 0) & sent)
            def _():
                some = pl.ds(*span)
                remote(rin.at[n, i, some], out.at[(some,) + pair_of(me, n)], out_send, out_recv, i).start()

        @pl.when(mask == 0)
        def _():
            for a in range(NA):
                out[(a,) + pair_of(me, n)] = rin[n, i, a]

    def run_unit(n, _):
        k = n // 2

        for g, group in enumerate(GROUPS):
            if g >= AHEAD:
                @pl.when(n == SEND_AT)
                def _():
                    send_group(*group)

            @pl.when(~outer & (n == FORWARD_AT[g]))
            def _():
                pass_forward(*group)

        @pl.when(n == 0)
        def _():
            pltpu.make_async_copy(rin.at[:, me], rin.at[:, me], in_loc).wait()

        for group in GROUPS:
            @pl.when(n == group[0])
            def _():
                arrive(*group)

        head = pl.ds(HC * chip + k, 1)
        unit(rin.at[n], rk.at[k], rkr.at[k], bu[head], bw[head], drk.at[k], duw.at[k], scratch,
             lambda i, m, inv, rd: after_softmax(n, i, m, inv, rd), lambda i: send_tile(n, i))

        @pl.when(n % 2 == 1)
        def _():
            copy = half_copy(k)
            copy.start()
            copy.wait()
            for r in range(NA):
                part(chip, k, r * T, T)[:] = (drk[k, NA * core + r] + pbuf[k, r]).T
            for s in range(3):
                fin_copy(k, s).start()

        return 0

    lax.fori_loop(0, NU, run_unit, 0)

    pass_on(0)
    pass_on(1)

    for mask in range(1, NT):
        remote(duw, duw_all.at[me], duw_send, duw_recv, jnp.bitwise_xor(me, mask)).start()
    duw_all[me] = duw[:]

    def late_work(c, heads):
        if c:
            pair_wait(heads, "wait_recv")
        local_work(0 if c else EARLY, local_count(c), c)

    at_chip(late_work)
    pass_on(2)
    for k in range(HC):
        far_relay(k)

    others = duw_all.at[pl.ds(0, NT - 1)]
    remote(others, others, duw_send, duw_recv, partner).wait()
    for h in range(NH):
        both = duw_all[2 * (h // HC), h % HC] + duw_all[2 * (h // HC) + 1, h % HC]
        for r, bias_out in enumerate((du_out, dw_out)):
            bias_out[h:h + 1] = both[r:r + 1]

    sent = rin.at[:, pl.ds(0, NT - 1)]
    remote(sent, sent, in_send, in_recv.at[0], partner).wait_send()
    sent = rin.at[:, pl.ds(0, 5)]
    remote(sent, sent, out_send, out_recv, partner).wait_send()
    for inner, count in ((True, 6), (False, 4)):
        @pl.when(outer != inner)
        def _():
            got = rin.at[:, pl.ds(0, count)]
            remote(got, got, out_send, out_recv, partner).wait_recv()

    @pl.when(~outer)
    def _():
        remote(rl, rl, fw_send, in_recv.at[0], partner).wait_send()

    @pl.when(chip != last)
    def _():
        some = st_out.at[:, 1]
        remote(some, some, st_send, st_recv.at[0], partner).wait_send()

    @pl.when(chip == 0)
    def _():
        remote(st_out, st_out, st_send_all, st_recv.at[0], partner).wait_send()

    def end_local(c, heads):
        pair_wait(heads, "wait_send")
        count = local_count(c)
        for x in (count - 2, count - 1):
            local_send(x, c).wait_send()
        whole = out.at[0, pl.ds(0, count // NU)]
        remote(whole, whole, lr_send.at[0], lr_recv, partner).wait_recv()

    at_chip(end_local)
    more = (HALF // 2 - CUT) // NA
    for c, rows in enumerate((-more, 0, 0, more)):
        @pl.when(chip == c)
        def _():
            sent = drk_out.at[:, pl.ds(0, (NT - 1) * T + rows)]
            remote(sent, sent, table_send, table_recv, partner).wait_send()

    got = drk_out.at[:, pl.ds(0, HALF)]
    remote(got, got, table_send, table_recv, partner).wait_recv()


def exchange_attend(xq, xd, xk, xv, bias_u, bias_w, rel):
    any_spec = pl.BlockSpec(memory_space=pl.ANY)
    vmem_spec = pl.BlockSpec(memory_space=pltpu.VMEM)
    dma = pltpu.SemaphoreType.DMA
    acts = pltpu.VMEM((NA, NA, NH, T, D), BF)
    bias = pltpu.VMEM((NH, D), F32)
    heads = pltpu.VMEM((HC, NT, T, D), BF)
    per_pair = dma((NU,))
    per_head = dma((HC,))
    two = dma((2,))
    one = dma(())
    return pl.pallas_call(
        kernel,
        out_shape=(acts, pltpu.VMEM((NH, NT * T, D), F32), bias, bias,
                   jax.ShapeDtypeStruct((NA, 2, NH, T, D), BF)),
        in_specs=[any_spec] * 7,
        out_specs=(vmem_spec,) * 4 + (any_spec,),
        scratch_shapes=[
            pltpu.VMEM((NU, NT, NA, T, D), BF), pltpu.VMEM((NU, 2, 2, T, D), BF), pltpu.VMEM((HC, NT, D, T), F32),
            pltpu.VMEM((HC, NA, D, T), F32), pltpu.VMEM((HC, 8, D), F32), pltpu.VMEM((NT, HC, 8, D), F32),
            heads, heads, pltpu.VMEM((2, NH, D), BF), bias, bias,
            pltpu.VMEM((2, 2, NA, T, D), BF), pltpu.VMEM((2, NA, T, D), BF), pltpu.VMEM((2, 2, 2, T, D), BF),
            pltpu.VMEM((NU, 2, 8, T), F32), pltpu.VMEM((HC, NU, 2, 8, T), F32),
            per_pair, per_pair, per_pair, per_head, per_head, dma((HC, 2)), dma((HC, 2)), two, two]
        + [one] * 9 + [per_head] + [one] * 5
        + UNIT_SCRATCH,
        compiler_params=pltpu.CompilerParams(collective_id=0, has_side_effects=True, vmem_limit_bytes=VMEM_LIMIT),
    )(xq, xd, xk, xv, bias_u, bias_w, rel)


def write_kernel(acts, table, bias_u, bias_w, *refs):
    sem = refs[-1]
    srcs = [acts.at[a] for a in range(NA)] + [table, bias_u, bias_w]
    copies = [pltpu.make_async_copy(src, dst, sem.at[n]) for n, (src, dst) in enumerate(zip(srcs, refs[:-1]))]
    for copy in copies:
        copy.start()
    for copy in copies:
        copy.wait()


def write_out(arrs):
    shapes = [arrs[0].shape[1:]] * NA + [arr.shape for arr in arrs[1:]]
    types = [arrs[0].dtype] * NA + [arr.dtype for arr in arrs[1:]]
    return pl.pallas_call(
        write_kernel,
        out_shape=tuple(map(jax.ShapeDtypeStruct, shapes, types)),
        in_specs=[pl.BlockSpec(memory_space=pltpu.VMEM)] * len(arrs),
        out_specs=(pl.BlockSpec(memory_space=pl.ANY),) * len(shapes),
        scratch_shapes=[pltpu.SemaphoreType.DMA((len(shapes),))],
        compiler_params=pltpu.CompilerParams(vmem_limit_bytes=1024 * 1024),
    )(*[pltpu.with_memory_space_constraint(arr, pltpu.VMEM) for arr in arrs])


def solution(mesh):
    seq_spec = P(None, 'cp', None, None)

    def local(query, key_in, value, bias_u, bias_w, rel_k, d_out):
        def by_head(arr):
            return arr.transpose(0, 2, 1, 3)

        rel = rel_k.transpose(1, 0, 2).reshape(NH, NT, T, D)
        acts = [by_head(arr) for arr in (query, d_out, key_in, value)]
        res = write_out(exchange_attend(*acts, bias_u, bias_w, rel)[:4])
        d_rel = res[4].reshape(NH, NT * T, D).transpose(1, 0, 2)
        return tuple(by_head(arr) for arr in res[:4]) + (res[5], res[6], d_rel)

    return jax.shard_map(local, mesh=mesh,
                         in_specs=(seq_spec, seq_spec, seq_spec, P(), P(), P(), seq_spec),
                         out_specs=(seq_spec, seq_spec, seq_spec, seq_spec, P(), P(), P()),
                         check_vma=False)
```

```python
import jax
import jax.numpy as jnp
from jax import lax
from jax.experimental import pallas as pl
from jax.experimental.pallas import tpu as pltpu
from jax.sharding import PartitionSpec as P

T = 256
D = 128
H = 128
NT = 8
NU = 6
NA = 4
HC = 3
HALF = 1024
CUT = 480
NH = 12
EARLY = 6
GROUPS = ((0, 1), (1, 1), (2, 2), (4, 2))
AHEAD = 3
SEND_AT = 1
FORWARD_AT = (0, 0, 1, 3)
VMEM_LIMIT = 39 * 1024 * 1024
F32 = jnp.float32
BF = jnp.bfloat16
SCALE = D ** -0.5
C2 = SCALE * 1.4426950408889634
MESH = pl.DeviceIdType.MESH


def dot_nt(lhs, rhs):
    return lax.dot_general(lhs, rhs, (((1,), (1,)), ((), ())), preferred_element_type=F32)


def row_max(arr):
    return jnp.max(arr, axis=1, keepdims=True)


def row_sum(arr):
    return jnp.sum(arr, axis=1, keepdims=True)


def dot_nn(lhs, rhs):
    return lax.dot_general(lhs, rhs, (((1,), (0,)), ((), ())), preferred_element_type=F32)


def unit(x, rk, rkr, u, w, drk, duw, scratch, after_softmax, after_tile):
    (s_ref, dp_ref, r_ref, mx_ref, l_ref, d_ref, u_ref, dk_ref, dv_ref, a_ref, c_ref, t_ref,
     oacc, qc_acc, qr_acc) = scratch
    nt = NT
    low = lower_mask()
    gather = gather_fn()
    dk_ref[:] = jnp.zeros_like(dk_ref)
    dv_ref[:] = jnp.zeros_like(dv_ref)

    def prep(i, sl):
        q = x[i, 0].astype(F32)
        a_ref[sl] = (q + u).astype(BF)
        c_ref[sl] = (q + w).astype(BF)
        mx_ref[:] = jnp.full((T, H), -jnp.inf, F32)
        r_ref[:] = jnp.full((2, T, H), -jnp.inf, F32)

    def logits(i, sl, n):
        j = i - n
        by = dot_nt(c_ref[sl], rkr[n])
        sc = dot_nt(a_ref[sl], x[j, 2])
        dp_ref[sl, j] = dot_nt(x[i, 1], x[j, 3])
        r0, r1 = [pltpu.roll(half, 1, 1, stride=1, stride_axis=0) for half in (by[:, :H], by[:, H:])]
        sc += shifted(low, r1, r0, r_ref[1], r_ref[0])
        r_ref[0] = r0
        r_ref[1] = r1
        s_ref[sl, j] = sc
        mx_ref[:] = jnp.maximum(mx_ref[:], jnp.maximum(sc[:, :H], sc[:, H:]))

    def softmax(i, sl):
        m = row_max(mx_ref[:])
        l_ref[:] = jnp.zeros_like(l_ref)
        d_ref[:] = jnp.zeros_like(d_ref)

        def body(j, _):
            p = jnp.exp2((s_ref[sl, j] - m) * C2)
            s_ref[sl, j] = p
            pd = p * dp_ref[sl, j]
            l_ref[:] += p[:, :H] + p[:, H:]
            d_ref[:] += pd[:, :H] + pd[:, H:]
            return 0

        lax.fori_loop(0, i + 1, body, 0)
        inv = 1.0 / row_sum(l_ref[:])
        rd = row_sum(d_ref[:]) * inv
        after_softmax(i, m, inv, rd)
        return inv, rd

    def grads(i, sl, j, inv, rd):
        pn = s_ref[sl, j] * inv
        pb = pn.astype(BF)
        ds = pn * (dp_ref[sl, j] - rd) * SCALE
        dsb = ds.astype(BF)
        oacc[:] += dot_nn(pb, x[j, 3])
        dv_ref[j] += dot_nn(t_ref[0], pb)
        qc_acc[:] += dot_nn(dsb, x[j, 2])
        dk_ref[j] += dot_nn(t_ref[1], dsb)
        g0, g1 = gather(ds)
        dist = shifted(low, g0, g1, u_ref[0], u_ref[1]).astype(BF)
        u_ref[0] = g0
        u_ref[1] = g1
        qr_acc[:] += dot_nn(dist, rk[i - j])
        drk[i - j] += dot_nn(t_ref[2], dist)

    prep(nt - 1, (nt - 1) % 2)

    def first(n, _):
        logits(nt - 1, (nt - 1) % 2, n)
        return 0

    lax.fori_loop(0, nt, first, 0)

    def tile(ii, _):
        i = nt - 1 - ii
        sl = i % 2
        inv, rd = softmax(i, sl)
        nxt = jnp.maximum(i - 1, 0)
        t_ref[0] = x[i, 1].T
        t_ref[1] = a_ref[sl].T
        t_ref[2] = c_ref[sl].T
        for acc in (oacc, qc_acc, qr_acc, u_ref):
            acc[:] = jnp.zeros_like(acc)
        prep(nxt, 1 - sl)

        def both(n, _):
            grads(i, sl, n, inv, rd)
            logits(nxt, 1 - sl, n)
            return 0

        lax.fori_loop(0, i, both, 0)
        grads(i, sl, i, inv, rd)
        qc = qc_acc[:]
        qr = qr_acc[:]
        for r, part in enumerate((qc, qr)):
            duw[r:r + 1] += jnp.sum(part, axis=0, keepdims=True)
        for r, res in enumerate((oacc[:], qc + qr, dk_ref[i].T, dv_ref[i].T)):
            x[i, r] = res.astype(BF)
        after_tile(i)
        return 0

    lax.fori_loop(0, nt, tile, 0)


def gather_fn():
    idx = (lax.broadcasted_iota(jnp.int32, (T, H), 0) - lax.broadcasted_iota(jnp.int32, (T, H), 1)) & (H - 1)

    def gather(arr):
        return [jnp.take_along_axis(half, idx, axis=1, mode="promise_in_bounds") for half in (arr[:, :H], arr[:, H:])]

    return gather


def lower_mask():
    return lax.broadcasted_iota(jnp.int32, (H, H), 1) <= lax.broadcasted_iota(jnp.int32, (H, H), 0)


def shifted(low, n0, n1, p0, p1):
    lo = jnp.concatenate([jnp.where(low, n0[:H], p1[:H]), jnp.where(low, n1[H:], n0[H:])], 0)
    hi = jnp.concatenate([jnp.where(low, p1[:H], p0[:H]), jnp.where(low, n0[H:], p1[H:])], 0)
    return jnp.concatenate([lo, hi], 1)


def row_tile(q, d_out, keys, vals, rk, u, w):
    last = len(keys) - 1
    low = lower_mask()
    gather = gather_fn()
    qf = q.astype(F32)
    a = (qf + u).astype(BF)
    c = (qf + w).astype(BF)
    by = [gather(dot_nt(c, rk[n])) for n in range(last + 1)]
    none = [jnp.full((T, H), -jnp.inf, F32)] * 2
    s = [dot_nt(a, key) + shifted(low, *by[last - j], *(by[last - j - 1] if j < last else none)) for j, key in enumerate(keys)]
    top = s[0]
    for other in s[1:]:
        top = jnp.maximum(top, other)
    m = row_max(top)
    p = [jnp.exp2((sj - m) * C2) for sj in s]
    dp = [dot_nt(d_out, val) for val in vals]
    inv = 1.0 / row_sum(sum(p))
    row_dot = row_sum(sum(pj * dj for pj, dj in zip(p, dp))) * inv
    out, d_q, prev = 0.0, 0.0, [jnp.zeros((T, H), F32)] * 2
    for j in range(last + 1):
        pn = p[j] * inv
        ds = pn * (dp[j] - row_dot) * SCALE
        out += dot_nn(pn.astype(BF), vals[j])
        mine = gather(ds)
        dist = shifted(low, *mine, *prev).astype(BF)
        prev = mine
        d_q += dot_nn(ds.astype(BF), keys[j]) + dot_nn(dist, rk[last - j])
    return out.astype(BF), d_q.astype(BF)


def col_tiles(qs, d_outs, keys, vals, rk, stats, u, w):
    low = lower_mask()
    gather = gather_fn()
    none = [jnp.full((T, H), -jnp.inf, F32)] * 2
    d_keys, d_vals = [0.0, 0.0], [0.0, 0.0]
    for i in range(len(qs)):
        qf = qs[i].astype(F32)
        a = (qf + u).astype(BF)
        c = (qf + w).astype(BF)
        by = {n: gather(dot_nt(c, rk[n])) for n in range(max(i - 2, 0), i + 1)}
        if i % 2 == 0:
            cols = jnp.concatenate([stats[i // 2], jnp.zeros((H - 8, T), F32)], 0).T
        m, inv, row_dot = [cols[:, r:r + 1] for r in range(HC * (i % 2), HC * (i % 2 + 1))]
        at, dot = a.T, d_outs[i].T
        for r in range(min(i + 1, 2)):
            n = i - r
            s = dot_nt(a, keys[r]) + shifted(low, *by[n], *(by[n - 1] if n else none))
            pn = jnp.exp2((s - m) * C2) * inv
            ds = pn * (dot_nt(d_outs[i], vals[r]) - row_dot) * SCALE
            d_vals[r] += dot_nn(dot, pn.astype(BF))
            d_keys[r] += dot_nn(at, ds.astype(BF))
    return [dk.T.astype(BF) for dk in d_keys], [dv.T.astype(BF) for dv in d_vals]


UNIT_SCRATCH = (
    [pltpu.VMEM((2, NT, T, T), F32)] * 2 + [pltpu.VMEM((2, T, H), F32)] + [pltpu.VMEM((T, H), F32)] * 3
    + [pltpu.VMEM((2, T, H), F32)] + [pltpu.VMEM((NT, D, T), F32)] * 2 + [pltpu.VMEM((2, T, D), BF)] * 2
    + [pltpu.VMEM((3, D, T), BF)] + [pltpu.VMEM((T, D), F32)] * 3)


def kernel(xq, xd, xk, xv, bias_u, bias_w, rel, out, drk_out, du_out, dw_out, lx,
           rin, rl, drk, pbuf, duw, duw_all, rk, rkr, bias, bu, bw, lblk, lrk, lres, st_out, st_in,
           in_recv, rl_recv, st_recv, half_send, half_recv, fin_recv, hop_recv, l_sem, lr_send,
           in_send, in_loc, fw_send, out_send, out_recv, table_send, table_recv, duw_send, duw_recv, rk_sem, px_send,
           px_recv, st_send, st_send_all, lr_recv, *scratch):
    me = lax.axis_index('cp')
    chip = me // 2
    core = me % 2
    last = NA - 1
    partner = jnp.bitwise_xor(me, 1)
    outer = (chip == 0) | (chip == last)
    ins = (xq, xd, xk, xv)
    neighbours = (1, 2, 4)

    def remote(src, dst, ssem, rsem, dev):
        return pltpu.make_async_remote_copy(src_ref=src, dst_ref=dst, send_sem=ssem, recv_sem=rsem,
                                            device_id=(dev,), device_id_type=MESH)

    def pair_of(dev, n):
        return 2 * (dev % 2) + n % 2, HC * (dev // 2) + n // 2

    def spot(a, dev, n):
        return ins[a].at[pair_of(dev, n)]

    def pairs(n, count):
        return pl.ds(n, count) if count > 1 else n

    def send_in(n, count, mask):
        dev = jnp.bitwise_xor(me, mask)
        bat, head = pair_of(dev, n)

        def send(first, via):
            for a in (first, first + 1):
                if via:
                    dst, rsem, to = rl.at[pairs(n, count), core, a % 2], rl_recv.at[n], jnp.bitwise_xor(dev, 4)
                else:
                    dst, rsem, to = rin.at[pairs(n, count), me, a], in_recv.at[n], dev
                remote(ins[a].at[pairs(bat, count), head], dst, in_send, rsem, to).start()

        for first in (0, 2):
            if mask < NU:
                send(first, False)
            else:
                through = chip == (0 if first else last)
                for via in (True, False):
                    @pl.when(through == via)
                    def _():
                        send(first, via)

    def send_group(n, count):
        for mask in (6, 2, 4, 7, 3, 5, 1):
            send_in(n, count, mask)

    def forward(n, count):
        dst = rin.at[pairs(n, count), pl.ds(2 * jnp.bitwise_xor(chip, 1), 2), pl.ds(2 * (chip % 2), 2)]
        return remote(rl.at[pairs(n, count)], dst, fw_send, in_recv.at[n], jnp.bitwise_xor(me, 4))

    def pass_forward(n, count):
        piece = rl.at[pairs(n, count)]
        remote(piece, piece, fw_send, rl_recv.at[n], jnp.bitwise_xor(me, 2)).wait_recv()
        forward(n, count).start()

    def arrive(n, count):
        piece = rin.at[pairs(n, count), pl.ds(0, NT - 1)]
        remote(piece, piece, in_send, in_recv.at[n], partner).wait_recv()

    def at_chip(act):
        for c, heads in enumerate(((3, 9), (9, 3), (0, 3), (0, 9))):
            @pl.when(chip == c)
            def _():
                act(c, pl.ds(*heads))

    def pair_wait(heads, wait):
        piece = lx.at[:, :, heads]
        getattr(remote(piece, piece, px_send, px_recv, partner), wait)()

    def pair_copies(heads):
        return [remote(ins[a].at[pl.ds(2 * (1 - core), 2), heads], lx.at[a, :, heads], px_send, px_recv, partner)
                for a in range(NA)]

    barrier = pltpu.get_barrier_semaphore()
    for mask in range(1, NT):
        pl.semaphore_signal(barrier, inc=1, device_id=(jnp.bitwise_xor(me, mask),), device_id_type=MESH)
    copies = [pltpu.make_async_copy(bias_u, bias.at[0], rk_sem.at[0]), pltpu.make_async_copy(bias_w, bias.at[1], rk_sem.at[1]),
              pltpu.make_async_copy(rel.at[pl.ds(HC * chip, HC)], rk, rk_sem.at[2])]
    for copy in copies:
        copy.start()
    for n in range(NU):
        for a in range(NA):
            pltpu.make_async_copy(spot(a, me, n), rin.at[n, me, a], in_loc).start()
    pl.semaphore_wait(barrier, NT - 1)
    for g, (n, count) in enumerate(GROUPS):
        if g < AHEAD:
            send_group(n, count)
        if g == 0:
            at_chip(lambda c, heads: [copy.start() for copy in pair_copies(heads)])

    for copy in copies:
        copy.wait()
    bu[:] = bias[0].astype(F32)
    bw[:] = bias[1].astype(F32)
    drk[:] = jnp.zeros_like(drk)
    duw[:] = jnp.zeros_like(duw)
    st_out[:] = jnp.zeros_like(st_out)
    flip = (lax.broadcasted_iota(jnp.int32, (T, T), 0) + lax.broadcasted_iota(jnp.int32, (T, T), 1) == T - 1).astype(BF)
    for k in range(HC):
        for n in range(NT):
            rkr[k, n] = dot_nn(flip, rk[k, n]).astype(BF)

    def half_copy(k):
        return remote(drk.at[k, pl.ds(NA * (1 - core), NA)], pbuf.at[k], half_send.at[k], half_recv.at[k], partner)

    def part(src_chip, k, lo=0, rows=HALF):
        return drk_out.at[HC * src_chip + k, pl.ds(HALF * core + lo, rows)]

    def fin_copy(k, s, arrived=False):
        piece = part(jnp.bitwise_xor(chip, s) if arrived else chip, k)
        rsem = fin_recv.at[k, s - 1] if s else table_recv
        return remote(piece, piece, table_send, rsem, jnp.bitwise_xor(me, neighbours[s]))

    even = ((0, HALF // 2), (HALF // 2, HALF // 2))
    uneven = ((0, CUT), (CUT, HALF - CUT))
    going = ((uneven[0], even[1]), ((0, HALF),), ((0, HALF),), (even[0], uneven[1]))
    coming = (((0, HALF),), even, uneven, ((0, HALF),))

    def each_span(spans, act):
        for c, here in enumerate(spans):
            @pl.when(chip == c)
            def _():
                act(here)

    def hop(k, s, span):
        piece = part(jnp.bitwise_xor(chip, s), k, *span)
        return remote(piece, piece, table_send, hop_recv.at[k, s - 1], jnp.bitwise_xor(me, neighbours[-s]))

    def relay(k, s, *span):
        piece = part(jnp.bitwise_xor(chip, s), k, *span)
        return remote(piece, piece, table_send, table_recv, partner)

    def far_relay(k):
        def act(spans):
            for r, span in enumerate(spans):
                piece = part(jnp.bitwise_xor(chip, last), k, *span)
                remote(piece, piece, table_send, hop_recv.at[k, r], partner).wait_recv()
                relay(k, last, *span).start()

        each_span(coming, act)

    def pass_on(k):
        for s in (1, 2):
            fin_copy(k, s, True).wait_recv()
            each_span(going, lambda spans: [hop(k, s, span).start() for span in spans[s - 1:s]])
            relay(k, s).start()

    def sent_parts(dev, owner):
        there = dev // 2
        rows = ((there == 0) & (owner != 0)) | ((there == 1) & (owner == last))
        cols = ((there == last) & (owner != last)) | ((there == 2) & (owner == 0))
        return ((0, NA), ~rows & ~cols), ((2, 2), rows), ((0, 2), cols)

    def stat_copy(n, whole):
        if whole:
            return remote(st_out.at[n], st_in.at[0, n], st_send_all, st_recv.at[n], 4 + core)
        return remote(st_out.at[n, 1], st_in.at[chip, n, 1], st_send, st_recv.at[n], 6 + core)

    def after_softmax(n, i, m, inv, rd):
        first = jnp.where(chip == 0, 4, 6)

        @pl.when((i >= first) & (chip != last))
        def _():
            lane = lax.broadcasted_iota(jnp.int32, (T, H), 1)
            table = jnp.where(lane == 0, m, jnp.where(lane == 1, inv, rd)).T
            for r in range(2):
                @pl.when(i % 2 == r)
                def _():
                    st_out[n, i // 2 - 2, HC * r:HC * (r + 1)] = table[:HC]

    def local_pair(x):
        owner = jnp.where(outer, x % HC + jnp.where(chip == 0, 1, 0), jnp.where(chip == 1, last, 0))
        n = jnp.where(outer, x // HC, x)
        return owner, n, 2 * core + n % 2, HC * owner + n // 2

    def local_loads(x, sl):
        _, n, bat, head = local_pair(x)
        copies = [pltpu.make_async_copy(rel.at[head, pl.ds(0, NA)], lrk.at[sl], l_sem.at[sl])]
        for a in range(NA):
            for r, src in enumerate((ins[a].at[bat, head], lx.at[a, n % 2, head])):
                where = core if r == 0 else 1 - core
                copies.append(pltpu.make_async_copy(src, lblk.at[sl, where, a], l_sem.at[sl]))
        return copies

    def local_send(x, c):
        sl = x % 2
        _, _, bat, head = local_pair(x)
        dst = out.at[pl.ds(2 * (c // 2), 2), bat, head]
        return remote(lres.at[sl, 1 - core], dst, lr_send.at[sl], lr_recv, partner)

    def local_work(lo, hi, c):
        for copy in local_loads(lo, lo % 2):
            copy.start()

        def one(x, _):
            sl = x % 2

            @pl.when(x + 1 < hi)
            def _():
                for copy in local_loads(x + 1, 1 - sl):
                    copy.start()

            pltpu.make_async_copy(rin.at[0, pl.ds(0, HC)], rin.at[0, pl.ds(0, HC)], l_sem.at[sl]).wait()

            @pl.when(x > 1)
            def _():
                local_send(x, c).wait_send()

            owner, n, bat, head = local_pair(x)
            u = bu[pl.ds(head, 1)]
            w = bw[pl.ds(head, 1)]
            q, do, key, val = [[lblk[sl, r, a] for r in range(2)] for a in range(NA)]
            table = lrk[sl]
            if c < 2:
                if c:
                    key = [rl[n, r, 0] for r in range(2)] + key
                    val = [rl[n, r, 1] for r in range(2)] + val
                for r in range(2):
                    upto = len(key) - 1 + r
                    res = row_tile(q[r], do[r], key[:upto], val[:upto], table, u, w)
                    for a in range(2):
                        lres[sl, r, a] = res[a]
            else:
                groups = (1,)
                piece = st_in.at[:, n, 1]
                if c != last:
                    groups = (0, 1)
                    piece = st_in.at[0, n]
                    q = q + [rl[n, r, 0] for r in range(2)]
                    do = do + [rl[n, r, 1] for r in range(2)]

                @pl.when((owner == 0) | (c != last))
                def _():
                    remote(piece, piece, st_send, st_recv.at[n], partner).wait_recv()

                stats = [st_in[owner, n, g] for g in groups]
                for a, res in enumerate(col_tiles(q, do, key, val, table, stats, u, w)):
                    for r in range(2):
                        lres[sl, r, a] = res[r]
            for a in range(2):
                out[2 * (c // 2) + a, bat, head] = lres[sl, core, a]
            local_send(x, c).start()
            return 0

        lax.fori_loop(lo, hi, one, 0)

    def local_count(c):
        return NU if c in (1, 2) else NU * HC

    @pl.when(chip == 0)
    def _():
        pair_wait(pl.ds(3, 9), "wait_recv")
        local_work(0, EARLY, 0)

    def send_tile(n, i):
        mask = jnp.bitwise_xor(me, i)
        for tile, whole, chips in ((6, False, chip != last), (4, True, chip == 0)):
            @pl.when((i == tile) & chips)
            def _():
                stat_copy(n, whole).start()

        for span, sent in sent_parts(i, chip):
            @pl.when((mask != 0) & sent)
            def _():
                some = pl.ds(*span)
                remote(rin.at[n, i, some], out.at[(some,) + pair_of(me, n)], out_send, out_recv, i).start()

        @pl.when(mask == 0)
        def _():
            for a in range(NA):
                out[(a,) + pair_of(me, n)] = rin[n, i, a]

    def run_unit(n, _):
        k = n // 2

        for g, group in enumerate(GROUPS):
            if g >= AHEAD:
                @pl.when(n == SEND_AT)
                def _():
                    send_group(*group)

            @pl.when(~outer & (n == FORWARD_AT[g]))
            def _():
                pass_forward(*group)

        @pl.when(n == 0)
        def _():
            pltpu.make_async_copy(rin.at[:, me], rin.at[:, me], in_loc).wait()

        for group in GROUPS:
            @pl.when(n == group[0])
            def _():
                arrive(*group)

        head = pl.ds(HC * chip + k, 1)
        unit(rin.at[n], rk.at[k], rkr.at[k], bu[head], bw[head], drk.at[k], duw.at[k], scratch,
             lambda i, m, inv, rd: after_softmax(n, i, m, inv, rd), lambda i: send_tile(n, i))

        @pl.when(n % 2 == 1)
        def _():
            copy = half_copy(k)
            copy.start()
            copy.wait()
            for r in range(NA):
                part(chip, k, r * T, T)[:] = (drk[k, NA * core + r] + pbuf[k, r]).T
            for s in range(3):
                fin_copy(k, s).start()

        return 0

    lax.fori_loop(0, NU, run_unit, 0)

    pass_on(0)
    pass_on(1)

    for mask in range(1, NT):
        remote(duw, duw_all.at[me], duw_send, duw_recv, jnp.bitwise_xor(me, mask)).start()
    duw_all[me] = duw[:]

    def late_work(c, heads):
        if c:
            pair_wait(heads, "wait_recv")
        local_work(0 if c else EARLY, local_count(c), c)

    at_chip(late_work)
    pass_on(2)
    for k in range(HC):
        far_relay(k)

    others = duw_all.at[pl.ds(0, NT - 1)]
    remote(others, others, duw_send, duw_recv, partner).wait()
    for h in range(NH):
        both = duw_all[2 * (h // HC), h % HC] + duw_all[2 * (h // HC) + 1, h % HC]
        for r, bias_out in enumerate((du_out, dw_out)):
            bias_out[h:h + 1] = both[r:r + 1]

    sent = rin.at[:, pl.ds(0, NT - 1)]
    remote(sent, sent, in_send, in_recv.at[0], partner).wait_send()
    sent = rin.at[:, pl.ds(0, 5)]
    remote(sent, sent, out_send, out_recv, partner).wait_send()
    for inner, count in ((True, 6), (False, 4)):
        @pl.when(outer != inner)
        def _():
            got = rin.at[:, pl.ds(0, count)]
            remote(got, got, out_send, out_recv, partner).wait_recv()

    @pl.when(~outer)
    def _():
        remote(rl, rl, fw_send, in_recv.at[0], partner).wait_send()

    @pl.when(chip != last)
    def _():
        some = st_out.at[:, 1]
        remote(some, some, st_send, st_recv.at[0], partner).wait_send()

    @pl.when(chip == 0)
    def _():
        remote(st_out, st_out, st_send_all, st_recv.at[0], partner).wait_send()

    def end_local(c, heads):
        pair_wait(heads, "wait_send")
        count = local_count(c)
        for x in (count - 2, count - 1):
            local_send(x, c).wait_send()
        whole = out.at[0, pl.ds(0, count // NU)]
        remote(whole, whole, lr_send.at[0], lr_recv, partner).wait_recv()

    at_chip(end_local)
    more = (HALF // 2 - CUT) // NA
    for c, rows in enumerate((-more, 0, 0, more)):
        @pl.when(chip == c)
        def _():
            sent = drk_out.at[:, pl.ds(0, (NT - 1) * T + rows)]
            remote(sent, sent, table_send, table_recv, partner).wait_send()

    got = drk_out.at[:, pl.ds(0, HALF)]
    remote(got, got, table_send, table_recv, partner).wait_recv()


def exchange_attend(xq, xd, xk, xv, bias_u, bias_w, rel):
    any_spec = pl.BlockSpec(memory_space=pl.ANY)
    vmem_spec = pl.BlockSpec(memory_space=pltpu.VMEM)
    dma = pltpu.SemaphoreType.DMA
    acts = pltpu.VMEM((NA, NA, NH, T, D), BF)
    bias = pltpu.VMEM((NH, D), F32)
    heads = pltpu.VMEM((HC, NT, T, D), BF)
    per_pair = dma((NU,))
    per_head = dma((HC,))
    two = dma((2,))
    one = dma(())
    return pl.pallas_call(
        kernel,
        out_shape=(acts, pltpu.VMEM((NH, NT * T, D), F32), bias, bias,
                   jax.ShapeDtypeStruct((NA, 2, NH, T, D), BF)),
        in_specs=[any_spec] * 7,
        out_specs=(vmem_spec,) * 4 + (any_spec,),
        scratch_shapes=[
            pltpu.VMEM((NU, NT, NA, T, D), BF), pltpu.VMEM((NU, 2, 2, T, D), BF), pltpu.VMEM((HC, NT, D, T), F32),
            pltpu.VMEM((HC, NA, D, T), F32), pltpu.VMEM((HC, 8, D), F32), pltpu.VMEM((NT, HC, 8, D), F32),
            heads, heads, pltpu.VMEM((2, NH, D), BF), bias, bias,
            pltpu.VMEM((2, 2, NA, T, D), BF), pltpu.VMEM((2, NA, T, D), BF), pltpu.VMEM((2, 2, 2, T, D), BF),
            pltpu.VMEM((NU, 2, 8, T), F32), pltpu.VMEM((HC, NU, 2, 8, T), F32),
            per_pair, per_pair, per_pair, per_head, per_head, dma((HC, 2)), dma((HC, 2)), two, two]
        + [one] * 9 + [per_head] + [one] * 5
        + UNIT_SCRATCH,
        compiler_params=pltpu.CompilerParams(collective_id=0, has_side_effects=True, vmem_limit_bytes=VMEM_LIMIT),
    )(xq, xd, xk, xv, bias_u, bias_w, rel)


def write_kernel(acts, table, bias_u, bias_w, *refs):
    sem = refs[-1]
    srcs = [acts.at[a] for a in range(NA)] + [table, bias_u, bias_w]
    copies = [pltpu.make_async_copy(src, dst, sem.at[n]) for n, (src, dst) in enumerate(zip(srcs, refs[:-1]))]
    for r, copy in enumerate(copies):
        copy.start(priority=r % 2)
    for copy in copies:
        copy.wait()


def write_out(arrs):
    shapes = [arrs[0].shape[1:]] * NA + [arr.shape for arr in arrs[1:]]
    types = [arrs[0].dtype] * NA + [arr.dtype for arr in arrs[1:]]
    return pl.pallas_call(
        write_kernel,
        out_shape=tuple(map(jax.ShapeDtypeStruct, shapes, types)),
        in_specs=[pl.BlockSpec(memory_space=pltpu.VMEM)] * len(arrs),
        out_specs=(pl.BlockSpec(memory_space=pl.ANY),) * len(shapes),
        scratch_shapes=[pltpu.SemaphoreType.DMA((len(shapes),))],
        compiler_params=pltpu.CompilerParams(vmem_limit_bytes=1024 * 1024),
    )(*[pltpu.with_memory_space_constraint(arr, pltpu.VMEM) for arr in arrs])


def solution(mesh):
    seq_spec = P(None, 'cp', None, None)

    def local(query, key_in, value, bias_u, bias_w, rel_k, d_out):
        def by_head(arr):
            return arr.transpose(0, 2, 1, 3)

        rel = rel_k.transpose(1, 0, 2).reshape(NH, NT, T, D)
        acts = [by_head(arr) for arr in (query, d_out, key_in, value)]
        res = write_out(exchange_attend(*acts, bias_u, bias_w, rel)[:4])
        d_rel = res[4].reshape(NH, NT * T, D).transpose(1, 0, 2)
        return tuple(by_head(arr) for arr in res[:4]) + (res[5], res[6], d_rel)

    return jax.shard_map(local, mesh=mesh,
                         in_specs=(seq_spec, seq_spec, seq_spec, P(), P(), P(), seq_spec),
                         out_specs=(seq_spec, seq_spec, seq_spec, seq_spec, P(), P(), P()),
                         check_vma=False)
```

```python
import jax
import jax.numpy as jnp
from jax import lax
from jax.experimental import pallas as pl
from jax.experimental.pallas import tpu as pltpu
from jax.sharding import PartitionSpec as P

T = 256
D = 128
H = 128
NT = 8
NU = 6
NA = 4
HC = 3
HALF = 1024
CUT = 472
CUT_BACK = 520
NH = 12
EARLY = 6
GROUPS = ((0, 1), (1, 1), (2, 2), (4, 2))
AHEAD = 3
SEND_AT = 1
FORWARD_AT = (0, 0, 1, 3)
VMEM_LIMIT = 39 * 1024 * 1024
F32 = jnp.float32
BF = jnp.bfloat16
SCALE = D ** -0.5
C2 = SCALE * 1.4426950408889634
MESH = pl.DeviceIdType.MESH


def dot_nt(lhs, rhs):
    return lax.dot_general(lhs, rhs, (((1,), (1,)), ((), ())), preferred_element_type=F32)


def row_max(arr):
    return jnp.max(arr, axis=1, keepdims=True)


def row_sum(arr):
    return jnp.sum(arr, axis=1, keepdims=True)


def dot_nn(lhs, rhs):
    return lax.dot_general(lhs, rhs, (((1,), (0,)), ((), ())), preferred_element_type=F32)


def unit(x, rk, rkr, u, w, drk, duw, scratch, after_softmax, after_tile):
    (s_ref, dp_ref, r_ref, mx_ref, l_ref, d_ref, u_ref, dk_ref, dv_ref, a_ref, c_ref, t_ref,
     oacc, qc_acc, qr_acc) = scratch
    nt = NT
    low = lower_mask()
    gather = gather_fn()
    dk_ref[:] = jnp.zeros_like(dk_ref)
    dv_ref[:] = jnp.zeros_like(dv_ref)

    def prep(i, sl):
        q = x[i, 0].astype(F32)
        a_ref[sl] = (q + u).astype(BF)
        c_ref[sl] = (q + w).astype(BF)
        mx_ref[:] = jnp.full((T, H), -jnp.inf, F32)
        r_ref[:] = jnp.full((2, T, H), -jnp.inf, F32)

    def logits(i, sl, n):
        j = i - n
        by = dot_nt(c_ref[sl], rkr[n])
        sc = dot_nt(a_ref[sl], x[j, 2])
        dp_ref[sl, j] = dot_nt(x[i, 1], x[j, 3])
        r0, r1 = [pltpu.roll(half, 1, 1, stride=1, stride_axis=0) for half in (by[:, :H], by[:, H:])]
        sc += shifted(low, r1, r0, r_ref[1], r_ref[0])
        r_ref[0] = r0
        r_ref[1] = r1
        s_ref[sl, j] = sc
        mx_ref[:] = jnp.maximum(mx_ref[:], jnp.maximum(sc[:, :H], sc[:, H:]))

    def softmax(i, sl):
        m = row_max(mx_ref[:])
        l_ref[:] = jnp.zeros_like(l_ref)
        d_ref[:] = jnp.zeros_like(d_ref)

        def body(j, _):
            p = jnp.exp2((s_ref[sl, j] - m) * C2)
            s_ref[sl, j] = p
            pd = p * dp_ref[sl, j]
            l_ref[:] += p[:, :H] + p[:, H:]
            d_ref[:] += pd[:, :H] + pd[:, H:]
            return 0

        lax.fori_loop(0, i + 1, body, 0)
        inv = 1.0 / row_sum(l_ref[:])
        rd = row_sum(d_ref[:]) * inv
        after_softmax(i, m, inv, rd)
        return inv, rd

    def grads(i, sl, j, inv, rd):
        pn = s_ref[sl, j] * inv
        pb = pn.astype(BF)
        ds = pn * (dp_ref[sl, j] - rd) * SCALE
        dsb = ds.astype(BF)
        oacc[:] += dot_nn(pb, x[j, 3])
        dv_ref[j] += dot_nn(t_ref[0], pb)
        qc_acc[:] += dot_nn(dsb, x[j, 2])
        dk_ref[j] += dot_nn(t_ref[1], dsb)
        g0, g1 = gather(ds)
        dist = shifted(low, g0, g1, u_ref[0], u_ref[1]).astype(BF)
        u_ref[0] = g0
        u_ref[1] = g1
        qr_acc[:] += dot_nn(dist, rk[i - j])
        drk[i - j] += dot_nn(t_ref[2], dist)

    prep(nt - 1, (nt - 1) % 2)

    def first(n, _):
        logits(nt - 1, (nt - 1) % 2, n)
        return 0

    lax.fori_loop(0, nt, first, 0)

    def tile(ii, _):
        i = nt - 1 - ii
        sl = i % 2
        inv, rd = softmax(i, sl)
        nxt = jnp.maximum(i - 1, 0)
        t_ref[0] = x[i, 1].T
        t_ref[1] = a_ref[sl].T
        t_ref[2] = c_ref[sl].T
        for acc in (oacc, qc_acc, qr_acc, u_ref):
            acc[:] = jnp.zeros_like(acc)
        prep(nxt, 1 - sl)

        def both(n, _):
            grads(i, sl, n, inv, rd)
            logits(nxt, 1 - sl, n)
            return 0

        lax.fori_loop(0, i, both, 0)
        grads(i, sl, i, inv, rd)
        qc = qc_acc[:]
        qr = qr_acc[:]
        for r, part in enumerate((qc, qr)):
            duw[r:r + 1] += jnp.sum(part, axis=0, keepdims=True)
        for r, res in enumerate((oacc[:], qc + qr, dk_ref[i].T, dv_ref[i].T)):
            x[i, r] = res.astype(BF)
        after_tile(i)
        return 0

    lax.fori_loop(0, nt, tile, 0)


def gather_fn():
    idx = (lax.broadcasted_iota(jnp.int32, (T, H), 0) - lax.broadcasted_iota(jnp.int32, (T, H), 1)) & (H - 1)

    def gather(arr):
        return [jnp.take_along_axis(half, idx, axis=1, mode="promise_in_bounds") for half in (arr[:, :H], arr[:, H:])]

    return gather


def lower_mask():
    return lax.broadcasted_iota(jnp.int32, (H, H), 1) <= lax.broadcasted_iota(jnp.int32, (H, H), 0)


def shifted(low, n0, n1, p0, p1):
    lo = jnp.concatenate([jnp.where(low, n0[:H], p1[:H]), jnp.where(low, n1[H:], n0[H:])], 0)
    hi = jnp.concatenate([jnp.where(low, p1[:H], p0[:H]), jnp.where(low, n0[H:], p1[H:])], 0)
    return jnp.concatenate([lo, hi], 1)


def row_tile(q, d_out, keys, vals, rk, u, w):
    last = len(keys) - 1
    low = lower_mask()
    gather = gather_fn()
    qf = q.astype(F32)
    a = (qf + u).astype(BF)
    c = (qf + w).astype(BF)
    by = [gather(dot_nt(c, rk[n])) for n in range(last + 1)]
    none = [jnp.full((T, H), -jnp.inf, F32)] * 2
    s = [dot_nt(a, key) + shifted(low, *by[last - j], *(by[last - j - 1] if j < last else none)) for j, key in enumerate(keys)]
    top = s[0]
    for other in s[1:]:
        top = jnp.maximum(top, other)
    m = row_max(top)
    p = [jnp.exp2((sj - m) * C2) for sj in s]
    dp = [dot_nt(d_out, val) for val in vals]
    inv = 1.0 / row_sum(sum(p))
    row_dot = row_sum(sum(pj * dj for pj, dj in zip(p, dp))) * inv
    out, d_q, prev = 0.0, 0.0, [jnp.zeros((T, H), F32)] * 2
    for j in range(last + 1):
        pn = p[j] * inv
        ds = pn * (dp[j] - row_dot) * SCALE
        out += dot_nn(pn.astype(BF), vals[j])
        mine = gather(ds)
        dist = shifted(low, *mine, *prev).astype(BF)
        prev = mine
        d_q += dot_nn(ds.astype(BF), keys[j]) + dot_nn(dist, rk[last - j])
    return out.astype(BF), d_q.astype(BF)


def col_tiles(qs, d_outs, keys, vals, rk, stats, u, w):
    low = lower_mask()
    gather = gather_fn()
    none = [jnp.full((T, H), -jnp.inf, F32)] * 2
    d_keys, d_vals = [0.0, 0.0], [0.0, 0.0]
    for i in range(len(qs)):
        qf = qs[i].astype(F32)
        a = (qf + u).astype(BF)
        c = (qf + w).astype(BF)
        by = {n: gather(dot_nt(c, rk[n])) for n in range(max(i - 2, 0), i + 1)}
        if i % 2 == 0:
            cols = jnp.concatenate([stats[i // 2], jnp.zeros((H - 8, T), F32)], 0).T
        m, inv, row_dot = [cols[:, r:r + 1] for r in range(HC * (i % 2), HC * (i % 2 + 1))]
        at, dot = a.T, d_outs[i].T
        for r in range(min(i + 1, 2)):
            n = i - r
            s = dot_nt(a, keys[r]) + shifted(low, *by[n], *(by[n - 1] if n else none))
            pn = jnp.exp2((s - m) * C2) * inv
            ds = pn * (dot_nt(d_outs[i], vals[r]) - row_dot) * SCALE
            d_vals[r] += dot_nn(dot, pn.astype(BF))
            d_keys[r] += dot_nn(at, ds.astype(BF))
    return [dk.T.astype(BF) for dk in d_keys], [dv.T.astype(BF) for dv in d_vals]


UNIT_SCRATCH = (
    [pltpu.VMEM((2, NT, T, T), F32)] * 2 + [pltpu.VMEM((2, T, H), F32)] + [pltpu.VMEM((T, H), F32)] * 3
    + [pltpu.VMEM((2, T, H), F32)] + [pltpu.VMEM((NT, D, T), F32)] * 2 + [pltpu.VMEM((2, T, D), BF)] * 2
    + [pltpu.VMEM((3, D, T), BF)] + [pltpu.VMEM((T, D), F32)] * 3)


def kernel(xq, xd, xk, xv, bias_u, bias_w, rel, out, drk_out, du_out, dw_out, lx,
           rin, rl, drk, pbuf, duw, duw_all, rk, rkr, bias, bu, bw, lblk, lrk, lres, st_out, st_in,
           in_recv, rl_recv, st_recv, half_send, half_recv, fin_recv, hop_recv, l_sem, lr_send,
           in_send, in_loc, fw_send, out_send, out_recv, table_send, table_recv, duw_send, duw_recv, rk_sem, px_send,
           px_recv, st_send, st_send_all, lr_recv, hop_send, *scratch):
    me = lax.axis_index('cp')
    chip = me // 2
    core = me % 2
    last = NA - 1
    partner = jnp.bitwise_xor(me, 1)
    outer = (chip == 0) | (chip == last)
    ins = (xq, xd, xk, xv)
    neighbours = (1, 2, 4)

    def remote(src, dst, ssem, rsem, dev):
        return pltpu.make_async_remote_copy(src_ref=src, dst_ref=dst, send_sem=ssem, recv_sem=rsem,
                                            device_id=(dev,), device_id_type=MESH)

    def pair_of(dev, n):
        return 2 * (dev % 2) + n % 2, HC * (dev // 2) + n // 2

    def spot(a, dev, n):
        return ins[a].at[pair_of(dev, n)]

    def pairs(n, count):
        return pl.ds(n, count) if count > 1 else n

    def send_in(n, count, mask):
        dev = jnp.bitwise_xor(me, mask)
        bat, head = pair_of(dev, n)

        def send(first, via):
            for a in (first, first + 1):
                if via:
                    dst, rsem, to = rl.at[pairs(n, count), core, a % 2], rl_recv.at[n], jnp.bitwise_xor(dev, 4)
                else:
                    dst, rsem, to = rin.at[pairs(n, count), me, a], in_recv.at[n], dev
                remote(ins[a].at[pairs(bat, count), head], dst, in_send, rsem, to).start()

        for first in (0, 2):
            if mask < NU:
                send(first, False)
            else:
                through = chip == (0 if first else last)
                for via in (True, False):
                    @pl.when(through == via)
                    def _():
                        send(first, via)

    def send_group(n, count):
        for mask in (6, 2, 4, 7, 3, 5, 1):
            send_in(n, count, mask)

    def forward(n, count):
        dst = rin.at[pairs(n, count), pl.ds(2 * jnp.bitwise_xor(chip, 1), 2), pl.ds(2 * (chip % 2), 2)]
        return remote(rl.at[pairs(n, count)], dst, fw_send, in_recv.at[n], jnp.bitwise_xor(me, 4))

    def pass_forward(n, count):
        piece = rl.at[pairs(n, count)]
        remote(piece, piece, fw_send, rl_recv.at[n], jnp.bitwise_xor(me, 2)).wait_recv()
        forward(n, count).start()

    def arrive(n, count):
        piece = rin.at[pairs(n, count), pl.ds(0, NT - 1)]
        remote(piece, piece, in_send, in_recv.at[n], partner).wait_recv()

    def at_chip(act):
        for c, heads in enumerate(((3, 9), (9, 3), (0, 3), (0, 9))):
            @pl.when(chip == c)
            def _():
                act(c, pl.ds(*heads))

    def pair_wait(heads, wait):
        piece = lx.at[:, :, heads]
        getattr(remote(piece, piece, px_send, px_recv, partner), wait)()

    def pair_copies(heads):
        return [remote(ins[a].at[pl.ds(2 * (1 - core), 2), heads], lx.at[a, :, heads], px_send, px_recv, partner)
                for a in range(NA)]

    barrier = pltpu.get_barrier_semaphore()
    for mask in range(1, NT):
        pl.semaphore_signal(barrier, inc=1, device_id=(jnp.bitwise_xor(me, mask),), device_id_type=MESH)
    copies = [pltpu.make_async_copy(bias_u, bias.at[0], rk_sem.at[0]), pltpu.make_async_copy(bias_w, bias.at[1], rk_sem.at[1]),
              pltpu.make_async_copy(rel.at[pl.ds(HC * chip, HC)], rk, rk_sem.at[2])]
    for copy in copies:
        copy.start()
    for n in range(NU):
        for a in range(NA):
            pltpu.make_async_copy(spot(a, me, n), rin.at[n, me, a], in_loc).start()
    pl.semaphore_wait(barrier, NT - 1)
    for g, (n, count) in enumerate(GROUPS):
        if g < AHEAD:
            send_group(n, count)
        if g == 0:
            at_chip(lambda c, heads: [copy.start() for copy in pair_copies(heads)])

    for copy in copies:
        copy.wait()
    bu[:] = bias[0].astype(F32)
    bw[:] = bias[1].astype(F32)
    drk[:] = jnp.zeros_like(drk)
    duw[:] = jnp.zeros_like(duw)
    st_out[:] = jnp.zeros_like(st_out)
    flip = (lax.broadcasted_iota(jnp.int32, (T, T), 0) + lax.broadcasted_iota(jnp.int32, (T, T), 1) == T - 1).astype(BF)
    for k in range(HC):
        for n in range(NT):
            rkr[k, n] = dot_nn(flip, rk[k, n]).astype(BF)

    def half_copy(k):
        return remote(drk.at[k, pl.ds(NA * (1 - core), NA)], pbuf.at[k], half_send.at[k], half_recv.at[k], partner)

    def part(src_chip, k, lo=0, rows=HALF):
        return drk_out.at[HC * src_chip + k, pl.ds(HALF * core + lo, rows)]

    def fin_copy(k, s, arrived=False):
        piece = part(jnp.bitwise_xor(chip, s) if arrived else chip, k)
        rsem = fin_recv.at[k, s - 1] if s else table_recv
        return remote(piece, piece, table_send, rsem, jnp.bitwise_xor(me, neighbours[s]))

    even = ((0, CUT_BACK), (CUT_BACK, HALF - CUT_BACK))
    uneven = ((0, CUT), (CUT, HALF - CUT))
    going = ((uneven[0], even[1]), ((0, HALF),), ((0, HALF),), (even[0], uneven[1]))
    coming = (((0, HALF),), even, uneven, ((0, HALF),))

    def each_span(spans, act):
        for c, here in enumerate(spans):
            @pl.when(chip == c)
            def _():
                act(here)

    def hop(k, s, span):
        piece = part(jnp.bitwise_xor(chip, s), k, *span)
        return remote(piece, piece, hop_send, hop_recv.at[k, s - 1], jnp.bitwise_xor(me, neighbours[-s]))

    def relay(k, s, *span):
        piece = part(jnp.bitwise_xor(chip, s), k, *span)
        return remote(piece, piece, table_send, table_recv, partner)

    def far_relay(k):
        def act(spans):
            for r, span in enumerate(spans):
                piece = part(jnp.bitwise_xor(chip, last), k, *span)
                remote(piece, piece, table_send, hop_recv.at[k, r], partner).wait_recv()
                relay(k, last, *span).start()

        each_span(coming, act)

    def pass_on(k):
        for s in (1, 2):
            fin_copy(k, s, True).wait_recv()
            each_span(going, lambda spans: [hop(k, s, span).start() for span in spans[s - 1:s]])
            relay(k, s).start()

    def sent_parts(dev, owner):
        there = dev // 2
        rows = ((there == 0) & (owner != 0)) | ((there == 1) & (owner == last))
        cols = ((there == last) & (owner != last)) | ((there == 2) & (owner == 0))
        return ((0, NA), ~rows & ~cols), ((2, 2), rows), ((0, 2), cols)

    def stat_copy(n, whole):
        if whole:
            return remote(st_out.at[n], st_in.at[0, n], st_send_all, st_recv.at[n], 4 + core)
        return remote(st_out.at[n, 1], st_in.at[chip, n, 1], st_send, st_recv.at[n], 6 + core)

    def after_softmax(n, i, m, inv, rd):
        first = jnp.where(chip == 0, 4, 6)

        @pl.when((i >= first) & (chip != last))
        def _():
            lane = lax.broadcasted_iota(jnp.int32, (T, H), 1)
            table = jnp.where(lane == 0, m, jnp.where(lane == 1, inv, rd)).T
            for r in range(2):
                @pl.when(i % 2 == r)
                def _():
                    st_out[n, i // 2 - 2, HC * r:HC * (r + 1)] = table[:HC]

    def local_pair(x):
        owner = jnp.where(outer, x % HC + jnp.where(chip == 0, 1, 0), jnp.where(chip == 1, last, 0))
        n = jnp.where(outer, x // HC, x)
        return owner, n, 2 * core + n % 2, HC * owner + n // 2

    def local_loads(x, sl):
        _, n, bat, head = local_pair(x)
        copies = [pltpu.make_async_copy(rel.at[head, pl.ds(0, NA)], lrk.at[sl], l_sem.at[sl])]
        for a in range(NA):
            for r, src in enumerate((ins[a].at[bat, head], lx.at[a, n % 2, head])):
                where = core if r == 0 else 1 - core
                copies.append(pltpu.make_async_copy(src, lblk.at[sl, where, a], l_sem.at[sl]))
        return copies

    def local_send(x, c):
        sl = x % 2
        _, _, bat, head = local_pair(x)
        dst = out.at[pl.ds(2 * (c // 2), 2), bat, head]
        return remote(lres.at[sl, 1 - core], dst, lr_send.at[sl], lr_recv, partner)

    def local_work(lo, hi, c):
        for copy in local_loads(lo, lo % 2):
            copy.start()

        def one(x, _):
            sl = x % 2

            @pl.when(x + 1 < hi)
            def _():
                for copy in local_loads(x + 1, 1 - sl):
                    copy.start()

            pltpu.make_async_copy(rin.at[0, pl.ds(0, HC)], rin.at[0, pl.ds(0, HC)], l_sem.at[sl]).wait()

            @pl.when(x > 1)
            def _():
                local_send(x, c).wait_send()

            owner, n, bat, head = local_pair(x)
            u = bu[pl.ds(head, 1)]
            w = bw[pl.ds(head, 1)]
            q, do, key, val = [[lblk[sl, r, a] for r in range(2)] for a in range(NA)]
            table = lrk[sl]
            if c < 2:
                if c:
                    key = [rl[n, r, 0] for r in range(2)] + key
                    val = [rl[n, r, 1] for r in range(2)] + val
                for r in range(2):
                    upto = len(key) - 1 + r
                    res = row_tile(q[r], do[r], key[:upto], val[:upto], table, u, w)
                    for a in range(2):
                        lres[sl, r, a] = res[a]
            else:
                groups = (1,)
                piece = st_in.at[:, n, 1]
                if c != last:
                    groups = (0, 1)
                    piece = st_in.at[0, n]
                    q = q + [rl[n, r, 0] for r in range(2)]
                    do = do + [rl[n, r, 1] for r in range(2)]

                @pl.when((owner == 0) | (c != last))
                def _():
                    remote(piece, piece, st_send, st_recv.at[n], partner).wait_recv()

                stats = [st_in[owner, n, g] for g in groups]
                for a, res in enumerate(col_tiles(q, do, key, val, table, stats, u, w)):
                    for r in range(2):
                        lres[sl, r, a] = res[r]
            for a in range(2):
                out[2 * (c // 2) + a, bat, head] = lres[sl, core, a]
            local_send(x, c).start()
            return 0

        lax.fori_loop(lo, hi, one, 0)

    def local_count(c):
        return NU if c in (1, 2) else NU * HC

    @pl.when(chip == 0)
    def _():
        pair_wait(pl.ds(3, 9), "wait_recv")
        local_work(0, EARLY, 0)

    def send_tile(n, i):
        mask = jnp.bitwise_xor(me, i)
        for tile, whole, chips in ((6, False, chip != last), (4, True, chip == 0)):
            @pl.when((i == tile) & chips)
            def _():
                stat_copy(n, whole).start()

        for span, sent in sent_parts(i, chip):
            @pl.when((mask != 0) & sent)
            def _():
                some = pl.ds(*span)
                remote(rin.at[n, i, some], out.at[(some,) + pair_of(me, n)], out_send, out_recv, i).start()

        @pl.when(mask == 0)
        def _():
            for a in range(NA):
                out[(a,) + pair_of(me, n)] = rin[n, i, a]

    def run_unit(n, _):
        k = n // 2

        for g, group in enumerate(GROUPS):
            if g >= AHEAD:
                @pl.when(n == SEND_AT)
                def _():
                    send_group(*group)

            @pl.when(~outer & (n == FORWARD_AT[g]))
            def _():
                pass_forward(*group)

        @pl.when(n == 0)
        def _():
            pltpu.make_async_copy(rin.at[:, me], rin.at[:, me], in_loc).wait()

        for group in GROUPS:
            @pl.when(n == group[0])
            def _():
                arrive(*group)

        head = pl.ds(HC * chip + k, 1)
        unit(rin.at[n], rk.at[k], rkr.at[k], bu[head], bw[head], drk.at[k], duw.at[k], scratch,
             lambda i, m, inv, rd: after_softmax(n, i, m, inv, rd), lambda i: send_tile(n, i))

        @pl.when(n % 2 == 1)
        def _():
            copy = half_copy(k)
            copy.start()
            copy.wait()
            for r in range(NA):
                part(chip, k, r * T, T)[:] = (drk[k, NA * core + r] + pbuf[k, r]).T
            for s in range(3):
                fin_copy(k, s).start()

        return 0

    lax.fori_loop(0, NU, run_unit, 0)

    pass_on(0)
    pass_on(1)

    for mask in range(1, NT):
        remote(duw, duw_all.at[me], duw_send, duw_recv, jnp.bitwise_xor(me, mask)).start()
    duw_all[me] = duw[:]

    def late_work(c, heads):
        if c:
            pair_wait(heads, "wait_recv")
        local_work(0 if c else EARLY, local_count(c), c)

    at_chip(late_work)
    pass_on(2)
    for k in range(HC):
        far_relay(k)

    others = duw_all.at[pl.ds(0, NT - 1)]
    remote(others, others, duw_send, duw_recv, partner).wait()
    for h in range(NH):
        both = duw_all[2 * (h // HC), h % HC] + duw_all[2 * (h // HC) + 1, h % HC]
        for r, bias_out in enumerate((du_out, dw_out)):
            bias_out[h:h + 1] = both[r:r + 1]

    sent = rin.at[:, pl.ds(0, NT - 1)]
    remote(sent, sent, in_send, in_recv.at[0], partner).wait_send()
    sent = rin.at[:, pl.ds(0, 5)]
    remote(sent, sent, out_send, out_recv, partner).wait_send()
    for inner, count in ((True, 6), (False, 4)):
        @pl.when(outer != inner)
        def _():
            got = rin.at[:, pl.ds(0, count)]
            remote(got, got, out_send, out_recv, partner).wait_recv()

    @pl.when(~outer)
    def _():
        remote(rl, rl, fw_send, in_recv.at[0], partner).wait_send()

    @pl.when(chip != last)
    def _():
        some = st_out.at[:, 1]
        remote(some, some, st_send, st_recv.at[0], partner).wait_send()

    @pl.when(chip == 0)
    def _():
        remote(st_out, st_out, st_send_all, st_recv.at[0], partner).wait_send()

    def end_local(c, heads):
        pair_wait(heads, "wait_send")
        count = local_count(c)
        for x in (count - 2, count - 1):
            local_send(x, c).wait_send()
        whole = out.at[0, pl.ds(0, count // NU)]
        remote(whole, whole, lr_send.at[0], lr_recv, partner).wait_recv()

    at_chip(end_local)
    def hops_sent(spans):
        sent = drk_out.at[pl.ds(0, HC), pl.ds(0, sum(rows for _, rows in spans))]
        remote(sent, sent, hop_send, table_recv, partner).wait_send()

    each_span(going, hops_sent)
    sent = drk_out.at[:, pl.ds(0, 6 * T)]
    remote(sent, sent, table_send, table_recv, partner).wait_send()
    got = drk_out.at[:, pl.ds(0, HALF)]
    remote(got, got, table_send, table_recv, partner).wait_recv()


def exchange_attend(xq, xd, xk, xv, bias_u, bias_w, rel):
    any_spec = pl.BlockSpec(memory_space=pl.ANY)
    vmem_spec = pl.BlockSpec(memory_space=pltpu.VMEM)
    dma = pltpu.SemaphoreType.DMA
    acts = pltpu.VMEM((NA, NA, NH, T, D), BF)
    bias = pltpu.VMEM((NH, D), F32)
    heads = pltpu.VMEM((HC, NT, T, D), BF)
    per_pair = dma((NU,))
    per_head = dma((HC,))
    two = dma((2,))
    one = dma(())
    return pl.pallas_call(
        kernel,
        out_shape=(acts, pltpu.VMEM((NH, NT * T, D), F32), bias, bias,
                   jax.ShapeDtypeStruct((NA, 2, NH, T, D), BF)),
        in_specs=[any_spec] * 7,
        out_specs=(vmem_spec,) * 4 + (any_spec,),
        scratch_shapes=[
            pltpu.VMEM((NU, NT, NA, T, D), BF), pltpu.VMEM((NU, 2, 2, T, D), BF), pltpu.VMEM((HC, NT, D, T), F32),
            pltpu.VMEM((HC, NA, D, T), F32), pltpu.VMEM((HC, 8, D), F32), pltpu.VMEM((NT, HC, 8, D), F32),
            heads, heads, pltpu.VMEM((2, NH, D), BF), bias, bias,
            pltpu.VMEM((2, 2, NA, T, D), BF), pltpu.VMEM((2, NA, T, D), BF), pltpu.VMEM((2, 2, 2, T, D), BF),
            pltpu.VMEM((NU, 2, 8, T), F32), pltpu.VMEM((HC, NU, 2, 8, T), F32),
            per_pair, per_pair, per_pair, per_head, per_head, dma((HC, 2)), dma((HC, 2)), two, two]
        + [one] * 9 + [per_head] + [one] * 6
        + UNIT_SCRATCH,
        compiler_params=pltpu.CompilerParams(collective_id=0, has_side_effects=True, vmem_limit_bytes=VMEM_LIMIT),
    )(xq, xd, xk, xv, bias_u, bias_w, rel)


def write_kernel(acts, table, bias_u, bias_w, *refs):
    sem = refs[-1]
    srcs = [acts.at[a] for a in range(NA)] + [table, bias_u, bias_w]
    copies = [pltpu.make_async_copy(src, dst, sem.at[n]) for n, (src, dst) in enumerate(zip(srcs, refs[:-1]))]
    for r, copy in enumerate(copies):
        copy.start(priority=r % 2)
    for copy in copies:
        copy.wait()


def write_out(arrs):
    shapes = [arrs[0].shape[1:]] * NA + [arr.shape for arr in arrs[1:]]
    types = [arrs[0].dtype] * NA + [arr.dtype for arr in arrs[1:]]
    return pl.pallas_call(
        write_kernel,
        out_shape=tuple(map(jax.ShapeDtypeStruct, shapes, types)),
        in_specs=[pl.BlockSpec(memory_space=pltpu.VMEM)] * len(arrs),
        out_specs=(pl.BlockSpec(memory_space=pl.ANY),) * len(shapes),
        scratch_shapes=[pltpu.SemaphoreType.DMA((len(shapes),))],
        compiler_params=pltpu.CompilerParams(vmem_limit_bytes=1024 * 1024),
    )(*[pltpu.with_memory_space_constraint(arr, pltpu.VMEM) for arr in arrs])


def solution(mesh):
    seq_spec = P(None, 'cp', None, None)

    def local(query, key_in, value, bias_u, bias_w, rel_k, d_out):
        def by_head(arr):
            return arr.transpose(0, 2, 1, 3)

        rel = rel_k.transpose(1, 0, 2).reshape(NH, NT, T, D)
        acts = [by_head(arr) for arr in (query, d_out, key_in, value)]
        res = write_out(exchange_attend(*acts, bias_u, bias_w, rel)[:4])
        d_rel = res[4].reshape(NH, NT * T, D).transpose(1, 0, 2)
        return tuple(by_head(arr) for arr in res[:4]) + (res[5], res[6], d_rel)

    return jax.shard_map(local, mesh=mesh,
                         in_specs=(seq_spec, seq_spec, seq_spec, P(), P(), P(), seq_spec),
                         out_specs=(seq_spec, seq_spec, seq_spec, seq_spec, P(), P(), P()),
                         check_vma=False)
```
